512 devices in a mesh: cons: 16 (over y, x_lo), blk: 32 (over x_hi, z, core).
Axes of the slice: x: 4 (x_hi: 2, x_lo: 2; x = x_hi * 2 + x_lo), y: 8, z: 8, core: 2. Of those that a mesh axis runs over, the one named last changes fastest.
Arguments:
- elevation: bfloat16 [16, 1280, 6144], P('cons', 'blk'), may hold values from -6 to 6
- legendre: bfloat16 [1280, 768, 768], P('blk', 'cons'), may hold values from -5 to 5, as said below
- cycle_weight: float32 [1280], P('blk'), may hold values from 0.0001782951 to 0.0014263608
- love_factor: float32 [768], replicated, may hold values from 0.000390625 to 0.0052083335
- assignment: int32 [16], replicated, may hold values from 0 to 15, each once
Outputs:
- loading: float32 [16, 1280, 6144], P('cons', 'blk')
The draws below stay inside these ranges and needn't reach their ends.
Inputs may be any that keep to these rules, and one draw needn't show every extreme that they name: `legendre`: fully normalized associated Legendre functions (the square integrates to 1 over [-1, 1]) of each cycle's latitude, every cycle within 26 degrees of the equator; zero where the degree is below the order.
All inputs are finite; a program needn't handle non-finite values.
Results may differ from the reference program's by a relative error of at most 0.02.
Values may be sent and summed in bfloat16 or wider, within the bound.
A program may use at most 128 MiB of HBM per device.

```python
import math
import jax
import jax.numpy as jnp
from jax import lax

FIELDS = 16
DEGREES = 768
ORDERS = 768
LONS = 6144
CYCLE_DEV = 40
CYCLES = 1280
N_BLK = 32


def draw_legendre(key, part):
    cosine_vals = jax.random.uniform(jax.random.fold_in(key, 11), (CYCLES,), jnp.float32, -0.43, 0.43)
    sine_vals = jnp.sqrt(1.0 - cosine_vals * cosine_vals)
    order_vals = jnp.arange(ORDERS).astype(jnp.float32)
    growth = 0.5 * jnp.log((2.0 * order_vals + 1.0) / jnp.maximum(2.0 * order_vals, 1.0))
    log_steps = jnp.where(order_vals[None, :] > 0.0, growth[None, :] + jnp.log(sine_vals)[:, None], 0.0)
    diagonal = jnp.exp(0.5 * jnp.log(0.5) + jnp.cumsum(log_steps, axis=1))
    order_sq = order_vals[None, :] * order_vals[None, :]

    def advance(state, degree):
        previous, earlier = state
        level = degree.astype(jnp.float32)
        coef_now = jnp.sqrt((4.0 * level * level - 1.0) / jnp.maximum(level * level - order_sq, 1.0))
        lower = level - 1.0
        coef_before = jnp.sqrt(jnp.maximum(4.0 * lower * lower - 1.0, 1.0) / jnp.maximum(lower * lower - order_sq, 1.0))
        generic = coef_now * (cosine_vals[:, None] * previous - earlier / coef_before)
        first_up = jnp.sqrt(2.0 * order_vals[None, :] + 3.0) * cosine_vals[:, None] * previous
        values = jnp.where(level == order_vals[None, :], diagonal, jnp.where(level == order_vals[None, :] + 1.0, first_up, jnp.where(level > order_vals[None, :] + 1.0, generic, 0.0)))
        return ((values, previous), values)
    zeros = jnp.zeros((CYCLES, ORDERS), jnp.float32)
    _, table = lax.scan(advance, (zeros, zeros), jnp.arange(DEGREES, dtype=jnp.int32))
    return jnp.transpose(table, (1, 2, 0)).astype(jnp.bfloat16)


def level_of(own_key, dims, shards, smallest, high):
    def one(dim, shards_of):
        steps = jax.random.uniform(jax.random.fold_in(jax.random.fold_in(own_key, 6), dim), (shards_of,), jnp.float32, smallest / len(shards), high / len(shards))
        return jnp.repeat(jnp.exp(steps), dims[dim] // shards_of).reshape((-1,) + (1,) * (len(dims) - dim - 1))

    level = one(*shards[0])
    for cut in shards[1:]:
        level = level * one(*cut)
    return level


def normal_values(own_key, dims, deviation, bound, split=(), kind=jnp.bfloat16):
    entries = jax.random.normal(own_key, dims, jnp.float32) * deviation
    if len(split) > 0:
        entries = level_of(own_key, dims, split, -0.22, 0.18) * entries
    return jnp.clip(entries, min=-bound, max=bound).astype(kind)


def setup_inputs(seed: int = 0) -> dict:
    keys = jax.random.split(jax.random.key(seed), 6)
    return {
        "elevation": normal_values(keys[0], (FIELDS, CYCLES, LONS), 1.0, 6.0, ((0, 16), (1, 32))),
        "legendre": draw_legendre(jax.random.fold_in(keys[5], 71), 0),
        "cycle_weight": jnp.clip(jnp.exp(math.log(0.0014263608) - 2.0794415 * jax.random.uniform(keys[2], (CYCLES,), jnp.float32) ** level_of(keys[2], (CYCLES,), ((0, 32),), -0.2, 0.2)), 0.0001782951, 0.0014263608),
        "love_factor": jnp.clip(jnp.exp(jax.random.uniform(keys[3], (DEGREES,), jnp.float32, math.log(0.000390625), math.log(0.0052083335))), 0.000390625, 0.0052083335),
        "assignment": jax.random.permutation(keys[4], FIELDS).astype(jnp.int32),
    }


def fourier_block(offset, length, period, orders):
    lon_index = offset + jnp.arange(length, dtype=jnp.int32)
    order_index = jnp.arange(orders, dtype=jnp.int32)
    phases = (lon_index[:, None] * order_index[None, :]) % period
    angles = phases.astype(jnp.float32) * jnp.float32(2.0 * 3.141592653589793 / period)
    stacked = jnp.stack([jnp.cos(angles), -jnp.sin(angles)], axis=2)
    return stacked.reshape(length, 2 * orders).astype(jnp.bfloat16)


def reference(elevation, legendre, cycle_weight, love_factor, assignment):
    table = fourier_block(0, LONS, LONS, ORDERS)

    def forward(field):
        summed = jnp.dot(field, table, preferred_element_type=jnp.float32)
        return (summed * cycle_weight[:, None]).astype(jnp.bfloat16)

    spectra = lax.map(forward, elevation)
    ordered = spectra[assignment].reshape(FIELDS, CYCLES, ORDERS, 2)

    def add_block(running, block_index):
        start = (block_index * CYCLE_DEV).astype(jnp.int32)
        values = lax.dynamic_slice_in_dim(legendre, start, CYCLE_DEV, 0).astype(jnp.float32)
        spec_block = lax.dynamic_slice_in_dim(ordered, start, CYCLE_DEV, 1).astype(jnp.float32)
        partial_value = jnp.einsum('jml,gjmp->lpgm', values, spec_block)
        rounded = lax.optimization_barrier(partial_value.astype(jnp.bfloat16))
        return running + rounded.astype(jnp.float32), None

    zeros = jnp.zeros((DEGREES, 2, FIELDS, ORDERS), jnp.float32)
    analysis, _ = lax.scan(add_block, zeros, jnp.arange(N_BLK, dtype=jnp.int32))
    coefficients = (analysis * love_factor[:, None, None, None]).astype(jnp.bfloat16)
    order_factor = jnp.where(jnp.arange(ORDERS) == 0, 1.0, 2.0).astype(jnp.float32)

    def synth_block(block_index):
        start = (block_index * CYCLE_DEV).astype(jnp.int32)
        values = lax.dynamic_slice_in_dim(legendre, start, CYCLE_DEV, 0).astype(jnp.float32)
        summed = jnp.einsum('jml,lpgm->gjmp', values, coefficients.astype(jnp.float32))
        return (summed * order_factor[None, None, :, None]).astype(jnp.bfloat16)

    blocks = lax.map(synth_block, jnp.arange(N_BLK, dtype=jnp.int32))
    synthesis = jnp.moveaxis(blocks, 0, 1).reshape(FIELDS, CYCLES, 2 * ORDERS)

    def inverse(field):
        return jnp.dot(field, table.T, preferred_element_type=jnp.float32)

    return lax.map(inverse, synthesis)
```

```python
import math
import numpy as np
import jax
import jax.numpy as jnp
from jax import lax
from jax.experimental import pallas as pl
from jax.experimental.pallas import tpu as pltpu
from jax.sharding import Mesh
from jax.sharding import PartitionSpec as P

RADIX = 48
LANES = 128
CYC = 40
TRI = 3


def by_phase(value, turn):
    re, im = value
    cos, sin = math.cos(2 * math.pi * turn), math.sin(2 * math.pi * turn)
    cos = 0.0 if abs(cos) < 1e-12 else cos
    sin = 0.0 if abs(sin) < 1e-12 else sin

    def scaled(array, factor):
        if array is None or factor == 0.0:
            return None
        if abs(factor - 1.0) < 1e-12:
            return array
        if abs(factor + 1.0) < 1e-12:
            return -array
        return array * np.float32(factor)

    return (
        added(scaled(re, cos), scaled(im, -sin)),
        added(scaled(re, sin), scaled(im, cos)),
    )


def added(a, b):
    if a is None:
        return b
    return a if b is None else a + b


def plus(a, b):
    return added(a[0], b[0]), added(a[1], b[1])


def conj(a):
    return a[0], None if a[1] is None else -a[1]


def at(half, index, length):
    index %= length
    return half[index] if 2 * index <= length else conj(half[length - index])


def factor_of(length):
    return 4 if length % 4 == 0 else (3 if length % 3 == 0 else 2)


def real_fft(values):
    n = len(values)
    if n == 1:
        return [(values[0], None)]
    p = factor_of(n)
    parts = [real_fft(values[i::p]) for i in range(p)]
    out = []
    for k in range(n // 2 + 1):
        total = at(parts[0], k, n // p)
        for i in range(1, p):
            total = plus(total, by_phase(at(parts[i], k, n // p), -i * k / n))
        out.append(total)
    return out


def real_inverse(half, n):
    if n == 1:
        return [half[0][0]]
    p = factor_of(n)
    short = n // p
    out = [None] * n
    for a in range(p):
        folded = []
        for r in range(short // 2 + 1):
            total = (None, None)
            for s in range(p):
                index = r + s * short
                total = plus(total, by_phase(at(half, index, n), index * a / n))
            if r == 0 or 2 * r == short:
                total = (total[0], None)
            folded.append(total)
        for kk, value in enumerate(real_inverse(folded, short)):
            out[p * kk + a] = value
    return out


def phase_tables(period):
    lane = np.arange(LANES)
    turn = np.arange(RADIX)[:, None] * lane[None, :] / period
    twiddle = np.stack([np.cos(2 * np.pi * turn), np.sin(2 * np.pi * turn)], 1)
    q = np.arange(period // RADIX // 8)[:, None] * lane[None, :] / LANES
    cos, sin = np.cos(2 * np.pi * q), np.sin(2 * np.pi * q)
    basis = np.concatenate([np.concatenate([cos, sin], 1), np.concatenate([-sin, cos], 1)], 0)
    return twiddle.reshape(2 * RADIX, LANES).astype(np.float32), basis.astype(jnp.bfloat16)


def forward_kernel(x_ref, weight_ref, twiddle_ref, basis_ref, out_ref, wide, mixed, rows):
    cons = out_ref.shape[0]
    wide[...] = x_ref[...].reshape(wide.shape).astype(jnp.float32)
    for triple in range(RADIX // TRI):
        mixed[triple * LANES + TRI * CYC : (triple + 1) * LANES, :] = jnp.zeros(
            (LANES - TRI * CYC, 2 * LANES), jnp.float32
        )

    @pl.loop(0, CYC // 8)
    def _(group):
        lines = pl.ds(pl.multiple_of(group * 8, 8), 8)
        half = real_fft([wide[lines, k * LANES : (k + 1) * LANES] for k in range(RADIX)])
        for r in range(RADIX):
            re, im = at(half, r, RADIX)
            cos, sin = twiddle_ref[2 * r : 2 * r + 1, :], twiddle_ref[2 * r + 1 : 2 * r + 2, :]
            if im is None:
                new_re, new_im = re * cos, -re * sin
            else:
                new_re, new_im = re * cos + im * sin, im * cos - re * sin
            start = (r // TRI) * LANES + (r % TRI) * CYC
            place = pl.ds(pl.multiple_of(start + group * 8, 8), 8)
            mixed[place, 0:LANES] = new_re
            mixed[place, LANES:] = new_im

    for triple in range(RADIX // TRI):
        block = mixed[triple * LANES : (triple + 1) * LANES, :].astype(jnp.bfloat16)
        got = lax.dot_general(
            basis_ref[...], block, (((1,), (1,)), ((), ())), preferred_element_type=jnp.float32
        )
        rows[triple * 2 * cons : (triple + 1) * 2 * cons, :] = got * weight_ref[...]
    for c in range(cons):
        for h in range(2):
            both = [
                rows[pl.ds(h * 16 * cons + p * cons + c, 8, stride=2 * cons), :] for p in range(2)
            ]
            out_ref[c, h] = jnp.concatenate(both, axis=0).astype(jnp.bfloat16)


def inverse_kernel(z_ref, twiddle_ref, basis_ref, out_ref, rows, mixed):
    cons = z_ref.shape[0]
    for c in range(cons):
        for h in range(2):
            place = (2 * c + h) * 16
            rows[place : place + 16, :] = z_ref[c, h].astype(jnp.float32)
    for triple in range(RADIX // TRI):
        h, t = divmod(triple, 8)
        both = [rows[pl.ds(h * 16 + p * 8 + t, cons, stride=32), :] for p in range(2)]
        lines = jnp.concatenate(both, axis=0).T.astype(jnp.bfloat16)
        mixed[triple * LANES : (triple + 1) * LANES, :] = jnp.dot(
            lines, basis_ref[...], preferred_element_type=jnp.float32
        )

    @pl.loop(0, CYC // 8)
    def _(group):
        turned = []
        for r in range(RADIX):
            start = (r // TRI) * LANES + (r % TRI) * CYC
            place = pl.ds(pl.multiple_of(start + group * 8, 8), 8)
            re, im = mixed[place, 0:LANES], mixed[place, LANES:]
            cos, sin = twiddle_ref[2 * r : 2 * r + 1, :], twiddle_ref[2 * r + 1 : 2 * r + 2, :]
            turned.append((re * cos - im * sin, re * sin + im * cos))
        middle = RADIX // 2
        half = [(turned[0][0], None)]
        for r in range(1, middle):
            pair = plus(turned[r], conj(turned[RADIX - r]))
            half.append((pair[0] * np.float32(0.5), pair[1] * np.float32(0.5)))
        half.append((turned[middle][0], None))
        lines = pl.ds(pl.multiple_of(group * 8, 8), 8)
        for k, value in enumerate(real_inverse(half, RADIX)):
            out_ref[0, lines, k * LANES : (k + 1) * LANES] = value


def forward(elevation, lane_weight, cons):
    period = elevation.shape[-1]
    twiddle, basis = phase_tables(period)
    return pl.pallas_call(
        forward_kernel,
        out_shape=jax.ShapeDtypeStruct((cons, 2, 16, LANES), jnp.bfloat16),
        in_specs=[pl.BlockSpec(memory_space=pltpu.VMEM)] * 4,
        out_specs=pl.BlockSpec(memory_space=pltpu.VMEM),
        scratch_shapes=[
            pltpu.VMEM((CYC, period), jnp.float32),
            pltpu.VMEM((RADIX // TRI * LANES, 2 * LANES), jnp.float32),
            pltpu.VMEM((RADIX // TRI * 2 * cons, LANES), jnp.float32),
        ],
        name="forward",
    )(elevation, lane_weight, jnp.asarray(twiddle), jnp.asarray(basis))


def inverse(pieces, period):
    cons = pieces.shape[0]
    twiddle, basis = phase_tables(period)
    return pl.pallas_call(
        inverse_kernel,
        out_shape=jax.ShapeDtypeStruct((1, CYC, period), jnp.float32),
        in_specs=[pl.BlockSpec(memory_space=pltpu.VMEM)] * 3,
        out_specs=pl.BlockSpec(memory_space=pltpu.VMEM),
        scratch_shapes=[
            pltpu.VMEM((2 * cons * 16, LANES), jnp.float32),
            pltpu.VMEM((RADIX // TRI * LANES, 2 * LANES), jnp.float32),
        ],
        name="inverse",
    )(pieces, jnp.asarray(twiddle), jnp.asarray(basis))


BLK = ("blk_0", "blk_1", "blk_2")


def filled_up(lines, length):
    spare = -lines.shape[0] % length
    if not spare:
        return lines
    return jnp.concatenate([lines, jnp.zeros((spare, *lines.shape[1:]), lines.dtype)])


def from_everyone(array, axis):
    copies = jnp.broadcast_to(array, (lax.axis_size(axis), *array.shape))
    return lax.all_to_all(copies, axis, split_axis=0, concat_axis=0, tiled=True)


def joined_along(tiles, dim):
    dims = list(tiles.shape[1:])
    dims[dim] *= tiles.shape[0]
    return jnp.moveaxis(tiles, 0, dim).reshape(dims)


def gathered_by_axis(array, axes, dim):
    far, near = axes
    tiles = from_everyone(from_everyone(array, far), near)
    return joined_along(tiles.swapaxes(0, 1).reshape(-1, *array.shape), dim)


def in_blocks(array, dim, length):
    dims = array.shape
    tiles = array.reshape(*dims[:dim], length, dims[dim] // length, *dims[dim + 1 :])
    return jnp.moveaxis(tiles, dim, 0)


def sent_and_summed(array, axis, dim):
    length = lax.axis_size(axis)
    tiles = lax.all_to_all(in_blocks(array, dim, length), axis, 0, 0, tiled=True)
    return jnp.sum(tiles.astype(jnp.float32), axis=0)


def summed_rows(array, axes, dim):
    far, near = axes
    tiles = in_blocks(array, dim, lax.axis_size(far))
    nearer = sent_and_summed(tiles, near, dim + 1)
    arrived = lax.all_to_all(
        nearer.astype(jnp.bfloat16), far, split_axis=0, concat_axis=0, tiled=True
    )
    return arrived.astype(jnp.float32).sum(axis=0)


def sum_by_parts(array, axes):
    lines = array.reshape(-1, array.shape[-1])
    padded = filled_up(lines, lax.axis_size(axes[0]) * lax.axis_size(axes[1]))
    whole = gathered_by_axis(summed_rows(padded, axes, 0).astype(jnp.bfloat16), axes, 0)
    return lax.slice_in_dim(whole, 0, len(lines)).reshape(array.shape).astype(jnp.float32)

def local(elevation, legendre, cycle_weight, love_factor, assignment):
    orders_dev = legendre.shape[1]
    cons = lax.axis_size("cons")
    lane_weight = jnp.pad(jnp.tile(cycle_weight, TRI), (0, LANES - TRI * CYC))[None, :]
    pieces = forward(elevation, lane_weight, cons)
    moved = lax.all_to_all(pieces, "cons", split_axis=0, concat_axis=0, tiled=True)
    moved = moved[..., : TRI * CYC].reshape(cons, 2, 2, 8, TRI, CYC)
    one_hot = (assignment[:, None] == jnp.arange(cons, dtype=jnp.int32)[None, :]).astype(
        jnp.bfloat16
    )
    ordered = jnp.einsum(
        "gf,fhptij->ghptij", one_hot, moved, preferred_element_type=jnp.float32
    ).astype(jnp.bfloat16)
    ordered = ordered.transpose(0, 2, 5, 1, 3, 4).reshape(cons, 2, CYC, orders_dev)
    whole = sum_by_parts(
        jnp.einsum("jml,gpjm->mpgl", legendre, ordered, preferred_element_type=jnp.float32).astype(
            jnp.bfloat16
        ),
        (("blk_0", "blk_1"), "blk_2"),
    )
    coefficients = (whole * love_factor).astype(jnp.bfloat16)
    order_index = lax.axis_index("cons") * orders_dev + jnp.arange(orders_dev, dtype=jnp.int32)
    order_factor = jnp.where(order_index == 0, 1.0, 2.0).astype(jnp.float32)
    summed = jnp.einsum(
        "jml,mpgl->gpmj", legendre, coefficients, preferred_element_type=jnp.float32
    )
    synthesis = (summed * order_factor[None, None, :, None]).astype(jnp.bfloat16)
    synthesis = synthesis.reshape(cons, 2, 2, 8, TRI * CYC).transpose(0, 2, 1, 3, 4)
    synthesis = jnp.pad(
        synthesis.reshape(cons, 2, 16, TRI * CYC), ((0, 0),) * 3 + ((0, LANES - TRI * CYC),)
    )
    returned = lax.all_to_all(synthesis, "cons", split_axis=0, concat_axis=0, tiled=True)
    return inverse(returned, elevation.shape[-1])


def solution(mesh):
    torus = Mesh(
        mesh.devices.reshape(mesh.shape["cons"], 2, 8, 2), ("cons", "blk_0", "blk_1", "blk_2")
    )
    placed = (P("cons", BLK, None), P(BLK, "cons", None), P(BLK), P(), P())
    return jax.shard_map(
        local, mesh=torus, in_specs=placed, out_specs=P("cons", BLK, None), check_vma=False
    )
```

```python
import functools
import math
import numpy as np
import jax
import jax.numpy as jnp
from jax import lax
from jax.experimental import pallas as pl
from jax.experimental.pallas import tpu as pltpu
from jax.sharding import PartitionSpec as P

RADIX = 48
LANES = 128
CYC = 40
TRI = 3


def by_phase(value, turn):
    re, im = value
    cos, sin = math.cos(2 * math.pi * turn), math.sin(2 * math.pi * turn)
    cos = 0.0 if abs(cos) < 1e-12 else cos
    sin = 0.0 if abs(sin) < 1e-12 else sin

    def scaled(array, factor):
        if array is None or factor == 0.0:
            return None
        if abs(factor - 1.0) < 1e-12:
            return array
        if abs(factor + 1.0) < 1e-12:
            return -array
        return array * np.float32(factor)

    return (
        added(scaled(re, cos), scaled(im, -sin)),
        added(scaled(re, sin), scaled(im, cos)),
    )


def added(a, b):
    if a is None:
        return b
    return a if b is None else a + b


def plus(a, b):
    return added(a[0], b[0]), added(a[1], b[1])


def conj(a):
    return a[0], None if a[1] is None else -a[1]


def at(half, index, length):
    index %= length
    return half[index] if 2 * index <= length else conj(half[length - index])


def factor_of(length):
    return 4 if length % 4 == 0 else (3 if length % 3 == 0 else 2)


def real_fft(values):
    n = len(values)
    if n == 1:
        return [(values[0], None)]
    p = factor_of(n)
    parts = [real_fft(values[i::p]) for i in range(p)]
    out = []
    for k in range(n // 2 + 1):
        total = at(parts[0], k, n // p)
        for i in range(1, p):
            total = plus(total, by_phase(at(parts[i], k, n // p), -i * k / n))
        out.append(total)
    return out


def real_inverse(half, n):
    if n == 1:
        return [half[0][0]]
    p = factor_of(n)
    short = n // p
    out = [None] * n
    for a in range(p):
        folded = []
        for r in range(short // 2 + 1):
            total = (None, None)
            for s in range(p):
                index = r + s * short
                total = plus(total, by_phase(at(half, index, n), index * a / n))
            if r == 0 or 2 * r == short:
                total = (total[0], None)
            folded.append(total)
        for kk, value in enumerate(real_inverse(folded, short)):
            out[p * kk + a] = value
    return out


def phase_tables(period):
    lane = np.arange(LANES)
    turn = np.arange(RADIX)[:, None] * lane[None, :] / period
    twiddle = np.stack([np.cos(2 * np.pi * turn), np.sin(2 * np.pi * turn)], 1)
    q = np.arange(period // RADIX // 8)[:, None] * lane[None, :] / LANES
    cos, sin = np.cos(2 * np.pi * q), np.sin(2 * np.pi * q)
    basis = np.concatenate([np.concatenate([cos, sin], 1), np.concatenate([-sin, cos], 1)], 0)
    return twiddle.reshape(2 * RADIX, LANES).astype(np.float32), basis.astype(jnp.bfloat16)


def forward_kernel(x_ref, weight_ref, twiddle_ref, basis_ref, out_ref, wide, mixed, rows):
    cons = out_ref.shape[0]
    wide[...] = x_ref[...].reshape(wide.shape).astype(jnp.float32)
    for triple in range(RADIX // TRI):
        mixed[triple * LANES + TRI * CYC : (triple + 1) * LANES, :] = jnp.zeros(
            (LANES - TRI * CYC, 2 * LANES), jnp.float32
        )

    @pl.loop(0, CYC // 8)
    def _(group):
        lines = pl.ds(pl.multiple_of(group * 8, 8), 8)
        half = real_fft([wide[lines, k * LANES : (k + 1) * LANES] for k in range(RADIX)])
        for r in range(RADIX):
            re, im = at(half, r, RADIX)
            cos, sin = twiddle_ref[2 * r : 2 * r + 1, :], twiddle_ref[2 * r + 1 : 2 * r + 2, :]
            if im is None:
                new_re, new_im = re * cos, -re * sin
            else:
                new_re, new_im = re * cos + im * sin, im * cos - re * sin
            start = (r // TRI) * LANES + (r % TRI) * CYC
            place = pl.ds(pl.multiple_of(start + group * 8, 8), 8)
            mixed[place, 0:LANES] = new_re
            mixed[place, LANES:] = new_im

    for triple in range(RADIX // TRI):
        block = mixed[triple * LANES : (triple + 1) * LANES, :].astype(jnp.bfloat16)
        got = lax.dot_general(
            basis_ref[...], block, (((1,), (1,)), ((), ())), preferred_element_type=jnp.float32
        )
        rows[triple * 2 * cons : (triple + 1) * 2 * cons, :] = got * weight_ref[...]
    for c in range(cons):
        for h in range(2):
            both = [
                rows[pl.ds(h * 16 * cons + p * cons + c, 8, stride=2 * cons), :] for p in range(2)
            ]
            out_ref[c, h] = jnp.concatenate(both, axis=0).astype(jnp.bfloat16)


def inverse_kernel(z_ref, twiddle_ref, basis_ref, out_ref, rows, mixed):
    cons = z_ref.shape[0]
    for c in range(cons):
        for h in range(2):
            place = (2 * c + h) * 16
            rows[place : place + 16, :] = z_ref[c, h].astype(jnp.float32)
    for triple in range(RADIX // TRI):
        h, t = divmod(triple, 8)
        both = [rows[pl.ds(h * 16 + p * 8 + t, cons, stride=32), :] for p in range(2)]
        lines = jnp.concatenate(both, axis=0).T.astype(jnp.bfloat16)
        mixed[triple * LANES : (triple + 1) * LANES, :] = jnp.dot(
            lines, basis_ref[...], preferred_element_type=jnp.float32
        )

    @pl.loop(0, CYC // 8)
    def _(group):
        turned = []
        for r in range(RADIX):
            start = (r // TRI) * LANES + (r % TRI) * CYC
            place = pl.ds(pl.multiple_of(start + group * 8, 8), 8)
            re, im = mixed[place, 0:LANES], mixed[place, LANES:]
            cos, sin = twiddle_ref[2 * r : 2 * r + 1, :], twiddle_ref[2 * r + 1 : 2 * r + 2, :]
            turned.append((re * cos - im * sin, re * sin + im * cos))
        middle = RADIX // 2
        half = [(turned[0][0], None)]
        for r in range(1, middle):
            pair = plus(turned[r], conj(turned[RADIX - r]))
            half.append((pair[0] * np.float32(0.5), pair[1] * np.float32(0.5)))
        half.append((turned[middle][0], None))
        lines = pl.ds(pl.multiple_of(group * 8, 8), 8)
        for k, value in enumerate(real_inverse(half, RADIX)):
            out_ref[0, lines, k * LANES : (k + 1) * LANES] = value


def forward(elevation, lane_weight, cons):
    period = elevation.shape[-1]
    twiddle, basis = phase_tables(period)
    return pl.pallas_call(
        forward_kernel,
        out_shape=jax.ShapeDtypeStruct((cons, 2, 16, LANES), jnp.bfloat16),
        in_specs=[pl.BlockSpec(memory_space=pltpu.VMEM)] * 4,
        out_specs=pl.BlockSpec(memory_space=pltpu.VMEM),
        scratch_shapes=[
            pltpu.VMEM((CYC, period), jnp.float32),
            pltpu.VMEM((RADIX // TRI * LANES, 2 * LANES), jnp.float32),
            pltpu.VMEM((RADIX // TRI * 2 * cons, LANES), jnp.float32),
        ],
        name="forward",
    )(elevation, lane_weight, jnp.asarray(twiddle), jnp.asarray(basis))


def inverse(pieces, period):
    cons = pieces.shape[0]
    twiddle, basis = phase_tables(period)
    return pl.pallas_call(
        inverse_kernel,
        out_shape=jax.ShapeDtypeStruct((1, CYC, period), jnp.float32),
        in_specs=[pl.BlockSpec(memory_space=pltpu.VMEM)] * 3,
        out_specs=pl.BlockSpec(memory_space=pltpu.VMEM),
        scratch_shapes=[
            pltpu.VMEM((2 * cons * 16, LANES), jnp.float32),
            pltpu.VMEM((RADIX // TRI * LANES, 2 * LANES), jnp.float32),
        ],
        name="inverse",
    )(pieces, jnp.asarray(twiddle), jnp.asarray(basis))


MESH = pl.DeviceIdType.MESH
F32 = jnp.float32
BF16 = jnp.bfloat16
KERNEL_ID = 0


def middle_kernel(
    ring, cons, pieces, legendre, love, assignment, out,
    held, wide, table, got, mixed, lines, part, first, later, staged, sent, other, coef,
    rows, back, returned,
    own_sem, swap_send, swap_recv, out_send, out_recv, sum_send, sum_recv, pair_send, pair_recv,
    all_send, all_recv, back_send, back_recv,
):
    c, b = lax.axis_index("cons"), lax.axis_index("blk")
    core = lax.rem(b, 2)
    z = lax.rem(b // 2, ring)
    line = b // (2 * ring)
    chip = b - core
    me = 2 * c + core
    peers = 2 * cons
    far = ring // 2
    depth = legendre.shape[2]
    half_orders = TRI * ring
    full = 2 * cons
    barrier = pltpu.get_barrier_semaphore()

    def slot(offset):
        return lax.rem(z + offset + ring, ring)

    def on_ring(offset):
        return (c, line * 2 * ring + slot(offset) * 2 + core)

    def peer(offset):
        index = lax.rem(me + offset, peers)
        return index // 2, lax.rem(index, 2)

    def remote(source, target, send, recv, device):
        return pltpu.make_async_remote_copy(
            src_ref=source,
            dst_ref=target,
            send_sem=send,
            recv_sem=recv,
            device_id=device,
            device_id_type=MESH,
        )

    def exchange(offset, source, landing, send, recv):
        there = peer(offset)
        return remote(
            source.at[there[0], there[1]],
            landing.at[c, core],
            send.at[offset],
            recv.at[offset],
            (there[0], chip + there[1]),
        )

    across = (c, (1 - line) * 2 * ring + z * 2 + core)

    @pl.loop(1, peers)
    def _(offset):
        there = peer(offset)
        pl.semaphore_signal(
            barrier, inc=1, device_id=(there[0], chip + there[1]), device_id_type=MESH
        )

    for target in (on_ring(1), on_ring(-1), across):
        pl.semaphore_signal(barrier, inc=1, device_id=target, device_id_type=MESH)

    def half_of(which):
        return legendre.at[:, pl.ds(pl.multiple_of(which * half_orders, 8), half_orders), :]

    mine = pltpu.make_async_copy(half_of(core), held.at[core], own_sem)
    mine.start()
    pl.semaphore_wait(barrier, peers + 2)

    swap = remote(half_of(1 - core), held.at[core], swap_send, swap_recv, (c, chip + 1 - core))
    swap.start()

    @pl.loop(1, peers)
    def _(offset):
        exchange(offset, pieces, got, out_send, out_recv).start()

    got[c, core] = pieces[c, core]

    def turn(which):
        @pl.loop(0, CYC)
        def _(j):
            place = pl.ds(pl.multiple_of(j * half_orders, 8), half_orders)
            for tile in range(depth // LANES):
                wide[tile, place, :] = held[
                    which, j, :, tile * LANES : (tile + 1) * LANES
                ].astype(F32)

        @pl.loop(0, ring)
        def _(t):
            place = pl.ds(pl.multiple_of(which * LANES, LANES), LANES)
            for tile in range(depth // LANES):
                taken = [
                    wide[tile, pl.ds(TRI * t + i, CYC, stride=half_orders), :] for i in range(TRI)
                ]
                taken.append(jnp.zeros((LANES - TRI * CYC, LANES), F32))
                table[t, place, tile * LANES : (tile + 1) * LANES] = jnp.concatenate(
                    taken, axis=0
                ).astype(BF16)

    mine.wait()
    turn(core)
    swap.wait()
    turn(1 - core)

    @pl.loop(1, peers)
    def _(offset):
        exchange(offset, pieces, got, out_send, out_recv).wait()

    for g in range(cons):
        field = assignment[g]
        for s in range(2):
            mixed[(s * cons + g) * 16 : (s * cons + g + 1) * 16, :] = got[field, s].astype(F32)
    for t in range(ring):
        for s in range(2):
            for p in range(2):
                lines[t, p * cons : (p + 1) * cons, s * LANES : (s + 1) * LANES] = mixed[
                    pl.ds(s * cons * 16 + p * 8 + t, cons, stride=16), :
                ]

    lane = lax.broadcasted_iota(jnp.int32, (full, 2 * LANES), 1)
    lane = jnp.where(lane >= LANES, lane - LANES, lane)
    which = jnp.where(lane < CYC, 0, jnp.where(lane < 2 * CYC, 1, jnp.where(lane < TRI * CYC, 2, 3)))

    def analysed(t):
        x = lines[t]
        left = [jnp.where(which == i, x, 0.0) for i in range(TRI)]
        part[t] = jnp.dot(
            jnp.concatenate(left, axis=0).astype(BF16), table[t], preferred_element_type=F32
        ).astype(BF16)

    def block(i):
        return pl.ds(i * full, full)

    def piece(i, p):
        return pl.ds(i * full + p * cons, cons)

    ways = (1, -1)

    def sum_step(way, step, i):
        device = on_ring(ways[way])
        send, recv = sum_send.at[way, step, i], sum_recv.at[way, step, i]
        if step == 0:
            return remote(part.at[slot(far), piece(i, way)], first.at[way, i], send, recv, device)
        return remote(staged.at[way, step - 1, i], later.at[way, step - 1, i], send, recv, device)

    analysed(slot(far))
    for i in range(TRI):
        for way in range(2):
            sum_step(way, 0, i).start()
    for step in range(1, far):
        for way in range(2):
            analysed(slot(ways[way] * (far - step)))
        for i in range(TRI):
            for way in range(2):
                owner = slot(ways[way] * (far - step))
                sum_step(way, step - 1, i).wait_recv()
                if step == 1:
                    for p in range(2):
                        value = part[owner, piece(i, p), :]
                        if p == way:
                            value = (value.astype(F32) + first[way, i].astype(F32)).astype(BF16)
                        staged[way, 0, i, p * cons : (p + 1) * cons, :] = value
                else:
                    staged[way, step - 1, i] = (
                        part[owner, block(i), :].astype(F32) + later[way, step - 2, i].astype(F32)
                    ).astype(BF16)
                sum_step(way, step, i).start()
    analysed(z)

    def pair_step(i):
        return remote(sent.at[i], other.at[i], pair_send.at[i], pair_recv.at[i], across)

    for i in range(TRI):
        for way in range(2):
            sum_step(way, far - 1, i).wait_recv()
        sent[i] = (
            part[z, block(i), :].astype(F32)
            + later[0, far - 2, i].astype(F32)
            + later[1, far - 2, i].astype(F32)
        ).astype(BF16)
        pair_step(i).start()

    def all_step(way, step, i):
        place = piece(i, way) if step == far - 1 else block(i)
        ref = coef.at[slot(-ways[way] * step), place]
        return remote(
            ref, ref, all_send.at[way, step, i], all_recv.at[way, step, i], on_ring(ways[way])
        )

    def all_arrival(way, step, i):
        place = piece(i, way) if step == far - 1 else block(i)
        ref = coef.at[slot(-ways[way] * (step + 1)), place]
        return remote(
            ref, ref, all_send.at[way, step, i], all_recv.at[way, step, i], on_ring(ways[way])
        )

    scale = love[...]
    for i in range(TRI):
        pair_step(i).wait_recv()
        coef[z, block(i), :] = (
            (sent[i].astype(F32) + other[i].astype(F32)) * scale
        ).astype(BF16)
        for way in range(2):
            all_step(way, 0, i).start()

    def synthesised(t):
        got_all = lax.dot_general(
            coef[t], table[t], (((1,), (1,)), ((), ())), preferred_element_type=F32
        )
        chosen = jnp.where(
            which == 0, got_all[:full], jnp.where(which == 1, got_all[full : 2 * full], got_all[2 * full :])
        )
        order = which + (TRI * t + core * half_orders + c * 2 * half_orders)
        chosen = chosen * jnp.where(order == 0, 1.0, 2.0).astype(F32)
        for s in range(2):
            place = pl.ds(pl.multiple_of(s * ring * full + t * full, 8), full)
            rows[place, :] = chosen[:, s * LANES : (s + 1) * LANES]

    for step in range(1, far):
        for i in range(TRI):
            for way in range(2):
                all_arrival(way, step - 1, i).wait_recv()
                all_step(way, step, i).start()
        if step == 1:
            synthesised(z)
        else:
            for way in ways:
                synthesised(slot(-way * (step - 1)))
    for way in ways:
        synthesised(slot(-way * (far - 1)))
    for i in range(TRI):
        for way in range(2):
            all_arrival(way, far - 1, i).wait_recv()
    synthesised(slot(far))

    for g in range(cons):
        for s in range(2):
            both = [
                rows[pl.ds(s * ring * full + p * cons + g, ring, stride=full), :] for p in range(2)
            ]
            back[g, s] = jnp.concatenate(both, axis=0).astype(BF16)

    @pl.loop(1, peers)
    def _(offset):
        exchange(offset, back, returned, back_send, back_recv).start()

    returned[c, core] = back[c, core]

    for i in range(TRI):
        pair_step(i).wait_send()
        for way in range(2):
            for step in range(far):
                sum_step(way, step, i).wait_send()
                all_step(way, step, i).wait_send()

    @pl.loop(1, peers)
    def _(offset):
        exchange(offset, back, returned, back_send, back_recv).wait()

    out[...] = returned[...]


def middle(pieces, legendre, love, assignment):
    cons = pieces.shape[0]
    depth = legendre.shape[2]
    ring = 8
    far = ring // 2
    full = 2 * cons
    dma = pltpu.SemaphoreType.DMA
    vmem = pltpu.VMEM
    return pl.pallas_call(
        functools.partial(middle_kernel, ring, cons),
        out_shape=jax.ShapeDtypeStruct(pieces.shape, BF16),
        in_specs=[
            pl.BlockSpec(memory_space=pltpu.VMEM),
            pl.BlockSpec(memory_space=pl.ANY),
            pl.BlockSpec(memory_space=pltpu.VMEM),
            pl.BlockSpec(memory_space=pltpu.SMEM),
        ],
        out_specs=pl.BlockSpec(memory_space=pltpu.VMEM),
        scratch_shapes=[
            vmem((2, CYC, TRI * ring, depth), BF16),
            vmem((depth // LANES, CYC * TRI * ring, LANES), F32),
            vmem((ring, 2 * LANES, depth), BF16),
            vmem(pieces.shape, BF16),
            vmem((2 * cons * 16, LANES), F32),
            vmem((ring, full, 2 * LANES), F32),
            vmem((ring, TRI * full, depth), BF16),
            vmem((2, TRI, cons, depth), BF16),
            vmem((2, far - 1, TRI, full, depth), BF16),
            vmem((2, far - 1, TRI, full, depth), BF16),
            vmem((TRI, full, depth), BF16),
            vmem((TRI, full, depth), BF16),
            vmem((ring, TRI * full, depth), BF16),
            vmem((2 * ring * full, LANES), F32),
            vmem(pieces.shape, BF16),
            vmem(pieces.shape, BF16),
            dma,
            dma,
            dma,
            dma((2 * cons,)),
            dma((2 * cons,)),
            dma((2, far, TRI)),
            dma((2, far, TRI)),
            dma((TRI,)),
            dma((TRI,)),
            dma((2, far, TRI)),
            dma((2, far, TRI)),
            dma((2 * cons,)),
            dma((2 * cons,)),
        ],
        compiler_params=pltpu.CompilerParams(
            collective_id=KERNEL_ID, has_side_effects=True, vmem_limit_bytes=50 * 2**20
        ),
        name="middle",
    )(pieces, legendre, love, assignment)


def local(elevation, legendre, cycle_weight, love_factor, assignment):
    cons = lax.axis_size("cons")
    lane_weight = jnp.pad(jnp.tile(cycle_weight, TRI), (0, LANES - TRI * CYC))[None, :]
    pieces = forward(elevation, lane_weight, cons)
    returned = middle(pieces, legendre, love_factor[None, :], assignment)
    return inverse(returned, elevation.shape[-1])


def solution(mesh):
    placed = (P("cons", "blk", None), P("blk", "cons", None), P("blk"), P(), P())
    return jax.shard_map(
        local, mesh=mesh, in_specs=placed, out_specs=P("cons", "blk", None), check_vma=False
    )
```

```python
import functools
import math
import numpy as np
import jax
import jax.numpy as jnp
from jax import lax
from jax.experimental import pallas as pl
from jax.experimental.pallas import tpu as pltpu
from jax.sharding import PartitionSpec as P

RADIX = 48
LANES = 128
CYC = 40
TRI = 3


def by_phase(value, turn):
    re, im = value
    cos, sin = math.cos(2 * math.pi * turn), math.sin(2 * math.pi * turn)
    cos = 0.0 if abs(cos) < 1e-12 else cos
    sin = 0.0 if abs(sin) < 1e-12 else sin

    def scaled(array, factor):
        if array is None or factor == 0.0:
            return None
        if abs(factor - 1.0) < 1e-12:
            return array
        if abs(factor + 1.0) < 1e-12:
            return -array
        return array * np.float32(factor)

    return (
        added(scaled(re, cos), scaled(im, -sin)),
        added(scaled(re, sin), scaled(im, cos)),
    )


def added(a, b):
    if a is None:
        return b
    return a if b is None else a + b


def plus(a, b):
    return added(a[0], b[0]), added(a[1], b[1])


def conj(a):
    return a[0], None if a[1] is None else -a[1]


def at(half, index, length):
    index %= length
    return half[index] if 2 * index <= length else conj(half[length - index])


def factor_of(length):
    return 4 if length % 4 == 0 else (3 if length % 3 == 0 else 2)


def real_fft(values):
    n = len(values)
    if n == 1:
        return [(values[0], None)]
    p = factor_of(n)
    parts = [real_fft(values[i::p]) for i in range(p)]
    out = []
    for k in range(n // 2 + 1):
        total = at(parts[0], k, n // p)
        for i in range(1, p):
            total = plus(total, by_phase(at(parts[i], k, n // p), -i * k / n))
        out.append(total)
    return out


def real_inverse(half, n):
    if n == 1:
        return [half[0][0]]
    p = factor_of(n)
    short = n // p
    out = [None] * n
    for a in range(p):
        folded = []
        for r in range(short // 2 + 1):
            total = (None, None)
            for s in range(p):
                index = r + s * short
                total = plus(total, by_phase(at(half, index, n), index * a / n))
            if r == 0 or 2 * r == short:
                total = (total[0], None)
            folded.append(total)
        for kk, value in enumerate(real_inverse(folded, short)):
            out[p * kk + a] = value
    return out


def phase_tables(period):
    lane = np.arange(LANES)
    turn = np.arange(RADIX)[:, None] * lane[None, :] / period
    twiddle = np.stack([np.cos(2 * np.pi * turn), np.sin(2 * np.pi * turn)], 1)
    q = np.arange(period // RADIX // 8)[:, None] * lane[None, :] / LANES
    cos, sin = np.cos(2 * np.pi * q), np.sin(2 * np.pi * q)
    basis = np.concatenate([np.concatenate([cos, sin], 1), np.concatenate([-sin, cos], 1)], 0)
    return twiddle.reshape(2 * RADIX, LANES).astype(np.float32), basis.astype(jnp.bfloat16)


def transformed(x_ref, weight, twiddle_ref, basis_ref, out_ref, wide, mixed, rows):
    cons = out_ref.shape[0]
    for triple in range(RADIX // TRI):
        mixed[triple * LANES + TRI * CYC : (triple + 1) * LANES, :] = jnp.zeros(
            (LANES - TRI * CYC, 2 * LANES), jnp.float32
        )
    wide[...] = x_ref[...].reshape(wide.shape).astype(jnp.float32)

    @pl.loop(0, CYC // 8)
    def _(group):
        lines = pl.ds(pl.multiple_of(group * 8, 8), 8)
        half = real_fft([wide[lines, k * LANES : (k + 1) * LANES] for k in range(RADIX)])
        for r in range(RADIX):
            re, im = at(half, r, RADIX)
            cos, sin = twiddle_ref[2 * r : 2 * r + 1, :], twiddle_ref[2 * r + 1 : 2 * r + 2, :]
            if im is None:
                new_re, new_im = re * cos, -re * sin
            else:
                new_re, new_im = re * cos + im * sin, im * cos - re * sin
            start = (r // TRI) * LANES + (r % TRI) * CYC
            place = pl.ds(pl.multiple_of(start + group * 8, 8), 8)
            mixed[place, 0:LANES] = new_re
            mixed[place, LANES:] = new_im

    for triple in range(RADIX // TRI):
        block = mixed[triple * LANES : (triple + 1) * LANES, :].astype(jnp.bfloat16)
        got = lax.dot_general(
            basis_ref[...], block, (((1,), (1,)), ((), ())), preferred_element_type=jnp.float32
        )
        rows[triple * 2 * cons : (triple + 1) * 2 * cons, :] = got * weight
    for c in range(cons):
        for h in range(2):
            both = [
                rows[pl.ds(h * 16 * cons + p * cons + c, 8, stride=2 * cons), :] for p in range(2)
            ]
            out_ref[c, h] = jnp.concatenate(both, axis=0).astype(jnp.bfloat16)


def inverse_kernel(z_ref, twiddle_ref, basis_ref, out_ref, rows, mixed):
    cons = z_ref.shape[0]
    for c in range(cons):
        for h in range(2):
            place = (2 * c + h) * 16
            rows[place : place + 16, :] = z_ref[c, h].astype(jnp.float32)
    for triple in range(RADIX // TRI):
        h, t = divmod(triple, 8)
        both = [rows[pl.ds(h * 16 + p * 8 + t, cons, stride=32), :] for p in range(2)]
        lines = jnp.concatenate(both, axis=0).T.astype(jnp.bfloat16)
        mixed[triple * LANES : (triple + 1) * LANES, :] = jnp.dot(
            lines, basis_ref[...], preferred_element_type=jnp.float32
        )

    @pl.loop(0, CYC // 8)
    def _(group):
        turned = []
        for r in range(RADIX):
            start = (r // TRI) * LANES + (r % TRI) * CYC
            place = pl.ds(pl.multiple_of(start + group * 8, 8), 8)
            re, im = mixed[place, 0:LANES], mixed[place, LANES:]
            cos, sin = twiddle_ref[2 * r : 2 * r + 1, :], twiddle_ref[2 * r + 1 : 2 * r + 2, :]
            turned.append((re * cos - im * sin, re * sin + im * cos))
        middle = RADIX // 2
        half = [(turned[0][0], None)]
        for r in range(1, middle):
            pair = plus(turned[r], conj(turned[RADIX - r]))
            half.append((pair[0] * np.float32(0.5), pair[1] * np.float32(0.5)))
        half.append((turned[middle][0], None))
        lines = pl.ds(pl.multiple_of(group * 8, 8), 8)
        for k, value in enumerate(real_inverse(half, RADIX)):
            out_ref[0, lines, k * LANES : (k + 1) * LANES] = value


def inverse(pieces, period):
    cons = pieces.shape[0]
    twiddle, basis = phase_tables(period)
    return pl.pallas_call(
        inverse_kernel,
        out_shape=jax.ShapeDtypeStruct((1, CYC, period), jnp.float32),
        in_specs=[pl.BlockSpec(memory_space=pltpu.VMEM)] * 3,
        out_specs=pl.BlockSpec(memory_space=pltpu.VMEM),
        scratch_shapes=[
            pltpu.VMEM((2 * cons * 16, LANES), jnp.float32),
            pltpu.VMEM((RADIX // TRI * LANES, 2 * LANES), jnp.float32),
        ],
        compiler_params=pltpu.CompilerParams(vmem_limit_bytes=10 * 2**20),
        name="inverse",
    )(pieces, jnp.asarray(twiddle), jnp.asarray(basis))


MESH = pl.DeviceIdType.MESH
F32 = jnp.float32
BF16 = jnp.bfloat16
KERNEL_ID = 0


def middle_kernel(
    ring, cons, elevation, legendre, cycle_weight, love_factor, assigned, twiddles, bases, out,
    height, weights, love, assignment, twiddle, basis, pieces, tall, spun, spread,
    held, wide, table, got, mixed, lines, part, first, later, staged, sent, other, coef,
    rows, back, returned,
    load_sem, own_sem, swap_send, swap_recv, out_send, out_recv, sum_send, sum_recv, pair_send, pair_recv,
    all_send, all_recv, back_send, back_recv,
):
    c, b = lax.axis_index("cons"), lax.axis_index("blk")
    core = lax.rem(b, 2)
    z = lax.rem(b // 2, ring)
    line = b // (2 * ring)
    chip = b - core
    me = 2 * c + core
    peers = 2 * cons
    far = ring // 2
    depth = legendre.shape[2]
    half_orders = TRI * ring
    full = 2 * cons
    barrier = pltpu.get_barrier_semaphore()

    def slot(offset):
        return lax.rem(z + offset + ring, ring)

    def on_ring(offset):
        return (c, line * 2 * ring + slot(offset) * 2 + core)

    def peer(offset):
        index = lax.rem(me + offset, peers)
        return index // 2, lax.rem(index, 2)

    def remote(source, target, send, recv, device):
        return pltpu.make_async_remote_copy(
            src_ref=source,
            dst_ref=target,
            send_sem=send,
            recv_sem=recv,
            device_id=device,
            device_id_type=MESH,
        )

    def exchange(offset, source, landing, send, recv):
        there = peer(offset)
        return remote(
            source.at[there[0], there[1]],
            landing.at[c, core],
            send.at[offset],
            recv.at[offset],
            (there[0], chip + there[1]),
        )

    across = (c, (1 - line) * 2 * ring + z * 2 + core)

    @pl.loop(1, peers)
    def _(offset):
        there = peer(offset)
        pl.semaphore_signal(
            barrier, inc=1, device_id=(there[0], chip + there[1]), device_id_type=MESH
        )

    for target in (on_ring(1), on_ring(-1), across):
        pl.semaphore_signal(barrier, inc=1, device_id=target, device_id_type=MESH)

    def half_of(which):
        return legendre.at[:, pl.ds(pl.multiple_of(which * half_orders, 8), half_orders), :]

    mine = pltpu.make_async_copy(half_of(core), held.at[core], own_sem)
    mine.start()
    pairs = (
        (elevation, height),
        (twiddles, twiddle),
        (bases, basis),
        (cycle_weight, weights),
        (assigned, assignment),
        (love_factor, love),
    )
    loads = [
        pltpu.make_async_copy(source, target, load_sem.at[i])
        for i, (source, target) in enumerate(pairs)
    ]
    for load in loads:
        load.start()
    for load in loads:
        load.wait()

    with jax.named_scope("fft"):
        lane_of = lax.broadcasted_iota(jnp.int32, (1, LANES), 1)
        day = lane_of - jnp.where(lane_of < CYC, 0, jnp.where(lane_of < 2 * CYC, CYC, 2 * CYC))
        weight = jnp.zeros((1, LANES), F32)
        for j in range(CYC):
            weight = jnp.where(day == j, weights[j], weight)
        transformed(height, weight, twiddle, basis, pieces, tall, spun, spread)

    with jax.named_scope("barrier"):
        pl.semaphore_wait(barrier, peers + 2)

    swap = remote(half_of(1 - core), held.at[core], swap_send, swap_recv, (c, chip + 1 - core))
    swap.start()

    @pl.loop(1, peers)
    def _(offset):
        exchange(offset, pieces, got, out_send, out_recv).start()

    got[c, core] = pieces[c, core]

    def turn(which):
        @pl.loop(0, CYC)
        def _(j):
            place = pl.ds(pl.multiple_of(j * half_orders, 8), half_orders)
            for tile in range(depth // LANES):
                wide[tile, place, :] = held[
                    which, j, :, tile * LANES : (tile + 1) * LANES
                ].astype(F32)

        @pl.loop(0, ring)
        def _(t):
            place = pl.ds(pl.multiple_of(which * LANES, LANES), LANES)
            for tile in range(depth // LANES):
                taken = [
                    wide[tile, pl.ds(TRI * t + i, CYC, stride=half_orders), :] for i in range(TRI)
                ]
                taken.append(jnp.zeros((LANES - TRI * CYC, LANES), F32))
                table[t, place, tile * LANES : (tile + 1) * LANES] = jnp.concatenate(
                    taken, axis=0
                ).astype(BF16)

    with jax.named_scope("turn_own"):
        mine.wait()
        turn(core)
    with jax.named_scope("swap_wait"):
        swap.wait()
    with jax.named_scope("turn_other"):
        turn(1 - core)

    with jax.named_scope("wait_out"):

        @pl.loop(1, peers)
        def _(offset):
            exchange(offset, pieces, got, out_send, out_recv).wait()

    with jax.named_scope("lines"):
        for g in range(cons):
            field = assignment[g]
            for s in range(2):
                mixed[(s * cons + g) * 16 : (s * cons + g + 1) * 16, :] = got[field, s].astype(F32)
        for t in range(ring):
            for s in range(2):
                for p in range(2):
                    lines[t, p * cons : (p + 1) * cons, s * LANES : (s + 1) * LANES] = mixed[
                        pl.ds(s * cons * 16 + p * 8 + t, cons, stride=16), :
                    ]

    lane = lax.broadcasted_iota(jnp.int32, (full, 2 * LANES), 1)
    lane = jnp.where(lane >= LANES, lane - LANES, lane)
    which = jnp.where(lane < CYC, 0, jnp.where(lane < 2 * CYC, 1, jnp.where(lane < TRI * CYC, 2, 3)))

    def analysed(t):
        x = lines[t]
        left = [jnp.where(which == i, x, 0.0) for i in range(TRI)]
        part[t] = jnp.dot(
            jnp.concatenate(left, axis=0).astype(BF16), table[t], preferred_element_type=F32
        ).astype(BF16)

    def block(i):
        return pl.ds(i * full, full)

    def piece(i, p):
        return pl.ds(i * full + p * cons, cons)

    ways = (1, -1)

    def sum_step(way, step, i):
        device = on_ring(ways[way])
        send, recv = sum_send.at[way, step, i], sum_recv.at[way, step, i]
        if step == 0:
            return remote(part.at[slot(far), piece(i, way)], first.at[way, i], send, recv, device)
        return remote(staged.at[way, step - 1, i], later.at[way, step - 1, i], send, recv, device)

    with jax.named_scope("first_part"):
        analysed(slot(far))
        for i in range(TRI):
            for way in range(2):
                sum_step(way, 0, i).start()
    for step in range(1, far):
      with jax.named_scope(f"part#s={step}"):
        for way in range(2):
            analysed(slot(ways[way] * (far - step)))
      with jax.named_scope(f"sum#s={step}"):
        for i in range(TRI):
            for way in range(2):
                owner = slot(ways[way] * (far - step))
                sum_step(way, step - 1, i).wait_recv()
                if step == 1:
                    for p in range(2):
                        value = part[owner, piece(i, p), :]
                        if p == way:
                            value = (value.astype(F32) + first[way, i].astype(F32)).astype(BF16)
                        staged[way, 0, i, p * cons : (p + 1) * cons, :] = value
                else:
                    staged[way, step - 1, i] = (
                        part[owner, block(i), :].astype(F32) + later[way, step - 2, i].astype(F32)
                    ).astype(BF16)
                sum_step(way, step, i).start()
    analysed(z)

    def pair_step(i):
        return remote(sent.at[i], other.at[i], pair_send.at[i], pair_recv.at[i], across)

    with jax.named_scope("last_sum"):
        for i in range(TRI):
            for way in range(2):
                sum_step(way, far - 1, i).wait_recv()
            sent[i] = (
                part[z, block(i), :].astype(F32)
                + later[0, far - 2, i].astype(F32)
                + later[1, far - 2, i].astype(F32)
            ).astype(BF16)
            pair_step(i).start()

    def all_step(way, step, i):
        place = piece(i, way) if step == far - 1 else block(i)
        ref = coef.at[slot(-ways[way] * step), place]
        return remote(
            ref, ref, all_send.at[way, step, i], all_recv.at[way, step, i], on_ring(ways[way])
        )

    def all_arrival(way, step, i):
        place = piece(i, way) if step == far - 1 else block(i)
        ref = coef.at[slot(-ways[way] * (step + 1)), place]
        return remote(
            ref, ref, all_send.at[way, step, i], all_recv.at[way, step, i], on_ring(ways[way])
        )

    scale = love[...].reshape(1, depth)
    with jax.named_scope("pair"):
        for i in range(TRI):
            pair_step(i).wait_recv()
            coef[z, block(i), :] = (
                (sent[i].astype(F32) + other[i].astype(F32)) * scale
            ).astype(BF16)
            for way in range(2):
                all_step(way, 0, i).start()

    def synthesised(t):
        got_all = lax.dot_general(
            coef[t], table[t], (((1,), (1,)), ((), ())), preferred_element_type=F32
        )
        chosen = jnp.where(
            which == 0, got_all[:full], jnp.where(which == 1, got_all[full : 2 * full], got_all[2 * full :])
        )
        order = which + (TRI * t + core * half_orders + c * 2 * half_orders)
        chosen = chosen * jnp.where(order == 0, 1.0, 2.0).astype(F32)
        for s in range(2):
            place = pl.ds(pl.multiple_of(s * ring * full + t * full, 8), full)
            rows[place, :] = chosen[:, s * LANES : (s + 1) * LANES]

    for step in range(1, far):
      with jax.named_scope(f"all#s={step}"):
        for i in range(TRI):
            for way in range(2):
                all_arrival(way, step - 1, i).wait_recv()
                all_step(way, step, i).start()
      with jax.named_scope(f"synth#s={step}"):
        if step == 1:
            synthesised(z)
        else:
            for way in ways:
                synthesised(slot(-way * (step - 1)))
    with jax.named_scope("synth_last"):
        for way in ways:
            synthesised(slot(-way * (far - 1)))
    with jax.named_scope("all_last"):
        for i in range(TRI):
            for way in range(2):
                all_arrival(way, far - 1, i).wait_recv()
    with jax.named_scope("synth_far"):
        synthesised(slot(far))

    with jax.named_scope("back"):
        for g in range(cons):
            for s in range(2):
                both = [
                    rows[pl.ds(s * ring * full + p * cons + g, ring, stride=full), :] for p in range(2)
                ]
                back[g, s] = jnp.concatenate(both, axis=0).astype(BF16)

    @pl.loop(1, peers)
    def _(offset):
        exchange(offset, back, returned, back_send, back_recv).start()

    returned[c, core] = back[c, core]

    for i in range(TRI):
        pair_step(i).wait_send()
        for way in range(2):
            for step in range(far):
                sum_step(way, step, i).wait_send()
                all_step(way, step, i).wait_send()

    with jax.named_scope("wait_back"):

        @pl.loop(1, peers)
        def _(offset):
            exchange(offset, back, returned, back_send, back_recv).wait()

    out[...] = returned[...]


def middle(elevation, legendre, cycle_weight, love_factor, assignment):
    cons = lax.axis_size("cons")
    period = elevation.shape[-1]
    depth = legendre.shape[2]
    ring = 8
    far = ring // 2
    full = 2 * cons
    dma = pltpu.SemaphoreType.DMA
    vmem = pltpu.VMEM
    twiddle, basis = phase_tables(period)
    pieces = (cons, 2, 16, LANES)
    return pl.pallas_call(
        functools.partial(middle_kernel, ring, cons),
        out_shape=jax.ShapeDtypeStruct(pieces, BF16),
        in_specs=[pl.BlockSpec(memory_space=pltpu.HBM)] * 7,
        out_specs=pl.BlockSpec(memory_space=pltpu.VMEM),
        scratch_shapes=[
            vmem((1, CYC, period), BF16),
            pltpu.SMEM((CYC,), F32),
            vmem((depth,), F32),
            pltpu.SMEM((cons,), jnp.int32),
            vmem(twiddle.shape, F32),
            vmem(basis.shape, BF16),
            vmem(pieces, BF16),
            vmem((CYC, period), F32),
            vmem((RADIX // TRI * LANES, 2 * LANES), F32),
            vmem((RADIX // TRI * full, LANES), F32),
            vmem((2, CYC, TRI * ring, depth), BF16),
            vmem((depth // LANES, CYC * TRI * ring, LANES), F32),
            vmem((ring, 2 * LANES, depth), BF16),
            vmem(pieces, BF16),
            vmem((2 * cons * 16, LANES), F32),
            vmem((ring, full, 2 * LANES), F32),
            vmem((ring, TRI * full, depth), BF16),
            vmem((2, TRI, cons, depth), BF16),
            vmem((2, far - 1, TRI, full, depth), BF16),
            vmem((2, far - 1, TRI, full, depth), BF16),
            vmem((TRI, full, depth), BF16),
            vmem((TRI, full, depth), BF16),
            vmem((ring, TRI * full, depth), BF16),
            vmem((2 * ring * full, LANES), F32),
            vmem(pieces, BF16),
            vmem(pieces, BF16),
            dma((6,)),
            dma,
            dma,
            dma,
            dma((2 * cons,)),
            dma((2 * cons,)),
            dma((2, far, TRI)),
            dma((2, far, TRI)),
            dma((TRI,)),
            dma((TRI,)),
            dma((2, far, TRI)),
            dma((2, far, TRI)),
            dma((2 * cons,)),
            dma((2 * cons,)),
        ],
        compiler_params=pltpu.CompilerParams(
            collective_id=KERNEL_ID, has_side_effects=True, vmem_limit_bytes=67_000_000
        ),
        name="middle",
    )(
        elevation,
        legendre,
        cycle_weight,
        love_factor,
        assignment,
        jnp.asarray(twiddle),
        jnp.asarray(basis),
    )


def local(elevation, legendre, cycle_weight, love_factor, assignment):
    returned = middle(elevation, legendre, cycle_weight, love_factor, assignment)
    return inverse(returned, elevation.shape[-1])


def solution(mesh):
    placed = (P("cons", "blk", None), P("blk", "cons", None), P("blk"), P(), P())
    return jax.shard_map(
        local, mesh=mesh, in_specs=placed, out_specs=P("cons", "blk", None), check_vma=False
    )
```

```python
import functools
import math
import numpy as np
import jax
import jax.numpy as jnp
from jax import lax
from jax.experimental import pallas as pl
from jax.experimental.pallas import tpu as pltpu
from jax.sharding import PartitionSpec as P

RADIX = 48
LANES = 128
CYC = 40
TRI = 3


def by_phase(value, turn):
    re, im = value
    cos, sin = math.cos(2 * math.pi * turn), math.sin(2 * math.pi * turn)
    cos = 0.0 if abs(cos) < 1e-12 else cos
    sin = 0.0 if abs(sin) < 1e-12 else sin

    def scaled(array, factor):
        if array is None or factor == 0.0:
            return None
        if abs(factor - 1.0) < 1e-12:
            return array
        if abs(factor + 1.0) < 1e-12:
            return -array
        return array * np.float32(factor)

    return (
        added(scaled(re, cos), scaled(im, -sin)),
        added(scaled(re, sin), scaled(im, cos)),
    )


def added(a, b):
    if a is None:
        return b
    return a if b is None else a + b


def plus(a, b):
    return added(a[0], b[0]), added(a[1], b[1])


def conj(a):
    return a[0], None if a[1] is None else -a[1]


def at(half, index, length):
    index %= length
    return half[index] if 2 * index <= length else conj(half[length - index])


def factor_of(length):
    return 4 if length % 4 == 0 else (3 if length % 3 == 0 else 2)


def real_fft(values):
    n = len(values)
    if n == 1:
        return [(values[0], None)]
    p = factor_of(n)
    parts = [real_fft(values[i::p]) for i in range(p)]
    out = []
    for k in range(n // 2 + 1):
        total = at(parts[0], k, n // p)
        for i in range(1, p):
            total = plus(total, by_phase(at(parts[i], k, n // p), -i * k / n))
        out.append(total)
    return out


def real_inverse(half, n):
    if n == 1:
        return [half[0][0]]
    p = factor_of(n)
    short = n // p
    out = [None] * n
    for a in range(p):
        folded = []
        for r in range(short // 2 + 1):
            total = (None, None)
            for s in range(p):
                index = r + s * short
                total = plus(total, by_phase(at(half, index, n), index * a / n))
            if r == 0 or 2 * r == short:
                total = (total[0], None)
            folded.append(total)
        for kk, value in enumerate(real_inverse(folded, short)):
            out[p * kk + a] = value
    return out


def phase_tables(period):
    lane = np.arange(LANES)
    turn = np.arange(RADIX)[:, None] * lane[None, :] / period
    twiddle = np.stack([np.cos(2 * np.pi * turn), np.sin(2 * np.pi * turn)], 1)
    q = np.arange(period // RADIX // 8)[:, None] * lane[None, :] / LANES
    cos, sin = np.cos(2 * np.pi * q), np.sin(2 * np.pi * q)
    basis = np.concatenate([np.concatenate([cos, sin], 1), np.concatenate([-sin, cos], 1)], 0)
    return twiddle.reshape(2 * RADIX, LANES).astype(np.float32), basis.astype(jnp.bfloat16)


def transformed(x_ref, weight, twiddle_ref, basis_ref, out_ref, mixed, rows):
    cons = out_ref.shape[0]
    for triple in range(RADIX // TRI):
        mixed[triple * LANES + TRI * CYC : (triple + 1) * LANES, :] = jnp.zeros(
            (LANES - TRI * CYC, 2 * LANES), jnp.float32
        )

    @pl.loop(0, CYC // 8)
    def _(group):
        lines = pl.ds(pl.multiple_of(group * 8, 8), 8)
        half = real_fft(
            [
                x_ref[0, lines, k * LANES : (k + 1) * LANES].astype(jnp.float32)
                for k in range(RADIX)
            ]
        )
        for r in range(RADIX):
            re, im = at(half, r, RADIX)
            cos, sin = twiddle_ref[2 * r : 2 * r + 1, :], twiddle_ref[2 * r + 1 : 2 * r + 2, :]
            if im is None:
                new_re, new_im = re * cos, -re * sin
            else:
                new_re, new_im = re * cos + im * sin, im * cos - re * sin
            start = (r // TRI) * LANES + (r % TRI) * CYC
            place = pl.ds(pl.multiple_of(start + group * 8, 8), 8)
            mixed[place, 0:LANES] = new_re
            mixed[place, LANES:] = new_im

    for triple in range(RADIX // TRI):
        block = mixed[triple * LANES : (triple + 1) * LANES, :].astype(jnp.bfloat16)
        got = lax.dot_general(
            basis_ref[...], block, (((1,), (1,)), ((), ())), preferred_element_type=jnp.float32
        )
        rows[triple * 2 * cons : (triple + 1) * 2 * cons, :] = got * weight
    for c in range(cons):
        for h in range(2):
            both = [
                rows[pl.ds(h * 16 * cons + p * cons + c, 8, stride=2 * cons), :] for p in range(2)
            ]
            out_ref[c, h] = jnp.concatenate(both, axis=0).astype(jnp.bfloat16)


def inverse_kernel(
    z_hbm, twiddle_hbm, basis_hbm, out_hbm, z_ref, twiddle_ref, basis_ref, rows, mixed, done, sems, out_sems
):
    pairs = ((z_hbm, z_ref), (twiddle_hbm, twiddle_ref), (basis_hbm, basis_ref))
    loads = [
        pltpu.make_async_copy(source, target, sems.at[i])
        for i, (source, target) in enumerate(pairs)
    ]
    for load in loads:
        load.start()
    for load in loads:
        load.wait()
    cons = z_ref.shape[0]
    for c in range(cons):
        for h in range(2):
            place = (2 * c + h) * 16
            rows[place : place + 16, :] = z_ref[c, h].astype(jnp.float32)
    for triple in range(RADIX // TRI):
        h, t = divmod(triple, 8)
        both = [rows[pl.ds(h * 16 + p * 8 + t, cons, stride=32), :] for p in range(2)]
        lines = jnp.concatenate(both, axis=0).T.astype(jnp.bfloat16)
        mixed[triple * LANES : (triple + 1) * LANES, :] = jnp.dot(
            lines, basis_ref[...], preferred_element_type=jnp.float32
        )

    def leave(group):
        lines = pl.ds(pl.multiple_of(group * 8, 8), 8)
        return pltpu.make_async_copy(done.at[group], out_hbm.at[0, lines], out_sems.at[group])

    @pl.loop(0, CYC // 8)
    def _(group):
        turned = []
        for r in range(RADIX):
            start = (r // TRI) * LANES + (r % TRI) * CYC
            place = pl.ds(pl.multiple_of(start + group * 8, 8), 8)
            re, im = mixed[place, 0:LANES], mixed[place, LANES:]
            cos, sin = twiddle_ref[2 * r : 2 * r + 1, :], twiddle_ref[2 * r + 1 : 2 * r + 2, :]
            turned.append((re * cos - im * sin, re * sin + im * cos))
        middle = RADIX // 2
        half = [(turned[0][0], None)]
        for r in range(1, middle):
            pair = plus(turned[r], conj(turned[RADIX - r]))
            half.append((pair[0] * np.float32(0.5), pair[1] * np.float32(0.5)))
        half.append((turned[middle][0], None))
        for k, value in enumerate(real_inverse(half, RADIX)):
            done[group, :, k * LANES : (k + 1) * LANES] = value
        leave(group).start()

    @pl.loop(0, CYC // 8)
    def _(group):
        leave(group).wait()


def inverse(pieces, period):
    cons = pieces.shape[0]
    twiddle, basis = phase_tables(period)
    return pl.pallas_call(
        inverse_kernel,
        out_shape=jax.ShapeDtypeStruct((1, CYC, period), jnp.float32),
        in_specs=[pl.BlockSpec(memory_space=pltpu.HBM)] * 3,
        out_specs=pl.BlockSpec(memory_space=pltpu.HBM),
        scratch_shapes=[
            pltpu.VMEM(pieces.shape, jnp.bfloat16),
            pltpu.VMEM(twiddle.shape, jnp.float32),
            pltpu.VMEM(basis.shape, jnp.bfloat16),
            pltpu.VMEM((2 * cons * 16, LANES), jnp.float32),
            pltpu.VMEM((RADIX // TRI * LANES, 2 * LANES), jnp.float32),
            pltpu.VMEM((CYC // 8, 8, period), jnp.float32),
            pltpu.SemaphoreType.DMA((3,)),
            pltpu.SemaphoreType.DMA((CYC // 8,)),
        ],
        compiler_params=pltpu.CompilerParams(vmem_limit_bytes=67_000_000),
        name="inverse",
    )(pieces, jnp.asarray(twiddle), jnp.asarray(basis))


MESH = pl.DeviceIdType.MESH
F32 = jnp.float32
BF16 = jnp.bfloat16
KERNEL_ID = 0


def middle_kernel(
    ring, cons, elevation, legendre, cycle_weight, love_factor, assigned, twiddles, bases, out,
    height, weights, love, assignment, twiddle, basis, pieces, spun, spread,
    held, wide, table, got, mixed, lines, part, first, later, staged, sent, other, coef,
    rows, back,
    load_sem, own_sem, swap_send, swap_recv, out_send, out_recv, sum_send, sum_recv, pair_send, pair_recv,
    all_send, all_recv, back_send, back_recv,
):
    c, b = lax.axis_index("cons"), lax.axis_index("blk")
    core = lax.rem(b, 2)
    z = lax.rem(b // 2, ring)
    line = b // (2 * ring)
    chip = b - core
    me = 2 * c + core
    peers = 2 * cons
    far = ring // 2
    depth = legendre.shape[2]
    half_orders = TRI * ring
    full = 2 * cons
    barrier = pltpu.get_barrier_semaphore()

    def slot(offset):
        return lax.rem(z + offset + ring, ring)

    def on_ring(offset):
        return (c, line * 2 * ring + slot(offset) * 2 + core)

    def peer(offset):
        index = lax.rem(me + offset, peers)
        return index // 2, lax.rem(index, 2)

    def outward(turn):
        odd = lax.rem(turn, 2)
        return peers // 2 + ((turn + 1) // 2) * (2 * odd - 1)

    def remote(source, target, send, recv, device):
        return pltpu.make_async_remote_copy(
            src_ref=source,
            dst_ref=target,
            send_sem=send,
            recv_sem=recv,
            device_id=device,
            device_id_type=MESH,
        )

    def exchange(offset, source, landing, send, recv):
        there = peer(offset)
        return remote(
            source.at[there[0], there[1]],
            landing.at[c, core],
            send.at[offset],
            recv.at[offset],
            (there[0], chip + there[1]),
        )

    across = (c, (1 - line) * 2 * ring + z * 2 + core)

    def half_of(which):
        return legendre.at[:, pl.ds(pl.multiple_of(which * half_orders, 8), half_orders), :]

    mine = pltpu.make_async_copy(half_of(core), held.at[core], own_sem)
    pairs = (
        (elevation, height),
        (twiddles, twiddle),
        (bases, basis),
        (cycle_weight, weights),
        (assigned, assignment),
        (love_factor, love),
    )
    loads = [
        pltpu.make_async_copy(source, target, load_sem.at[i])
        for i, (source, target) in enumerate(pairs)
    ]
    with jax.named_scope("signals"):
        for load in loads:
            load.start()

        @pl.loop(0, peers - 1)
        def _(turn):
            there = peer(outward(turn))
            pl.semaphore_signal(
                barrier, inc=1, device_id=(there[0], chip + there[1]), device_id_type=MESH
            )

        for target in (on_ring(1), on_ring(-1), across):
            pl.semaphore_signal(barrier, inc=1, device_id=target, device_id_type=MESH)
        mine.start()
    with jax.named_scope("loads"):
        for load in loads:
            load.wait()

    with jax.named_scope("fft"):
        lane_of = lax.broadcasted_iota(jnp.int32, (1, LANES), 1)
        day = lane_of - jnp.where(lane_of < CYC, 0, jnp.where(lane_of < 2 * CYC, CYC, 2 * CYC))
        weight = jnp.zeros((1, LANES), F32)
        for j in range(CYC):
            weight = jnp.where(day == j, weights[j], weight)
        transformed(height, weight, twiddle, basis, pieces, spun, spread)

    with jax.named_scope("barrier"):
        pl.semaphore_wait(barrier, peers + 2)

    swap = remote(half_of(1 - core), held.at[core], swap_send, swap_recv, (c, chip + 1 - core))
    swap.start()

    @pl.loop(0, peers - 1)
    def _(turn):
        exchange(outward(turn), pieces, got, out_send, out_recv).start()

    got[c, core] = pieces[c, core]

    def turn(which):
        @pl.loop(0, CYC)
        def _(j):
            place = pl.ds(pl.multiple_of(j * half_orders, 8), half_orders)
            for tile in range(depth // LANES):
                wide[tile, place, :] = held[
                    which, j, :, tile * LANES : (tile + 1) * LANES
                ].astype(F32)

        @pl.loop(0, ring)
        def _(t):
            place = pl.ds(pl.multiple_of(which * LANES, LANES), LANES)
            for tile in range(depth // LANES):
                taken = [
                    wide[tile, pl.ds(TRI * t + i, CYC, stride=half_orders), :] for i in range(TRI)
                ]
                taken.append(jnp.zeros((LANES - TRI * CYC, LANES), F32))
                table[t, place, tile * LANES : (tile + 1) * LANES] = jnp.concatenate(
                    taken, axis=0
                ).astype(BF16)

    with jax.named_scope("turn_own"):
        mine.wait()
        turn(core)
    with jax.named_scope("swap_wait"):
        swap.wait()
    with jax.named_scope("turn_other"):
        turn(1 - core)

    with jax.named_scope("wait_out"):

        @pl.loop(1, peers)
        def _(offset):
            exchange(offset, pieces, got, out_send, out_recv).wait()

    with jax.named_scope("lines"):
        for g in range(cons):
            field = assignment[g]
            for s in range(2):
                mixed[(s * cons + g) * 16 : (s * cons + g + 1) * 16, :] = got[field, s].astype(F32)
        for t in range(ring):
            for s in range(2):
                for p in range(2):
                    lines[t, p * cons : (p + 1) * cons, s * LANES : (s + 1) * LANES] = mixed[
                        pl.ds(s * cons * 16 + p * 8 + t, cons, stride=16), :
                    ]

    lane = lax.broadcasted_iota(jnp.int32, (full, 2 * LANES), 1)
    lane = jnp.where(lane >= LANES, lane - LANES, lane)
    which = jnp.where(lane < CYC, 0, jnp.where(lane < 2 * CYC, 1, jnp.where(lane < TRI * CYC, 2, 3)))

    def analysed(t):
        x = lines[t]
        left = [jnp.where(which == i, x, 0.0) for i in range(TRI)]
        part[t] = jnp.dot(
            jnp.concatenate(left, axis=0).astype(BF16), table[t], preferred_element_type=F32
        ).astype(BF16)

    def piece(i, p):
        return pl.ds(i * full + p * cons, cons)

    ways = (1, -1)

    def sum_step(way, step, i, p):
        device = on_ring(ways[way])
        send, recv = sum_send.at[way, step, i, p], sum_recv.at[way, step, i, p]
        if step == 0:
            return remote(part.at[slot(far), piece(i, p)], first.at[way, i], send, recv, device)
        landing = later.at[way, step - 1, i, p]
        if step == 1 and p != way:
            owner = slot(ways[way] * (far - 1))
            return remote(part.at[owner, piece(i, p)], landing, send, recv, device)
        return remote(staged.at[way, step - 1, i, p], landing, send, recv, device)

    triples, ends = range(TRI), range(2)
    with jax.named_scope("first_part"):
        analysed(slot(far))
        for i in triples:
            for way in ends:
                sum_step(way, 0, i, way).start()
        for way in ends:
            analysed(slot(ways[way] * (far - 1)))
            for i in triples:
                sum_step(way, 1, i, 1 - way).start()
        for way in ends:
            analysed(slot(ways[way] * (far - 2)))
    for step in range(1, far):
        with jax.named_scope(f"sum#s={step}"):
            for late in ends:
                for i in triples:
                    for way in ends:
                        p = way if late else 1 - way
                        if step == 1 and not late:
                            continue
                        owner = slot(ways[way] * (far - step))
                        sum_step(way, step - 1, i, p).wait_recv()
                        come = first[way, i] if step == 1 else later[way, step - 2, i, p]
                        staged[way, step - 1, i, p] = (
                            part[owner, piece(i, p), :].astype(F32) + come.astype(F32)
                        ).astype(BF16)
                        sum_step(way, step, i, p).start()
        if step == 1:
            for way in ends:
                analysed(slot(ways[way] * (far - 3)))
        elif step == 2:
            analysed(z)

    def pair_step(i, p):
        return remote(
            sent.at[i, p], other.at[i, p], pair_send.at[i, p], pair_recv.at[i, p], across
        )

    with jax.named_scope("last_sum"):
        for i in triples:
            for p in ends:
                for way in ends:
                    sum_step(way, far - 1, i, p).wait_recv()
                sent[i, p] = (
                    part[z, piece(i, p), :].astype(F32)
                    + later[0, far - 2, i, p].astype(F32)
                    + later[1, far - 2, i, p].astype(F32)
                ).astype(BF16)
                pair_step(i, p).start()

    def all_step(way, step, i, p, late=0):
        ref = coef.at[slot(-ways[way] * (step + late)), piece(i, p)]
        send, recv = all_send.at[way, step, i, p], all_recv.at[way, step, i, p]
        return remote(ref, ref, send, recv, on_ring(ways[way]))

    def all_arrival(way, step, i, p):
        return all_step(way, step, i, p, 1)

    with jax.named_scope("pair"):
        scale = love[...].reshape(1, depth)
        for i in triples:
            for p in ends:
                pair_step(i, p).wait_recv()
                coef[z, piece(i, p), :] = (
                    (sent[i, p].astype(F32) + other[i, p].astype(F32)) * scale
                ).astype(BF16)
                for way in ends:
                    all_step(way, 0, i, p).start()

    def synthesised(t):
        got_all = lax.dot_general(
            coef[t], table[t], (((1,), (1,)), ((), ())), preferred_element_type=F32
        )
        chosen = jnp.where(
            which == 0, got_all[:full], jnp.where(which == 1, got_all[full : 2 * full], got_all[2 * full :])
        )
        order = which + (TRI * t + core * half_orders + c * 2 * half_orders)
        chosen = chosen * jnp.where(order == 0, 1.0, 2.0).astype(F32)
        for s in range(2):
            place = pl.ds(pl.multiple_of(s * ring * full + t * full, 8), full)
            rows[place, :] = chosen[:, s * LANES : (s + 1) * LANES]

    for step in range(1, far):
        with jax.named_scope(f"all#s={step}"):
            for i in triples:
                for p in ends:
                    for way in ends:
                        all_arrival(way, step - 1, i, p).wait_recv()
                        if step < far - 1 or p == way:
                            all_step(way, step, i, p).start()
        with jax.named_scope(f"synth#s={step}"):
            if step == 1:
                synthesised(z)
            else:
                for way in ways:
                    synthesised(slot(-way * (step - 1)))
    with jax.named_scope("synth_last"):
        for way in ways:
            synthesised(slot(-way * (far - 1)))
    with jax.named_scope("all_last"):
        for i in triples:
            for way in ends:
                all_arrival(way, far - 1, i, way).wait_recv()
    with jax.named_scope("synth_far"):
        synthesised(slot(far))

    with jax.named_scope("back"):
        for g in range(cons):
            for s in range(2):
                both = [
                    rows[pl.ds(s * ring * full + p * cons + g, ring, stride=full), :] for p in range(2)
                ]
                back[g, s] = jnp.concatenate(both, axis=0).astype(BF16)

    @pl.loop(0, peers - 1)
    def _(turn):
        exchange(outward(turn), back, out, back_send, back_recv).start()

    kept = pltpu.make_async_copy(back.at[c, core], out.at[c, core], own_sem)
    kept.start()

    with jax.named_scope("wait_sends"):
        for i in triples:
            for p in ends:
                pair_step(i, p).wait_send()
                for way in ends:
                    for step in range(far):
                        if step > 0 or p == way:
                            sum_step(way, step, i, p).wait_send()
                        if step < far - 1 or p == way:
                            all_step(way, step, i, p).wait_send()
        kept.wait()

    with jax.named_scope("wait_back"):

        @pl.loop(1, peers)
        def _(offset):
            exchange(offset, back, out, back_send, back_recv).wait()


def middle(elevation, legendre, cycle_weight, love_factor, assignment):
    cons = lax.axis_size("cons")
    period = elevation.shape[-1]
    depth = legendre.shape[2]
    ring = 8
    far = ring // 2
    full = 2 * cons
    dma = pltpu.SemaphoreType.DMA
    vmem = pltpu.VMEM
    twiddle, basis = phase_tables(period)
    pieces = (cons, 2, 16, LANES)
    return pl.pallas_call(
        functools.partial(middle_kernel, ring, cons),
        out_shape=jax.ShapeDtypeStruct(pieces, BF16),
        in_specs=[pl.BlockSpec(memory_space=pltpu.HBM)] * 7,
        out_specs=pl.BlockSpec(memory_space=pltpu.HBM),
        scratch_shapes=[
            vmem((1, CYC, period), BF16),
            pltpu.SMEM((CYC,), F32),
            vmem((depth,), F32),
            pltpu.SMEM((cons,), jnp.int32),
            vmem(twiddle.shape, F32),
            vmem(basis.shape, BF16),
            vmem(pieces, BF16),
            vmem((RADIX // TRI * LANES, 2 * LANES), F32),
            vmem((RADIX // TRI * full, LANES), F32),
            vmem((2, CYC, TRI * ring, depth), BF16),
            vmem((depth // LANES, CYC * TRI * ring, LANES), F32),
            vmem((ring, 2 * LANES, depth), BF16),
            vmem(pieces, BF16),
            vmem((2 * cons * 16, LANES), F32),
            vmem((ring, full, 2 * LANES), F32),
            vmem((ring, TRI * full, depth), BF16),
            vmem((2, TRI, cons, depth), BF16),
            vmem((2, far - 1, TRI, 2, cons, depth), BF16),
            vmem((2, far - 1, TRI, 2, cons, depth), BF16),
            vmem((TRI, 2, cons, depth), BF16),
            vmem((TRI, 2, cons, depth), BF16),
            vmem((ring, TRI * full, depth), BF16),
            vmem((2 * ring * full, LANES), F32),
            vmem(pieces, BF16),
            dma((6,)),
            dma,
            dma,
            dma,
            dma((2 * cons,)),
            dma((2 * cons,)),
            dma((2, far, TRI, 2)),
            dma((2, far, TRI, 2)),
            dma((TRI, 2)),
            dma((TRI, 2)),
            dma((2, far, TRI, 2)),
            dma((2, far, TRI, 2)),
            dma((2 * cons,)),
            dma((2 * cons,)),
        ],
        compiler_params=pltpu.CompilerParams(
            collective_id=KERNEL_ID, has_side_effects=True, vmem_limit_bytes=67_000_000
        ),
        name="middle",
    )(
        elevation,
        legendre,
        cycle_weight,
        love_factor,
        assignment,
        jnp.asarray(twiddle),
        jnp.asarray(basis),
    )


def local(elevation, legendre, cycle_weight, love_factor, assignment):
    returned = middle(elevation, legendre, cycle_weight, love_factor, assignment)
    return inverse(returned, elevation.shape[-1])


def solution(mesh):
    placed = (P("cons", "blk", None), P("blk", "cons", None), P("blk"), P(), P())
    return jax.shard_map(
        local, mesh=mesh, in_specs=placed, out_specs=P("cons", "blk", None), check_vma=False
    )
```

```python
import functools
import math
import numpy as np
import jax
import jax.numpy as jnp
from jax import lax
from jax.experimental import pallas as pl
from jax.experimental.pallas import tpu as pltpu
from jax.sharding import PartitionSpec as P

RADIX = 48
LANES = 128
CYC = 40
TRI = 3


def by_phase(value, turn):
    re, im = value
    cos, sin = math.cos(2 * math.pi * turn), math.sin(2 * math.pi * turn)
    cos = 0.0 if abs(cos) < 1e-12 else cos
    sin = 0.0 if abs(sin) < 1e-12 else sin

    def scaled(array, factor):
        if array is None or factor == 0.0:
            return None
        if abs(factor - 1.0) < 1e-12:
            return array
        if abs(factor + 1.0) < 1e-12:
            return -array
        return array * np.float32(factor)

    return (
        added(scaled(re, cos), scaled(im, -sin)),
        added(scaled(re, sin), scaled(im, cos)),
    )


def added(a, b):
    if a is None:
        return b
    return a if b is None else a + b


def plus(a, b):
    return added(a[0], b[0]), added(a[1], b[1])


def conj(a):
    return a[0], None if a[1] is None else -a[1]


def at(half, index, length):
    index %= length
    return half[index] if 2 * index <= length else conj(half[length - index])


def factor_of(length):
    return 4 if length % 4 == 0 else (3 if length % 3 == 0 else 2)


def real_fft(values):
    n = len(values)
    if n == 1:
        return [(values[0], None)]
    p = factor_of(n)
    parts = [real_fft(values[i::p]) for i in range(p)]
    out = []
    for k in range(n // 2 + 1):
        total = at(parts[0], k, n // p)
        for i in range(1, p):
            total = plus(total, by_phase(at(parts[i], k, n // p), -i * k / n))
        out.append(total)
    return out


def real_inverse(half, n):
    if n == 1:
        return [half[0][0]]
    p = factor_of(n)
    short = n // p
    out = [None] * n
    for a in range(p):
        folded = []
        for r in range(short // 2 + 1):
            total = (None, None)
            for s in range(p):
                index = r + s * short
                total = plus(total, by_phase(at(half, index, n), index * a / n))
            if r == 0 or 2 * r == short:
                total = (total[0], None)
            folded.append(total)
        for kk, value in enumerate(real_inverse(folded, short)):
            out[p * kk + a] = value
    return out


def phase_tables(period):
    lane = np.arange(LANES)
    turn = np.arange(RADIX)[:, None] * lane[None, :] / period
    twiddle = np.stack([np.cos(2 * np.pi * turn), np.sin(2 * np.pi * turn)], 1)
    q = np.arange(period // RADIX // 8)[:, None] * lane[None, :] / LANES
    cos, sin = np.cos(2 * np.pi * q), np.sin(2 * np.pi * q)
    basis = np.concatenate([np.concatenate([cos, sin], 1), np.concatenate([-sin, cos], 1)], 0)
    return twiddle.reshape(2 * RADIX, LANES).astype(np.float32), basis.astype(jnp.bfloat16)


def transformed(x_ref, weight, twiddle_ref, basis_ref, out_ref, mixed, rows):
    cons = out_ref.shape[0] // 2
    for triple in range(RADIX // TRI):
        mixed[triple * LANES + TRI * CYC : (triple + 1) * LANES, :] = jnp.zeros(
            (LANES - TRI * CYC, 2 * LANES), jnp.float32
        )

    @pl.loop(0, CYC // 8)
    def _(group):
        lines = pl.ds(pl.multiple_of(group * 8, 8), 8)
        half = real_fft(
            [
                x_ref[0, lines, k * LANES : (k + 1) * LANES].astype(jnp.float32)
                for k in range(RADIX)
            ]
        )
        for r in range(RADIX):
            re, im = at(half, r, RADIX)
            cos, sin = twiddle_ref[2 * r : 2 * r + 1, :], twiddle_ref[2 * r + 1 : 2 * r + 2, :]
            if im is None:
                new_re, new_im = re * cos, -re * sin
            else:
                new_re, new_im = re * cos + im * sin, im * cos - re * sin
            start = (r // TRI) * LANES + (r % TRI) * CYC
            place = pl.ds(pl.multiple_of(start + group * 8, 8), 8)
            mixed[place, 0:LANES] = new_re
            mixed[place, LANES:] = new_im

    for triple in range(RADIX // TRI):
        block = mixed[triple * LANES : (triple + 1) * LANES, :].astype(jnp.bfloat16)
        got = lax.dot_general(
            basis_ref[...], block, (((1,), (1,)), ((), ())), preferred_element_type=jnp.float32
        )
        rows[triple * 2 * cons : (triple + 1) * 2 * cons, :] = got * weight
    for c in range(cons):
        for h in range(2):
            both = [
                rows[pl.ds(h * 16 * cons + p * cons + c, 8, stride=2 * cons), :] for p in range(2)
            ]
            out_ref[2 * c + h] = jnp.concatenate(both, axis=0).astype(jnp.bfloat16)


def inverse_kernel(
    z_hbm, twiddle_hbm, basis_hbm, out_hbm, z_ref, twiddle_ref, basis_ref, rows, mixed, done, sems, out_sems
):
    pairs = ((z_hbm, z_ref), (twiddle_hbm, twiddle_ref), (basis_hbm, basis_ref))
    loads = [
        pltpu.make_async_copy(source, target, sems.at[i])
        for i, (source, target) in enumerate(pairs)
    ]
    for load in loads:
        load.start()
    for load in loads:
        load.wait()
    cons = z_ref.shape[0] // 2
    for source in range(2 * cons):
        rows[source * 16 : (source + 1) * 16, :] = z_ref[source].astype(jnp.float32)
    for triple in range(RADIX // TRI):
        h, t = divmod(triple, 8)
        both = [rows[pl.ds(h * 16 + p * 8 + t, cons, stride=32), :] for p in range(2)]
        lines = jnp.concatenate(both, axis=0).T.astype(jnp.bfloat16)
        mixed[triple * LANES : (triple + 1) * LANES, :] = jnp.dot(
            lines, basis_ref[...], preferred_element_type=jnp.float32
        )

    def leave(group):
        lines = pl.ds(pl.multiple_of(group * 8, 8), 8)
        return pltpu.make_async_copy(done.at[group], out_hbm.at[0, lines], out_sems.at[group])

    @pl.loop(0, CYC // 8)
    def _(group):
        turned = []
        for r in range(RADIX):
            start = (r // TRI) * LANES + (r % TRI) * CYC
            place = pl.ds(pl.multiple_of(start + group * 8, 8), 8)
            re, im = mixed[place, 0:LANES], mixed[place, LANES:]
            cos, sin = twiddle_ref[2 * r : 2 * r + 1, :], twiddle_ref[2 * r + 1 : 2 * r + 2, :]
            turned.append((re * cos - im * sin, re * sin + im * cos))
        middle = RADIX // 2
        half = [(turned[0][0], None)]
        for r in range(1, middle):
            pair = plus(turned[r], conj(turned[RADIX - r]))
            half.append((pair[0] * np.float32(0.5), pair[1] * np.float32(0.5)))
        half.append((turned[middle][0], None))
        for k, value in enumerate(real_inverse(half, RADIX)):
            done[group, :, k * LANES : (k + 1) * LANES] = value
        leave(group).start()

    @pl.loop(0, CYC // 8)
    def _(group):
        leave(group).wait()


def inverse(pieces, period):
    cons = pieces.shape[0] // 2
    twiddle, basis = phase_tables(period)
    return pl.pallas_call(
        inverse_kernel,
        out_shape=jax.ShapeDtypeStruct((1, CYC, period), jnp.float32),
        in_specs=[pl.BlockSpec(memory_space=pltpu.HBM)] * 3,
        out_specs=pl.BlockSpec(memory_space=pltpu.HBM),
        scratch_shapes=[
            pltpu.VMEM(pieces.shape, jnp.bfloat16),
            pltpu.VMEM(twiddle.shape, jnp.float32),
            pltpu.VMEM(basis.shape, jnp.bfloat16),
            pltpu.VMEM((2 * cons * 16, LANES), jnp.float32),
            pltpu.VMEM((RADIX // TRI * LANES, 2 * LANES), jnp.float32),
            pltpu.VMEM((CYC // 8, 8, period), jnp.float32),
            pltpu.SemaphoreType.DMA((3,)),
            pltpu.SemaphoreType.DMA((CYC // 8,)),
        ],
        compiler_params=pltpu.CompilerParams(vmem_limit_bytes=67_000_000),
        name="inverse",
    )(pieces, jnp.asarray(twiddle), jnp.asarray(basis))


MESH = pl.DeviceIdType.MESH
F32 = jnp.float32
BF16 = jnp.bfloat16
KERNEL_ID = 0


def middle_kernel(
    ring, cons, elevation, legendre, cycle_weight, love_factor, assigned, twiddles, bases, out,
    height, weights, love, assignment, twiddle, basis, pieces, spun, spread,
    held, wide, table, got, mixed, lines, part, first, later, staged, sent, other, coef,
    rows, back,
    load_sem, own_sem, swap_send, swap_recv, out_send, out_recv, sum_send, pair_send, all_send,
    ring_recv, pair_recv, back_send, back_recv,
):
    c, b = lax.axis_index("cons"), lax.axis_index("blk")
    core = lax.rem(b, 2)
    z = lax.rem(b // 2, ring)
    line = b // (2 * ring)
    chip = b - core
    me = 2 * c + core
    peers = 2 * cons
    far = ring // 2
    depth = legendre.shape[2]
    half_orders = TRI * ring
    full = 2 * cons
    barrier = pltpu.get_barrier_semaphore()

    def slot(offset):
        return lax.rem(z + offset + ring, ring)

    def on_ring(offset):
        return (c, line * 2 * ring + slot(offset) * 2 + core)

    def outward(turn):
        odd = lax.rem(turn, 2)
        return peers // 2 + ((turn + 1) // 2) * (2 * odd - 1)

    def remote(source, target, send, recv, device):
        return pltpu.make_async_remote_copy(
            src_ref=source,
            dst_ref=target,
            send_sem=send,
            recv_sem=recv,
            device_id=device,
            device_id_type=MESH,
        )

    def exchange(offset, source, landing, send, recv):
        index = lax.rem(me + offset, peers)
        there = (index // 2, chip + lax.rem(index, 2))
        return remote(source.at[index], landing.at[me], send, recv, there)

    def exchanged(source, landing, send, recv):
        rest = pl.ds(0, peers - 1)
        return remote(source.at[rest], landing.at[rest], send, recv, (c, chip + 1 - core))

    across = (c, (1 - line) * 2 * ring + z * 2 + core)

    def half_of(which):
        return legendre.at[:, pl.ds(pl.multiple_of(which * half_orders, 8), half_orders), :]

    mine = pltpu.make_async_copy(half_of(core), held.at[core], own_sem)
    pairs = (
        (elevation, height),
        (twiddles, twiddle),
        (bases, basis),
        (cycle_weight, weights),
        (assigned, assignment),
        (love_factor, love),
    )
    loads = [
        pltpu.make_async_copy(source, target, load_sem.at[i])
        for i, (source, target) in enumerate(pairs)
    ]
    with jax.named_scope("signals"):
        for load in loads:
            load.start()

        @pl.loop(0, peers - 1)
        def _(turn):
            index = lax.rem(me + outward(turn), peers)
            there = (index // 2, chip + lax.rem(index, 2))
            pl.semaphore_signal(barrier, inc=1, device_id=there, device_id_type=MESH)

        for target in (on_ring(1), on_ring(-1), across):
            pl.semaphore_signal(barrier, inc=1, device_id=target, device_id_type=MESH)
        mine.start()
    with jax.named_scope("loads"):
        for load in loads:
            load.wait()

    with jax.named_scope("fft"):
        lane_of = lax.broadcasted_iota(jnp.int32, (1, LANES), 1)
        day = lane_of - jnp.where(lane_of < CYC, 0, jnp.where(lane_of < 2 * CYC, CYC, 2 * CYC))
        weight = jnp.zeros((1, LANES), F32)
        for j in range(CYC):
            weight = jnp.where(day == j, weights[j], weight)
        transformed(height, weight, twiddle, basis, pieces, spun, spread)

    with jax.named_scope("barrier"):
        pl.semaphore_wait(barrier, peers + 2)

    swap = remote(half_of(1 - core), held.at[core], swap_send, swap_recv, (c, chip + 1 - core))
    swap.start()

    @pl.loop(0, peers - 1)
    def _(turn):
        exchange(outward(turn), pieces, got, out_send, out_recv).start()

    got[me] = pieces[me]

    def turn(which):
        @pl.loop(0, CYC)
        def _(j):
            place = pl.ds(pl.multiple_of(j * half_orders, 8), half_orders)
            for tile in range(depth // LANES):
                wide[tile, place, :] = held[
                    which, j, :, tile * LANES : (tile + 1) * LANES
                ].astype(F32)

        @pl.loop(0, ring)
        def _(t):
            place = pl.ds(pl.multiple_of(which * LANES, LANES), LANES)
            for tile in range(depth // LANES):
                taken = [
                    wide[tile, pl.ds(TRI * t + i, CYC, stride=half_orders), :] for i in range(TRI)
                ]
                taken.append(jnp.zeros((LANES - TRI * CYC, LANES), F32))
                table[t, place, tile * LANES : (tile + 1) * LANES] = jnp.concatenate(
                    taken, axis=0
                ).astype(BF16)

    with jax.named_scope("turn_own"):
        mine.wait()
        turn(core)
    with jax.named_scope("swap_wait"):
        swap.wait()
    with jax.named_scope("turn_other"):
        turn(1 - core)

    with jax.named_scope("wait_out"):
        exchanged(pieces, got, out_send, out_recv).wait()

    with jax.named_scope("lines"):
        for g in range(cons):
            field = assignment[g]
            for s in range(2):
                mixed[(s * cons + g) * 16 : (s * cons + g + 1) * 16, :] = got[2 * field + s].astype(F32)
        for t in range(ring):
            for s in range(2):
                for p in range(2):
                    lines[t, p * cons : (p + 1) * cons, s * LANES : (s + 1) * LANES] = mixed[
                        pl.ds(s * cons * 16 + p * 8 + t, cons, stride=16), :
                    ]

    lane = lax.broadcasted_iota(jnp.int32, (full, 2 * LANES), 1)
    lane = jnp.where(lane >= LANES, lane - LANES, lane)
    which = jnp.where(lane < CYC, 0, jnp.where(lane < 2 * CYC, 1, jnp.where(lane < TRI * CYC, 2, 3)))

    def analysed(t):
        x = lines[t]
        left = [jnp.where(which == i, x, 0.0) for i in range(TRI)]
        part[t] = jnp.dot(
            jnp.concatenate(left, axis=0).astype(BF16), table[t], preferred_element_type=F32
        ).astype(BF16)

    def piece(i, p):
        return pl.ds(i * full + p * cons, cons)

    ways = (1, -1)

    def sum_step(way, step, i, p):
        device = on_ring(ways[way])
        send, recv = sum_send, ring_recv.at[way, step, i, p]
        if step == 0:
            return remote(part.at[slot(far), piece(i, p)], first.at[way, i], send, recv, device)
        landing = later.at[way, step - 1, i, p]
        if step == 1 and p != way:
            owner = slot(ways[way] * (far - 1))
            return remote(part.at[owner, piece(i, p)], landing, send, recv, device)
        return remote(staged.at[way, step - 1, i, p], landing, send, recv, device)

    triples, ends = range(TRI), range(2)
    with jax.named_scope("first_part"):
        analysed(slot(far))
        for i in triples:
            for way in ends:
                sum_step(way, 0, i, way).start()
        for way in ends:
            analysed(slot(ways[way] * (far - 1)))
            for i in triples:
                sum_step(way, 1, i, 1 - way).start()
        for way in ends:
            analysed(slot(ways[way] * (far - 2)))
    for step in range(1, far):
        with jax.named_scope(f"sum#s={step}"):
            for late in ends:
                for i in triples:
                    for way in ends:
                        p = way if late else 1 - way
                        if step == 1 and not late:
                            continue
                        owner = slot(ways[way] * (far - step))
                        sum_step(way, step - 1, i, p).wait_recv()
                        come = first[way, i] if step == 1 else later[way, step - 2, i, p]
                        staged[way, step - 1, i, p] = (
                            part[owner, piece(i, p), :].astype(F32) + come.astype(F32)
                        ).astype(BF16)
                        sum_step(way, step, i, p).start()
        if step == 1:
            for way in ends:
                analysed(slot(ways[way] * (far - 3)))
        elif step == 2:
            analysed(z)

    def pair_step(i, p):
        return remote(
            sent.at[i, p], other.at[i, p], pair_send, pair_recv.at[i, p], across
        )

    with jax.named_scope("last_sum"):
        for i in triples:
            for p in ends:
                for way in ends:
                    sum_step(way, far - 1, i, p).wait_recv()
                sent[i, p] = (
                    part[z, piece(i, p), :].astype(F32)
                    + later[0, far - 2, i, p].astype(F32)
                    + later[1, far - 2, i, p].astype(F32)
                ).astype(BF16)
                pair_step(i, p).start()

    def all_step(way, step, i, p, late=0):
        ref = coef.at[slot(-ways[way] * (step + late)), piece(i, p)]
        return remote(ref, ref, all_send, ring_recv.at[way, step, i, p], on_ring(ways[way]))

    def all_arrival(way, step, i, p):
        return all_step(way, step, i, p, 1)

    with jax.named_scope("pair"):
        scale = love[...].reshape(1, depth)
        for i in triples:
            for p in ends:
                pair_step(i, p).wait_recv()
                coef[z, piece(i, p), :] = (
                    (sent[i, p].astype(F32) + other[i, p].astype(F32)) * scale
                ).astype(BF16)
                for way in ends:
                    all_step(way, 0, i, p).start()

    def synthesised(t):
        got_all = lax.dot_general(
            coef[t], table[t], (((1,), (1,)), ((), ())), preferred_element_type=F32
        )
        chosen = jnp.where(
            which == 0, got_all[:full], jnp.where(which == 1, got_all[full : 2 * full], got_all[2 * full :])
        )
        order = which + (TRI * t + core * half_orders + c * 2 * half_orders)
        chosen = chosen * jnp.where(order == 0, 1.0, 2.0).astype(F32)
        for s in range(2):
            place = pl.ds(pl.multiple_of(s * ring * full + t * full, 8), full)
            rows[place, :] = chosen[:, s * LANES : (s + 1) * LANES]

    for step in range(1, far):
        with jax.named_scope(f"all#s={step}"):
            for i in triples:
                for p in ends:
                    for way in ends:
                        all_arrival(way, step - 1, i, p).wait_recv()
                        if step < far - 1 or p == way:
                            all_step(way, step, i, p).start()
        with jax.named_scope(f"synth#s={step}"):
            if step == 1:
                synthesised(z)
            else:
                for way in ways:
                    synthesised(slot(-way * (step - 1)))
    with jax.named_scope("synth_last"):
        for way in ways:
            synthesised(slot(-way * (far - 1)))
    with jax.named_scope("all_last"):
        for i in triples:
            for way in ends:
                all_arrival(way, far - 1, i, way).wait_recv()
    with jax.named_scope("synth_far"):
        synthesised(slot(far))

    with jax.named_scope("back"):
        for g in range(cons):
            for s in range(2):
                both = [
                    rows[pl.ds(s * ring * full + p * cons + g, ring, stride=full), :] for p in range(2)
                ]
                back[2 * g + s] = jnp.concatenate(both, axis=0).astype(BF16)

    @pl.loop(0, peers - 1)
    def _(turn):
        exchange(outward(turn), back, out, back_send, back_recv).start()

    kept = pltpu.make_async_copy(back.at[me], out.at[me], own_sem)
    kept.start()

    with jax.named_scope("wait_sends"):
        most = pl.ds(0, ring - 1)
        remote(part.at[most], part.at[most], sum_send, own_sem, across).wait_send()
        remote(coef.at[most], coef.at[most], all_send, own_sem, across).wait_send()
        remote(sent, other, pair_send, own_sem, across).wait_send()
        kept.wait()

    with jax.named_scope("wait_back"):
        exchanged(back, out, back_send, back_recv).wait()


def middle(elevation, legendre, cycle_weight, love_factor, assignment):
    cons = lax.axis_size("cons")
    period = elevation.shape[-1]
    depth = legendre.shape[2]
    ring = 8
    far = ring // 2
    full = 2 * cons
    dma = pltpu.SemaphoreType.DMA
    vmem = pltpu.VMEM
    twiddle, basis = phase_tables(period)
    pieces = (2 * cons, 16, LANES)
    return pl.pallas_call(
        functools.partial(middle_kernel, ring, cons),
        out_shape=jax.ShapeDtypeStruct(pieces, BF16),
        in_specs=[pl.BlockSpec(memory_space=pltpu.HBM)] * 7,
        out_specs=pl.BlockSpec(memory_space=pltpu.HBM),
        scratch_shapes=[
            vmem((1, CYC, period), BF16),
            pltpu.SMEM((CYC,), F32),
            vmem((depth,), F32),
            pltpu.SMEM((cons,), jnp.int32),
            vmem(twiddle.shape, F32),
            vmem(basis.shape, BF16),
            vmem(pieces, BF16),
            vmem((RADIX // TRI * LANES, 2 * LANES), F32),
            vmem((RADIX // TRI * full, LANES), F32),
            vmem((2, CYC, TRI * ring, depth), BF16),
            vmem((depth // LANES, CYC * TRI * ring, LANES), F32),
            vmem((ring, 2 * LANES, depth), BF16),
            vmem(pieces, BF16),
            vmem((2 * cons * 16, LANES), F32),
            vmem((ring, full, 2 * LANES), F32),
            vmem((ring, TRI * full, depth), BF16),
            vmem((2, TRI, cons, depth), BF16),
            vmem((2, far - 1, TRI, 2, cons, depth), BF16),
            vmem((2, far - 1, TRI, 2, cons, depth), BF16),
            vmem((TRI, 2, cons, depth), BF16),
            vmem((TRI, 2, cons, depth), BF16),
            vmem((ring, TRI * full, depth), BF16),
            vmem((2 * ring * full, LANES), F32),
            vmem(pieces, BF16),
            dma((6,)),
            dma,
            dma,
            dma,
            dma,
            dma,
            dma,
            dma,
            dma,
            dma((2, far, TRI, 2)),
            dma((TRI, 2)),
            dma,
            dma,
        ],
        compiler_params=pltpu.CompilerParams(
            collective_id=KERNEL_ID, has_side_effects=True, vmem_limit_bytes=67_000_000
        ),
        name="middle",
    )(
        elevation,
        legendre,
        cycle_weight,
        love_factor,
        assignment,
        jnp.asarray(twiddle),
        jnp.asarray(basis),
    )


def local(elevation, legendre, cycle_weight, love_factor, assignment):
    returned = middle(elevation, legendre, cycle_weight, love_factor, assignment)
    return inverse(returned, elevation.shape[-1])


def solution(mesh):
    placed = (P("cons", "blk", None), P("blk", "cons", None), P("blk"), P(), P())
    return jax.shard_map(
        local, mesh=mesh, in_specs=placed, out_specs=P("cons", "blk", None), check_vma=False
    )
```

```python
import functools
import math
import numpy as np
import jax
import jax.numpy as jnp
from jax import lax
from jax.experimental import pallas as pl
from jax.experimental.pallas import tpu as pltpu
from jax.sharding import PartitionSpec as P

RADIX = 48
LANES = 128
CYC = 40
TRI = 3


def by_phase(value, turn):
    re, im = value
    cos, sin = math.cos(2 * math.pi * turn), math.sin(2 * math.pi * turn)
    cos = 0.0 if abs(cos) < 1e-12 else cos
    sin = 0.0 if abs(sin) < 1e-12 else sin

    def scaled(array, factor):
        if array is None or factor == 0.0:
            return None
        if abs(factor - 1.0) < 1e-12:
            return array
        if abs(factor + 1.0) < 1e-12:
            return -array
        return array * np.float32(factor)

    return (
        added(scaled(re, cos), scaled(im, -sin)),
        added(scaled(re, sin), scaled(im, cos)),
    )


def added(a, b):
    if a is None:
        return b
    return a if b is None else a + b


def plus(a, b):
    return added(a[0], b[0]), added(a[1], b[1])


def conj(a):
    return a[0], None if a[1] is None else -a[1]


def at(half, index, length):
    index %= length
    return half[index] if 2 * index <= length else conj(half[length - index])


def factor_of(length):
    return 4 if length % 4 == 0 else (3 if length % 3 == 0 else 2)


def real_fft(values):
    n = len(values)
    if n == 1:
        return [(values[0], None)]
    p = factor_of(n)
    parts = [real_fft(values[i::p]) for i in range(p)]
    out = []
    for k in range(n // 2 + 1):
        total = at(parts[0], k, n // p)
        for i in range(1, p):
            total = plus(total, by_phase(at(parts[i], k, n // p), -i * k / n))
        out.append(total)
    return out


def real_inverse(half, n):
    if n == 1:
        return [half[0][0]]
    p = factor_of(n)
    short = n // p
    out = [None] * n
    for a in range(p):
        folded = []
        for r in range(short // 2 + 1):
            total = (None, None)
            for s in range(p):
                index = r + s * short
                total = plus(total, by_phase(at(half, index, n), index * a / n))
            if r == 0 or 2 * r == short:
                total = (total[0], None)
            folded.append(total)
        for kk, value in enumerate(real_inverse(folded, short)):
            out[p * kk + a] = value
    return out


def phase_tables(period):
    lane = np.arange(LANES)
    turn = np.arange(RADIX)[:, None] * lane[None, :] / period
    twiddle = np.stack([np.cos(2 * np.pi * turn), np.sin(2 * np.pi * turn)], 1)
    q = np.arange(period // RADIX // 8)[:, None] * lane[None, :] / LANES
    cos, sin = np.cos(2 * np.pi * q), np.sin(2 * np.pi * q)
    basis = np.concatenate([np.concatenate([cos, sin], 1), np.concatenate([-sin, cos], 1)], 0)
    return twiddle.reshape(2 * RADIX, LANES).astype(np.float32), basis.astype(jnp.bfloat16)


def transformed(x_ref, weight, twiddle_ref, basis_ref, out_ref, mixed, rows):
    cons = out_ref.shape[0] // 2
    for triple in range(RADIX // TRI):
        mixed[triple * LANES + TRI * CYC : (triple + 1) * LANES, :] = jnp.zeros(
            (LANES - TRI * CYC, 2 * LANES), jnp.float32
        )

    @pl.loop(0, CYC // 8)
    def _(group):
        lines = pl.ds(pl.multiple_of(group * 8, 8), 8)
        half = real_fft(
            [
                x_ref[0, lines, k * LANES : (k + 1) * LANES].astype(jnp.float32)
                for k in range(RADIX)
            ]
        )
        for r in range(RADIX):
            re, im = at(half, r, RADIX)
            cos, sin = twiddle_ref[2 * r : 2 * r + 1, :], twiddle_ref[2 * r + 1 : 2 * r + 2, :]
            if im is None:
                new_re, new_im = re * cos, -re * sin
            else:
                new_re, new_im = re * cos + im * sin, im * cos - re * sin
            start = (r // TRI) * LANES + (r % TRI) * CYC
            place = pl.ds(pl.multiple_of(start + group * 8, 8), 8)
            mixed[place, 0:LANES] = new_re
            mixed[place, LANES:] = new_im

    for triple in range(RADIX // TRI):
        block = mixed[triple * LANES : (triple + 1) * LANES, :].astype(jnp.bfloat16)
        got = lax.dot_general(
            basis_ref[...], block, (((1,), (1,)), ((), ())), preferred_element_type=jnp.float32
        )
        rows[triple * 2 * cons : (triple + 1) * 2 * cons, :] = got * weight
    for c in range(cons):
        for h in range(2):
            both = [
                rows[pl.ds(h * 16 * cons + p * cons + c, 8, stride=2 * cons), :] for p in range(2)
            ]
            out_ref[2 * c + h] = jnp.concatenate(both, axis=0).astype(jnp.bfloat16)


def inverse_kernel(
    z_hbm, twiddle_hbm, basis_hbm, out_hbm, z_ref, twiddle_ref, basis_ref, rows, mixed, done, sems, out_sems
):
    pairs = ((z_hbm, z_ref), (twiddle_hbm, twiddle_ref), (basis_hbm, basis_ref))
    loads = [
        pltpu.make_async_copy(source, target, sems.at[i])
        for i, (source, target) in enumerate(pairs)
    ]
    for load in loads:
        load.start()
    for load in loads:
        load.wait()
    cons = z_ref.shape[0] // 2
    for source in range(2 * cons):
        rows[source * 16 : (source + 1) * 16, :] = z_ref[source].astype(jnp.float32)
    for triple in range(RADIX // TRI):
        h, t = divmod(triple, 8)
        both = [rows[pl.ds(h * 16 + p * 8 + t, cons, stride=32), :] for p in range(2)]
        lines = jnp.concatenate(both, axis=0).T.astype(jnp.bfloat16)
        mixed[triple * LANES : (triple + 1) * LANES, :] = jnp.dot(
            lines, basis_ref[...], preferred_element_type=jnp.float32
        )

    def leave(group):
        lines = pl.ds(pl.multiple_of(group * 8, 8), 8)
        return pltpu.make_async_copy(done.at[group], out_hbm.at[0, lines], out_sems.at[group])

    @pl.loop(0, CYC // 8)
    def _(group):
        turned = []
        for r in range(RADIX):
            start = (r // TRI) * LANES + (r % TRI) * CYC
            place = pl.ds(pl.multiple_of(start + group * 8, 8), 8)
            re, im = mixed[place, 0:LANES], mixed[place, LANES:]
            cos, sin = twiddle_ref[2 * r : 2 * r + 1, :], twiddle_ref[2 * r + 1 : 2 * r + 2, :]
            turned.append((re * cos - im * sin, re * sin + im * cos))
        middle = RADIX // 2
        half = [(turned[0][0], None)]
        for r in range(1, middle):
            pair = plus(turned[r], conj(turned[RADIX - r]))
            half.append((pair[0] * np.float32(0.5), pair[1] * np.float32(0.5)))
        half.append((turned[middle][0], None))
        for k, value in enumerate(real_inverse(half, RADIX)):
            done[group, :, k * LANES : (k + 1) * LANES] = value
        leave(group).start()

    @pl.loop(0, CYC // 8)
    def _(group):
        leave(group).wait()


def inverse(pieces, period):
    cons = pieces.shape[0] // 2
    twiddle, basis = phase_tables(period)
    return pl.pallas_call(
        inverse_kernel,
        out_shape=jax.ShapeDtypeStruct((1, CYC, period), jnp.float32),
        in_specs=[pl.BlockSpec(memory_space=pltpu.HBM)] * 3,
        out_specs=pl.BlockSpec(memory_space=pltpu.HBM),
        scratch_shapes=[
            pltpu.VMEM(pieces.shape, jnp.bfloat16),
            pltpu.VMEM(twiddle.shape, jnp.float32),
            pltpu.VMEM(basis.shape, jnp.bfloat16),
            pltpu.VMEM((2 * cons * 16, LANES), jnp.float32),
            pltpu.VMEM((RADIX // TRI * LANES, 2 * LANES), jnp.float32),
            pltpu.VMEM((CYC // 8, 8, period), jnp.float32),
            pltpu.SemaphoreType.DMA((3,)),
            pltpu.SemaphoreType.DMA((CYC // 8,)),
        ],
        compiler_params=pltpu.CompilerParams(vmem_limit_bytes=67_000_000),
        name="inverse",
    )(pieces, jnp.asarray(twiddle), jnp.asarray(basis))


MESH = pl.DeviceIdType.MESH
F32 = jnp.float32
BF16 = jnp.bfloat16
KERNEL_ID = 0


def middle_kernel(
    ring, cons, elevation, legendre, cycle_weight, love_factor, assigned, twiddles, bases, out,
    height, weights, love, assignment, twiddle, basis, pieces, spun, spread,
    held, wide, table, got, mixed, lines, part, first, later, staged, sent, other, crossed, coef,
    rows, back,
    load_sem, own_sem, swap_send, swap_recv, out_send, out_recv, sum_send, pair_send, all_send,
    ring_recv, pair_recv, cross_recv, back_send, back_recv,
):
    c, b = lax.axis_index("cons"), lax.axis_index("blk")
    core = lax.rem(b, 2)
    z = lax.rem(b // 2, ring)
    line = b // (2 * ring)
    chip = b - core
    me = 2 * c + core
    peers = 2 * cons
    far = ring // 2
    depth = legendre.shape[2]
    half_orders = TRI * ring
    full = 2 * cons
    barrier = pltpu.get_barrier_semaphore()

    def slot(offset):
        return lax.rem(z + offset + ring, ring)

    def on_ring(offset):
        return (c, line * 2 * ring + slot(offset) * 2 + core)

    def outward(turn):
        odd = lax.rem(turn, 2)
        return peers // 2 + ((turn + 1) // 2) * (2 * odd - 1)

    def remote(source, target, send, recv, device):
        return pltpu.make_async_remote_copy(
            src_ref=source,
            dst_ref=target,
            send_sem=send,
            recv_sem=recv,
            device_id=device,
            device_id_type=MESH,
        )

    def exchange(offset, source, landing, send, recv):
        index = lax.rem(me + offset, peers)
        there = (index // 2, chip + lax.rem(index, 2))
        return remote(source.at[index], landing.at[me], send, recv, there)

    def exchanged(source, landing, send, recv):
        rest = pl.ds(0, peers - 1)
        return remote(source.at[rest], landing.at[rest], send, recv, (c, chip + 1 - core))

    across = (c, (1 - line) * 2 * ring + z * 2 + core)

    def half_of(which):
        return legendre.at[:, pl.ds(pl.multiple_of(which * half_orders, 8), half_orders), :]

    mine = pltpu.make_async_copy(half_of(core), held.at[core], own_sem)
    pairs = (
        (elevation, height),
        (twiddles, twiddle),
        (bases, basis),
        (cycle_weight, weights),
        (assigned, assignment),
        (love_factor, love),
    )
    loads = [
        pltpu.make_async_copy(source, target, load_sem.at[i])
        for i, (source, target) in enumerate(pairs)
    ]
    with jax.named_scope("signals"):
        for load in loads:
            load.start()

        @pl.loop(0, peers - 1)
        def _(turn):
            index = lax.rem(me + outward(turn), peers)
            there = (index // 2, chip + lax.rem(index, 2))
            pl.semaphore_signal(barrier, inc=1, device_id=there, device_id_type=MESH)

        for target in (on_ring(1), on_ring(-1), on_ring(2), on_ring(-2), across):
            pl.semaphore_signal(barrier, inc=1, device_id=target, device_id_type=MESH)
        mine.start()
    with jax.named_scope("loads"):
        for load in loads:
            load.wait()

    with jax.named_scope("fft"):
        lane_of = lax.broadcasted_iota(jnp.int32, (1, LANES), 1)
        day = lane_of - jnp.where(lane_of < CYC, 0, jnp.where(lane_of < 2 * CYC, CYC, 2 * CYC))
        weight = jnp.zeros((1, LANES), F32)
        for j in range(CYC):
            weight = jnp.where(day == j, weights[j], weight)
        transformed(height, weight, twiddle, basis, pieces, spun, spread)

    with jax.named_scope("barrier"):
        pl.semaphore_wait(barrier, peers + 4)

    swap = remote(half_of(1 - core), held.at[core], swap_send, swap_recv, (c, chip + 1 - core))
    swap.start()

    @pl.loop(0, peers - 1)
    def _(turn):
        exchange(outward(turn), pieces, got, out_send, out_recv).start()

    got[me] = pieces[me]

    def turn(which):
        @pl.loop(0, CYC)
        def _(j):
            place = pl.ds(pl.multiple_of(j * half_orders, 8), half_orders)
            for tile in range(depth // LANES):
                wide[tile, place, :] = held[
                    which, j, :, tile * LANES : (tile + 1) * LANES
                ].astype(F32)

        @pl.loop(0, ring)
        def _(t):
            place = pl.ds(pl.multiple_of(which * LANES, LANES), LANES)
            for tile in range(depth // LANES):
                taken = [
                    wide[tile, pl.ds(TRI * t + i, CYC, stride=half_orders), :] for i in range(TRI)
                ]
                taken.append(jnp.zeros((LANES - TRI * CYC, LANES), F32))
                table[t, place, tile * LANES : (tile + 1) * LANES] = jnp.concatenate(
                    taken, axis=0
                ).astype(BF16)

    with jax.named_scope("turn_own"):
        mine.wait()
        turn(core)
    with jax.named_scope("swap_wait"):
        swap.wait()
    with jax.named_scope("turn_other"):
        turn(1 - core)

    with jax.named_scope("wait_out"):
        exchanged(pieces, got, out_send, out_recv).wait()

    with jax.named_scope("lines"):
        for g in range(cons):
            field = assignment[g]
            for s in range(2):
                mixed[(s * cons + g) * 16 : (s * cons + g + 1) * 16, :] = got[2 * field + s].astype(F32)
        for t in range(ring):
            for s in range(2):
                for p in range(2):
                    lines[t, p * cons : (p + 1) * cons, s * LANES : (s + 1) * LANES] = mixed[
                        pl.ds(s * cons * 16 + p * 8 + t, cons, stride=16), :
                    ]

    lane = lax.broadcasted_iota(jnp.int32, (full, 2 * LANES), 1)
    lane = jnp.where(lane >= LANES, lane - LANES, lane)
    which = jnp.where(lane < CYC, 0, jnp.where(lane < 2 * CYC, 1, jnp.where(lane < TRI * CYC, 2, 3)))

    def analysed(t):
        x = lines[t]
        left = [jnp.where(which == i, x, 0.0) for i in range(TRI)]
        part[t] = jnp.dot(
            jnp.concatenate(left, axis=0).astype(BF16), table[t], preferred_element_type=F32
        ).astype(BF16)

    def piece(i, p):
        return pl.ds(pl.multiple_of(i * full + p * cons, cons), cons)

    ways, triples, ends = (1, -1), range(TRI), range(2)
    scale = love[...].reshape(1, depth)

    def synthesised(t):
        got_all = lax.dot_general(
            coef[t], table[t], (((1,), (1,)), ((), ())), preferred_element_type=F32
        )
        chosen = jnp.where(
            which == 0,
            got_all[:full],
            jnp.where(which == 1, got_all[full : 2 * full], got_all[2 * full :]),
        )
        order = which + (TRI * t + core * half_orders + c * 2 * half_orders)
        chosen = chosen * jnp.where(order == 0, 1.0, 2.0).astype(F32)
        for s in range(2):
            place = pl.ds(pl.multiple_of(s * ring * full + t * full, 8), full)
            rows[place, :] = chosen[:, s * LANES : (s + 1) * LANES]

    def sum_sent(source, target, way, step, i, p, hops=1):
        return remote(
            source, target, sum_send, ring_recv.at[way, step, i, p], on_ring(hops * ways[way])
        )

    @pl.when(core == 0)
    def _():
        def sum_step(way, step, i, p):
            if step == 0:
                source = part.at[slot(far), piece(i, p)]
                return sum_sent(source, first.at[way, i], way, step, i, p, 2)
            target = later.at[way, step - 1, i, p]
            if step == 1:
                source = part.at[slot(ways[way] * (far - 1)), piece(i, p)]
            else:
                source = staged.at[way, step - 1, i, p]
            return sum_sent(source, target, way, step, i, p)

        with jax.named_scope("first_part"):
            analysed(slot(far))
            for i in triples:
                for way in ends:
                    sum_step(way, 0, i, way).start()
            for way in ends:
                analysed(slot(ways[way] * (far - 1)))
                for i in triples:
                    for p in (1 - way, way):
                        sum_step(way, 1, i, p).start()
            for step in range(2, far):
                for way in ends:
                    analysed(slot(ways[way] * (far - step)))
            analysed(z)
        for step in range(2, far):
            with jax.named_scope(f"sum#s={step}"):
                for i in triples:
                    for late in ends:
                        for way in ends:
                            p = way if late else 1 - way
                            owner = slot(ways[way] * (far - step))
                            sum_step(way, step - 1, i, p).wait_recv()
                            total = part[owner, piece(i, p), :].astype(F32) + later[
                                way, step - 2, i, p
                            ].astype(F32)
                            if step == 2 and late:
                                sum_step(way, 0, i, p).wait_recv()
                                total = total + first[way, i].astype(F32)
                            staged[way, step - 1, i, p] = total.astype(BF16)
                            sum_step(way, step, i, p).start()

        def pair_step(i, p):
            return remote(
                sent.at[i, p], other.at[i, p], pair_send, pair_recv.at[i, p], across
            )

        with jax.named_scope("last_sum"):
            for i in triples:
                for p in ends:
                    for way in ends:
                        sum_step(way, far - 1, i, p).wait_recv()
                    sent[i, p] = (
                        part[z, piece(i, p), :].astype(F32)
                        + later[0, far - 2, i, p].astype(F32)
                        + later[1, far - 2, i, p].astype(F32)
                    ).astype(BF16)
                    pair_step(i, p).start()

        def all_step(way, step, i, p, late=0):
            hops = 2 if step == far else 1
            distance = far - 2 if step == far else step
            distance = distance + late * hops
            ref = coef.at[slot(-ways[way] * distance), piece(i, p)]
            return remote(
                ref, ref, all_send, ring_recv.at[way, step, i, p], on_ring(hops * ways[way])
            )

        with jax.named_scope("pair"):
            for i in triples:
                for p in ends:
                    pair_step(i, p).wait_recv()
                    coef[z, piece(i, p), :] = (
                        (sent[i, p].astype(F32) + other[i, p].astype(F32)) * scale
                    ).astype(BF16)
                    for way in ends:
                        all_step(way, 0, i, p).start()
        for step in range(1, far - 1):
            with jax.named_scope(f"all#s={step}"):
                for i in triples:
                    for p in ends:
                        for way in ends:
                            all_step(way, step - 1, i, p, 1).wait_recv()
                            all_step(way, step, i, p).start()
                            if step == far - 2 and p == way:
                                all_step(way, far, i, p).start()
            with jax.named_scope(f"synth#s={step}"):
                for owner in (0,) if step == 1 else (step - 1, 1 - step):
                    synthesised(slot(owner))
        with jax.named_scope("synth_last"):
            for owner in (far - 2, 2 - far):
                synthesised(slot(owner))
        with jax.named_scope("all_last"):
            for i in triples:
                for p in ends:
                    for way in ends:
                        all_step(way, far - 2, i, p, 1).wait_recv()
            for owner in (far - 1, 1 - far):
                synthesised(slot(owner))
            for i in triples:
                for way in ends:
                    all_step(way, far, i, way, 1).wait_recv()
        with jax.named_scope("synth_far"):
            synthesised(slot(far))
        most = pl.ds(0, ring - 1)
        remote(part.at[most], part.at[most], sum_send, own_sem, across).wait_send()
        remote(coef.at[most], coef.at[most], all_send, own_sem, across).wait_send()
        remote(sent, other, pair_send, own_sem, across).wait_send()

    @pl.when(core == 1)
    def _():
        owners = [far]
        for distance in range(far - 1, 0, -1):
            owners += [distance, -distance]
        owners.append(0)

        def mixed_sum(owner, i):
            k = owners.index(owner)
            return part[slot(owner), piece(i, line), :].astype(F32) + crossed[k, i].astype(F32)

        def taken(owner, turn):
            k = owners.index(owner)
            remote(
                crossed.at[k], crossed.at[k], pair_send, cross_recv.at[turn, k], across
            ).wait_recv()

        def sum_step(way, step, i):
            if step == 0:
                return sum_sent(sent.at[i, 0], first.at[way, i], way, 0, i, 0)
            source, target = staged.at[way, step - 1, i, 0], later.at[way, step - 1, i, 0]
            return sum_sent(source, target, way, step, i, 0)

        with jax.named_scope("first_part"):
            for k, owner in enumerate(owners):
                analysed(slot(owner))
                for i in triples:
                    remote(
                        part.at[slot(owner), piece(i, 1 - line)],
                        crossed.at[k, i],
                        pair_send,
                        cross_recv.at[0, k],
                        across,
                    ).start()
        with jax.named_scope("sum#s=0"):
            taken(far, 0)
            for i in triples:
                sent[i, 0] = mixed_sum(far, i).astype(BF16)
                sum_step(i % 2, 0, i).start()
        for step in range(1, far):
            with jax.named_scope(f"sum#s={step}"):
                for way in ends:
                    taken(ways[way] * (far - step), 0)
                for late in ends:
                    for i in triples:
                        for way in ends:
                            if late != (way == i % 2):
                                continue
                            total = mixed_sum(ways[way] * (far - step), i)
                            if step > 1 or late:
                                sum_step(way, step - 1, i).wait_recv()
                                come = first[way, i] if step == 1 else later[way, step - 2, i, 0]
                                total = total + come.astype(F32)
                            staged[way, step - 1, i, 0] = total.astype(BF16)
                            sum_step(way, step, i).start()

        def all_step(way, step, i, late=0):
            ref = coef.at[slot(-ways[way] * (step + late)), piece(i, line)]
            return remote(
                ref, ref, all_send, ring_recv.at[way, step, i, 0], on_ring(ways[way])
            )

        def shared(owner, i):
            ref = coef.at[slot(owner), piece(i, line)]
            k = owners.index(owner)
            return remote(ref, ref, pair_send, cross_recv.at[1, k], across)

        with jax.named_scope("last_sum"):
            taken(0, 0)
            for i in triples:
                for way in ends:
                    sum_step(way, far - 1, i).wait_recv()
                coef[z, piece(i, line), :] = (
                    (
                        mixed_sum(0, i)
                        + later[0, far - 2, i, 0].astype(F32)
                        + later[1, far - 2, i, 0].astype(F32)
                    )
                    * scale
                ).astype(BF16)
                for way in ends:
                    all_step(way, 0, i).start()
                shared(0, i).start()

        def ended(owner):
            taken(owner, 1)
            synthesised(slot(owner))

        for step in range(1, far):
            with jax.named_scope(f"all#s={step}"):
                for i in triples:
                    for way in ends:
                        all_step(way, step - 1, i, 1).wait_recv()
                        if step < far - 1 or way == i % 2:
                            all_step(way, step, i).start()
                        shared(-ways[way] * step, i).start()
            with jax.named_scope(f"synth#s={step}"):
                if step == 2:
                    ended(0)
                elif step == 3:
                    for way in ways:
                        ended(way)
        with jax.named_scope("all_last"):
            for i in triples:
                all_step(i % 2, far - 1, i, 1).wait_recv()
                shared(far, i).start()
        with jax.named_scope("synth_last"):
            for distance in range(2, far):
                for way in ways:
                    ended(way * distance)
            ended(far)
        most = pl.ds(0, ring - 1)
        remote(crossed.at[most], crossed.at[most], sum_send, own_sem, across).wait_send()
        remote(crossed.at[most], crossed.at[most], all_send, own_sem, across).wait_send()
        remote(coef, coef, pair_send, own_sem, across).wait_send()

    with jax.named_scope("back"):
        for g in range(cons):
            for s in range(2):
                both = [
                    rows[pl.ds(s * ring * full + p * cons + g, ring, stride=full), :] for p in range(2)
                ]
                back[2 * g + s] = jnp.concatenate(both, axis=0).astype(BF16)

    @pl.loop(0, peers - 1)
    def _(turn):
        exchange(outward(turn), back, out, back_send, back_recv).start()

    kept = pltpu.make_async_copy(back.at[me], out.at[me], own_sem)
    kept.start()

    with jax.named_scope("wait_sends"):
        kept.wait()

    with jax.named_scope("wait_back"):
        exchanged(back, out, back_send, back_recv).wait()


def middle(elevation, legendre, cycle_weight, love_factor, assignment):
    cons = lax.axis_size("cons")
    period = elevation.shape[-1]
    depth = legendre.shape[2]
    ring = 8
    far = ring // 2
    full = 2 * cons
    dma = pltpu.SemaphoreType.DMA
    vmem = pltpu.VMEM
    twiddle, basis = phase_tables(period)
    pieces = (2 * cons, 16, LANES)
    return pl.pallas_call(
        functools.partial(middle_kernel, ring, cons),
        out_shape=jax.ShapeDtypeStruct(pieces, BF16),
        in_specs=[pl.BlockSpec(memory_space=pltpu.HBM)] * 7,
        out_specs=pl.BlockSpec(memory_space=pltpu.HBM),
        scratch_shapes=[
            vmem((1, CYC, period), BF16),
            pltpu.SMEM((CYC,), F32),
            vmem((depth,), F32),
            pltpu.SMEM((cons,), jnp.int32),
            vmem(twiddle.shape, F32),
            vmem(basis.shape, BF16),
            vmem(pieces, BF16),
            vmem((RADIX // TRI * LANES, 2 * LANES), F32),
            vmem((RADIX // TRI * full, LANES), F32),
            vmem((2, CYC, TRI * ring, depth), BF16),
            vmem((depth // LANES, CYC * TRI * ring, LANES), F32),
            vmem((ring, 2 * LANES, depth), BF16),
            vmem(pieces, BF16),
            vmem((2 * cons * 16, LANES), F32),
            vmem((ring, full, 2 * LANES), F32),
            vmem((ring, TRI * full, depth), BF16),
            vmem((2, TRI, cons, depth), BF16),
            vmem((2, far - 1, TRI, 2, cons, depth), BF16),
            vmem((2, far - 1, TRI, 2, cons, depth), BF16),
            vmem((TRI, 2, cons, depth), BF16),
            vmem((TRI, 2, cons, depth), BF16),
            vmem((ring, TRI, cons, depth), BF16),
            vmem((ring, TRI * full, depth), BF16),
            vmem((2 * ring * full, LANES), F32),
            vmem(pieces, BF16),
            dma((6,)),
            dma,
            dma,
            dma,
            dma,
            dma,
            dma,
            dma,
            dma,
            dma((2, far + 1, TRI, 2)),
            dma((TRI, 2)),
            dma((2, ring)),
            dma,
            dma,
        ],
        compiler_params=pltpu.CompilerParams(
            collective_id=KERNEL_ID, has_side_effects=True, vmem_limit_bytes=67_000_000
        ),
        name="middle",
    )(
        elevation,
        legendre,
        cycle_weight,
        love_factor,
        assignment,
        jnp.asarray(twiddle),
        jnp.asarray(basis),
    )


def local(elevation, legendre, cycle_weight, love_factor, assignment):
    returned = middle(elevation, legendre, cycle_weight, love_factor, assignment)
    return inverse(returned, elevation.shape[-1])


def solution(mesh):
    placed = (P("cons", "blk", None), P("blk", "cons", None), P("blk"), P(), P())
    return jax.shard_map(
        local, mesh=mesh, in_specs=placed, out_specs=P("cons", "blk", None), check_vma=False
    )
```

```python
import functools
import math
import numpy as np
import jax
import jax.numpy as jnp
from jax import lax
from jax.experimental import pallas as pl
from jax.experimental.pallas import tpu as pltpu
from jax.sharding import PartitionSpec as P

RADIX = 48
LANES = 128
CYC = 40
TRI = 3


def by_phase(value, turn):
    re, im = value
    cos, sin = math.cos(2 * math.pi * turn), math.sin(2 * math.pi * turn)
    cos = 0.0 if abs(cos) < 1e-12 else cos
    sin = 0.0 if abs(sin) < 1e-12 else sin

    def scaled(array, factor):
        if array is None or factor == 0.0:
            return None
        if abs(factor - 1.0) < 1e-12:
            return array
        if abs(factor + 1.0) < 1e-12:
            return -array
        return array * np.float32(factor)

    return (
        added(scaled(re, cos), scaled(im, -sin)),
        added(scaled(re, sin), scaled(im, cos)),
    )


def added(a, b):
    if a is None:
        return b
    return a if b is None else a + b


def plus(a, b):
    return added(a[0], b[0]), added(a[1], b[1])


def conj(a):
    return a[0], None if a[1] is None else -a[1]


def at(half, index, length):
    index %= length
    return half[index] if 2 * index <= length else conj(half[length - index])


def factor_of(length):
    return 4 if length % 4 == 0 else (3 if length % 3 == 0 else 2)


def real_fft(values):
    n = len(values)
    if n == 1:
        return [(values[0], None)]
    p = factor_of(n)
    parts = [real_fft(values[i::p]) for i in range(p)]
    out = []
    for k in range(n // 2 + 1):
        total = at(parts[0], k, n // p)
        for i in range(1, p):
            total = plus(total, by_phase(at(parts[i], k, n // p), -i * k / n))
        out.append(total)
    return out


def real_inverse(half, n):
    if n == 1:
        return [half[0][0]]
    p = factor_of(n)
    short = n // p
    out = [None] * n
    for a in range(p):
        folded = []
        for r in range(short // 2 + 1):
            total = (None, None)
            for s in range(p):
                index = r + s * short
                total = plus(total, by_phase(at(half, index, n), index * a / n))
            if r == 0 or 2 * r == short:
                total = (total[0], None)
            folded.append(total)
        for kk, value in enumerate(real_inverse(folded, short)):
            out[p * kk + a] = value
    return out


def phase_tables(period):
    lane = np.arange(LANES)
    turn = np.arange(RADIX)[:, None] * lane[None, :] / period
    twiddle = np.stack([np.cos(2 * np.pi * turn), np.sin(2 * np.pi * turn)], 1)
    q = np.arange(period // RADIX // 8)[:, None] * lane[None, :] / LANES
    cos, sin = np.cos(2 * np.pi * q), np.sin(2 * np.pi * q)
    basis = np.concatenate([np.concatenate([cos, sin], 1), np.concatenate([-sin, cos], 1)], 0)
    return twiddle.reshape(2 * RADIX, LANES).astype(np.float32), basis.astype(jnp.bfloat16)


def transformed(x_ref, weight, twiddle_ref, basis_ref, out_ref, mixed, rows):
    cons = out_ref.shape[0] // 2
    for triple in range(RADIX // TRI):
        mixed[triple * LANES + TRI * CYC : (triple + 1) * LANES, :] = jnp.zeros(
            (LANES - TRI * CYC, 2 * LANES), jnp.float32
        )

    @pl.loop(0, CYC // 8)
    def _(group):
        lines = pl.ds(pl.multiple_of(group * 8, 8), 8)
        half = real_fft(
            [
                x_ref[0, lines, k * LANES : (k + 1) * LANES].astype(jnp.float32)
                for k in range(RADIX)
            ]
        )
        for r in range(RADIX):
            re, im = at(half, r, RADIX)
            cos, sin = twiddle_ref[2 * r : 2 * r + 1, :], twiddle_ref[2 * r + 1 : 2 * r + 2, :]
            if im is None:
                new_re, new_im = re * cos, -re * sin
            else:
                new_re, new_im = re * cos + im * sin, im * cos - re * sin
            start = (r // TRI) * LANES + (r % TRI) * CYC
            place = pl.ds(pl.multiple_of(start + group * 8, 8), 8)
            mixed[place, 0:LANES] = new_re
            mixed[place, LANES:] = new_im

    for triple in range(RADIX // TRI):
        block = mixed[triple * LANES : (triple + 1) * LANES, :].astype(jnp.bfloat16)
        got = lax.dot_general(
            basis_ref[...], block, (((1,), (1,)), ((), ())), preferred_element_type=jnp.float32
        )
        rows[triple * 2 * cons : (triple + 1) * 2 * cons, :] = got * weight
    for c in range(cons):
        for h in range(2):
            both = [
                rows[pl.ds(h * 16 * cons + p * cons + c, 8, stride=2 * cons), :] for p in range(2)
            ]
            out_ref[2 * c + h] = jnp.concatenate(both, axis=0).astype(jnp.bfloat16)


def inverse_kernel(
    z_hbm, twiddle_hbm, basis_hbm, out_hbm, z_ref, twiddle_ref, basis_ref, rows, mixed, done, sems, out_sems
):
    pairs = ((z_hbm, z_ref), (twiddle_hbm, twiddle_ref), (basis_hbm, basis_ref))
    loads = [
        pltpu.make_async_copy(source, target, sems.at[i])
        for i, (source, target) in enumerate(pairs)
    ]
    for load in loads:
        load.start()
    for load in loads:
        load.wait()
    cons = z_ref.shape[0] // 2
    for source in range(2 * cons):
        rows[source * 16 : (source + 1) * 16, :] = z_ref[source].astype(jnp.float32)
    for triple in range(RADIX // TRI):
        h, t = divmod(triple, 8)
        both = [rows[pl.ds(h * 16 + p * 8 + t, cons, stride=32), :] for p in range(2)]
        lines = jnp.concatenate(both, axis=0).T.astype(jnp.bfloat16)
        mixed[triple * LANES : (triple + 1) * LANES, :] = jnp.dot(
            lines, basis_ref[...], preferred_element_type=jnp.float32
        )

    def leave(group):
        lines = pl.ds(pl.multiple_of(group * 8, 8), 8)
        return pltpu.make_async_copy(done.at[group], out_hbm.at[0, lines], out_sems.at[group])

    @pl.loop(0, CYC // 8)
    def _(group):
        turned = []
        for r in range(RADIX):
            start = (r // TRI) * LANES + (r % TRI) * CYC
            place = pl.ds(pl.multiple_of(start + group * 8, 8), 8)
            re, im = mixed[place, 0:LANES], mixed[place, LANES:]
            cos, sin = twiddle_ref[2 * r : 2 * r + 1, :], twiddle_ref[2 * r + 1 : 2 * r + 2, :]
            turned.append((re * cos - im * sin, re * sin + im * cos))
        middle = RADIX // 2
        half = [(turned[0][0], None)]
        for r in range(1, middle):
            pair = plus(turned[r], conj(turned[RADIX - r]))
            half.append((pair[0] * np.float32(0.5), pair[1] * np.float32(0.5)))
        half.append((turned[middle][0], None))
        for k, value in enumerate(real_inverse(half, RADIX)):
            done[group, :, k * LANES : (k + 1) * LANES] = value
        leave(group).start()

    @pl.loop(0, CYC // 8)
    def _(group):
        leave(group).wait()


def inverse(pieces, period):
    cons = pieces.shape[0] // 2
    twiddle, basis = phase_tables(period)
    return pl.pallas_call(
        inverse_kernel,
        out_shape=jax.ShapeDtypeStruct((1, CYC, period), jnp.float32),
        in_specs=[pl.BlockSpec(memory_space=pltpu.HBM)] * 3,
        out_specs=pl.BlockSpec(memory_space=pltpu.HBM),
        scratch_shapes=[
            pltpu.VMEM(pieces.shape, jnp.bfloat16),
            pltpu.VMEM(twiddle.shape, jnp.float32),
            pltpu.VMEM(basis.shape, jnp.bfloat16),
            pltpu.VMEM((2 * cons * 16, LANES), jnp.float32),
            pltpu.VMEM((RADIX // TRI * LANES, 2 * LANES), jnp.float32),
            pltpu.VMEM((CYC // 8, 8, period), jnp.float32),
            pltpu.SemaphoreType.DMA((3,)),
            pltpu.SemaphoreType.DMA((CYC // 8,)),
        ],
        compiler_params=pltpu.CompilerParams(vmem_limit_bytes=67_000_000),
        name="inverse",
    )(pieces, jnp.asarray(twiddle), jnp.asarray(basis))


MESH = pl.DeviceIdType.MESH
F32 = jnp.float32
BF16 = jnp.bfloat16
KERNEL_ID = 0


def middle_kernel(
    ring, cons, elevation, legendre, cycle_weight, love_factor, assigned, twiddles, bases, out,
    height, weights, love, assignment, twiddle, basis, pieces, spun, spread,
    held, wide, table, got, mixed, lines, part, first, later, staged, sent, other, crossed, coef,
    rows, back,
    own_sem, swap_send, swap_recv, out_send, out_recv, sum_send, pair_send, all_send,
    ring_recv, cross_recv, back_send, back_recv,
):
    c, b = lax.axis_index("cons"), lax.axis_index("blk")
    core = lax.rem(b, 2)
    z = lax.rem(b // 2, ring)
    line = b // (2 * ring)
    chip = b - core
    me = 2 * c + core
    peers = 2 * cons
    far = ring // 2
    depth = legendre.shape[2]
    half_orders = TRI * ring
    full = 2 * cons
    barrier = pltpu.get_barrier_semaphore()

    def slot(offset):
        return lax.rem(z + offset + ring, ring)

    def on_ring(offset):
        return (c, line * 2 * ring + slot(offset) * 2 + core)

    outward = sorted(range(1, peers), key=lambda offset: abs(offset - peers // 2))

    def remote(source, target, send, recv, device):
        return pltpu.make_async_remote_copy(
            src_ref=source,
            dst_ref=target,
            send_sem=send,
            recv_sem=recv,
            device_id=device,
            device_id_type=MESH,
        )

    def exchange(offset, source, landing, send, recv):
        index = lax.rem(me + offset, peers)
        there = (index // 2, chip + lax.rem(index, 2))
        return remote(source.at[index], landing.at[me], send, recv, there)

    def exchanged(source, landing, send, recv):
        rest = pl.ds(0, peers - 1)
        return remote(source.at[rest], landing.at[rest], send, recv, (c, chip + 1 - core))

    across = (c, (1 - line) * 2 * ring + z * 2 + core)

    def half_of(which):
        return legendre.at[:, pl.ds(pl.multiple_of(which * half_orders, 8), half_orders), :]

    mine = pltpu.make_async_copy(half_of(core), held.at[core], own_sem)
    pairs = (
        (elevation, height),
        (twiddles, twiddle),
        (bases, basis),
        (cycle_weight, weights),
        (assigned, assignment),
        (love_factor, love),
    )
    loads = [
        pltpu.make_async_copy(source, target, cross_recv.at[1, i])
        for i, (source, target) in enumerate(pairs)
    ]
    with jax.named_scope("signals"):
        for load in loads:
            load.start()

        for offset in outward:
            index = lax.rem(me + offset, peers)
            there = (index // 2, chip + lax.rem(index, 2))
            pl.semaphore_signal(barrier, inc=1, device_id=there, device_id_type=MESH)

        for target in (on_ring(1), on_ring(-1), on_ring(2), on_ring(-2), across):
            pl.semaphore_signal(barrier, inc=1, device_id=target, device_id_type=MESH)
        mine.start()
    with jax.named_scope("loads"):
        for load in loads:
            load.wait()

    with jax.named_scope("fft"):
        lane_of = lax.broadcasted_iota(jnp.int32, (1, LANES), 1)
        day = lane_of - jnp.where(lane_of < CYC, 0, jnp.where(lane_of < 2 * CYC, CYC, 2 * CYC))
        weight = jnp.zeros((1, LANES), F32)
        for j in range(CYC):
            weight = jnp.where(day == j, weights[j], weight)
        transformed(height, weight, twiddle, basis, pieces, spun, spread)

    with jax.named_scope("barrier"):
        pl.semaphore_wait(barrier, peers + 4)

    swap = remote(half_of(1 - core), held.at[core], swap_send, swap_recv, (c, chip + 1 - core))
    swap.start()

    for offset in outward:
        exchange(offset, pieces, got, out_send, out_recv).start()

    got[me] = pieces[me]

    def turn(which):
        @pl.loop(0, CYC)
        def _(j):
            place = pl.ds(pl.multiple_of(j * half_orders, 8), half_orders)
            for tile in range(depth // LANES):
                wide[tile, place, :] = held[
                    which, j, :, tile * LANES : (tile + 1) * LANES
                ].astype(F32)

        @pl.loop(0, ring)
        def _(t):
            place = pl.ds(pl.multiple_of(which * LANES, LANES), LANES)
            for tile in range(depth // LANES):
                taken = [
                    wide[tile, pl.ds(TRI * t + i, CYC, stride=half_orders), :] for i in range(TRI)
                ]
                taken.append(jnp.zeros((LANES - TRI * CYC, LANES), F32))
                table[t, place, tile * LANES : (tile + 1) * LANES] = jnp.concatenate(
                    taken, axis=0
                ).astype(BF16)

    with jax.named_scope("turn_own"):
        mine.wait()
        turn(core)
    with jax.named_scope("swap_wait"):
        swap.wait()
    with jax.named_scope("turn_other"):
        turn(1 - core)

    with jax.named_scope("wait_out"):
        exchanged(pieces, got, out_send, out_recv).wait()

    with jax.named_scope("lines"):
        for g in range(cons):
            field = assignment[g]
            for s in range(2):
                mixed[(s * cons + g) * 16 : (s * cons + g + 1) * 16, :] = got[2 * field + s].astype(F32)
        for t in range(ring):
            for s in range(2):
                for p in range(2):
                    lines[t, p * cons : (p + 1) * cons, s * LANES : (s + 1) * LANES] = mixed[
                        pl.ds(s * cons * 16 + p * 8 + t, cons, stride=16), :
                    ]

    lane = lax.broadcasted_iota(jnp.int32, (full, 2 * LANES), 1)
    lane = jnp.where(lane >= LANES, lane - LANES, lane)
    which = jnp.where(lane < CYC, 0, jnp.where(lane < 2 * CYC, 1, jnp.where(lane < TRI * CYC, 2, 3)))

    def analysed(t):
        x = lines[t]
        left = [jnp.where(which == i, x, 0.0) for i in range(TRI)]
        part[t] = jnp.dot(
            jnp.concatenate(left, axis=0).astype(BF16), table[t], preferred_element_type=F32
        ).astype(BF16)

    def piece(i, p):
        return pl.ds(pl.multiple_of(i * full + p * cons, cons), cons)

    ways, triples, ends = (1, -1), range(TRI), range(2)
    scale = love[...].reshape(1, depth)

    def synthesised(t):
        got_all = lax.dot_general(
            coef[t], table[t], (((1,), (1,)), ((), ())), preferred_element_type=F32
        )
        chosen = jnp.where(
            which == 0,
            got_all[:full],
            jnp.where(which == 1, got_all[full : 2 * full], got_all[2 * full :]),
        )
        order = which + (TRI * t + core * half_orders + c * 2 * half_orders)
        chosen = chosen * jnp.where(order == 0, 1.0, 2.0).astype(F32)
        for s in range(2):
            place = pl.ds(pl.multiple_of(s * ring * full + t * full, 8), full)
            rows[place, :] = chosen[:, s * LANES : (s + 1) * LANES]

    def sum_sent(source, target, way, step, i, p, hops=1):
        return remote(
            source, target, sum_send, ring_recv.at[way, step, i, p], on_ring(hops * ways[way])
        )

    @pl.when(core == 0)
    def _():
        def sum_step(way, step, i, p):
            if step == 0:
                source = part.at[slot(far), piece(i, p)]
                return sum_sent(source, first.at[way, i], way, step, i, p, 2)
            target = later.at[way, step - 1, i, p]
            if step == 1:
                source = part.at[slot(ways[way] * (far - 1)), piece(i, p)]
            else:
                source = staged.at[way, step - 1, i, p]
            return sum_sent(source, target, way, step, i, p)

        with jax.named_scope("first_part"):
            analysed(slot(far))
            for i in triples:
                for way in ends:
                    sum_step(way, 0, i, way).start()
            for way in ends:
                analysed(slot(ways[way] * (far - 1)))
                for i in triples:
                    for p in (1 - way, way):
                        sum_step(way, 1, i, p).start()
            for step in range(2, far):
                for way in ends:
                    analysed(slot(ways[way] * (far - step)))
            analysed(z)
        for step in range(2, far):
            with jax.named_scope(f"sum#s={step}"):
                for i in triples:
                    for late in ends:
                        for way in ends:
                            p = way if late else 1 - way
                            owner = slot(ways[way] * (far - step))
                            sum_step(way, step - 1, i, p).wait_recv()
                            total = part[owner, piece(i, p), :].astype(F32) + later[
                                way, step - 2, i, p
                            ].astype(F32)
                            if step == 2 and late:
                                sum_step(way, 0, i, p).wait_recv()
                                total = total + first[way, i].astype(F32)
                            staged[way, step - 1, i, p] = total.astype(BF16)
                            sum_step(way, step, i, p).start()

        def pair_step(i, p):
            return remote(
                sent.at[i, p], other.at[i, p], pair_send, cross_recv.at[0, 2 * i + p], across
            )

        with jax.named_scope("last_sum"):
            for i in triples:
                for p in ends:
                    for way in ends:
                        sum_step(way, far - 1, i, p).wait_recv()
                    sent[i, p] = (
                        part[z, piece(i, p), :].astype(F32)
                        + later[0, far - 2, i, p].astype(F32)
                        + later[1, far - 2, i, p].astype(F32)
                    ).astype(BF16)
                    pair_step(i, p).start()

        def all_step(way, step, i, p, late=0):
            hops = 2 if step == far else 1
            distance = far - 2 if step == far else step
            distance = distance + late * hops
            ref = coef.at[slot(-ways[way] * distance), piece(i, p)]
            if step == far:
                recv = cross_recv.at[1, TRI * way + i]
            else:
                recv = ring_recv.at[way, step, i, p]
            return remote(ref, ref, all_send, recv, on_ring(hops * ways[way]))

        with jax.named_scope("pair"):
            for i in triples:
                for p in ends:
                    pair_step(i, p).wait_recv()
                    coef[z, piece(i, p), :] = (
                        (sent[i, p].astype(F32) + other[i, p].astype(F32)) * scale
                    ).astype(BF16)
                    for way in ends:
                        all_step(way, 0, i, p).start()
        for step in range(1, far - 1):
            with jax.named_scope(f"all#s={step}"):
                for i in triples:
                    for p in ends:
                        for way in ends:
                            all_step(way, step - 1, i, p, 1).wait_recv()
                            all_step(way, step, i, p).start()
                            if step == far - 2 and p == way:
                                all_step(way, far, i, p).start()
            with jax.named_scope(f"synth#s={step}"):
                for owner in (0,) if step == 1 else (step - 1, 1 - step):
                    synthesised(slot(owner))
        with jax.named_scope("synth_last"):
            for owner in (far - 2, 2 - far):
                synthesised(slot(owner))
        with jax.named_scope("all_last"):
            for i in triples:
                for p in ends:
                    for way in ends:
                        all_step(way, far - 2, i, p, 1).wait_recv()
            for owner in (far - 1, 1 - far):
                synthesised(slot(owner))
            for i in triples:
                for way in ends:
                    all_step(way, far, i, way, 1).wait_recv()
        with jax.named_scope("synth_far"):
            synthesised(slot(far))
        most = pl.ds(0, ring - 1)
        remote(part.at[most], part.at[most], sum_send, own_sem, across).wait_send()
        remote(coef.at[most], coef.at[most], all_send, own_sem, across).wait_send()
        remote(sent, other, pair_send, own_sem, across).wait_send()

    @pl.when(core == 1)
    def _():
        owners = [far]
        for distance in range(far - 1, 0, -1):
            owners += [distance, -distance]
        owners.append(0)

        def mixed_sum(owner, i):
            k = owners.index(owner)
            return part[slot(owner), piece(i, line), :].astype(F32) + crossed[k, i].astype(F32)

        def taken(owner, turn):
            k = owners.index(owner)
            remote(
                crossed.at[k], crossed.at[k], pair_send, cross_recv.at[turn, k], across
            ).wait_recv()

        def sum_step(way, step, i):
            if step == 0:
                return sum_sent(sent.at[i, 0], first.at[way, i], way, 0, i, 0)
            source, target = staged.at[way, step - 1, i, 0], later.at[way, step - 1, i, 0]
            return sum_sent(source, target, way, step, i, 0)

        with jax.named_scope("first_part"):
            for k, owner in enumerate(owners):
                analysed(slot(owner))
                for i in triples:
                    remote(
                        part.at[slot(owner), piece(i, 1 - line)],
                        crossed.at[k, i],
                        pair_send,
                        cross_recv.at[0, k],
                        across,
                    ).start()
        with jax.named_scope("sum#s=0"):
            taken(far, 0)
            for i in triples:
                sent[i, 0] = mixed_sum(far, i).astype(BF16)
                sum_step(i % 2, 0, i).start()
        for step in range(1, far):
            with jax.named_scope(f"sum#s={step}"):
                for way in ends:
                    taken(ways[way] * (far - step), 0)
                for late in ends:
                    for i in triples:
                        for way in ends:
                            if late != (way == i % 2):
                                continue
                            total = mixed_sum(ways[way] * (far - step), i)
                            if step > 1 or late:
                                sum_step(way, step - 1, i).wait_recv()
                                come = first[way, i] if step == 1 else later[way, step - 2, i, 0]
                                total = total + come.astype(F32)
                            staged[way, step - 1, i, 0] = total.astype(BF16)
                            sum_step(way, step, i).start()

        def all_step(way, step, i, late=0):
            ref = coef.at[slot(-ways[way] * (step + late)), piece(i, line)]
            return remote(
                ref, ref, all_send, ring_recv.at[way, step, i, 0], on_ring(ways[way])
            )

        def shared(owner, i):
            ref = coef.at[slot(owner), piece(i, line)]
            k = owners.index(owner)
            return remote(ref, ref, pair_send, cross_recv.at[1, k], across)

        with jax.named_scope("last_sum"):
            taken(0, 0)
            for i in triples:
                for way in ends:
                    sum_step(way, far - 1, i).wait_recv()
                coef[z, piece(i, line), :] = (
                    (
                        mixed_sum(0, i)
                        + later[0, far - 2, i, 0].astype(F32)
                        + later[1, far - 2, i, 0].astype(F32)
                    )
                    * scale
                ).astype(BF16)
                for way in ends:
                    all_step(way, 0, i).start()
                shared(0, i).start()

        def ended(owner):
            taken(owner, 1)
            synthesised(slot(owner))

        for step in range(1, far):
            with jax.named_scope(f"all#s={step}"):
                for i in triples:
                    for way in ends:
                        all_step(way, step - 1, i, 1).wait_recv()
                        if step < far - 1 or way == i % 2:
                            all_step(way, step, i).start()
                        shared(-ways[way] * step, i).start()
            with jax.named_scope(f"synth#s={step}"):
                if step == 2:
                    ended(0)
                elif step == 3:
                    for way in ways:
                        ended(way)
        with jax.named_scope("all_last"):
            for i in triples:
                all_step(i % 2, far - 1, i, 1).wait_recv()
                shared(far, i).start()
        with jax.named_scope("synth_last"):
            for distance in range(2, far):
                for way in ways:
                    ended(way * distance)
            ended(far)
        most = pl.ds(0, ring - 1)
        remote(crossed.at[most], crossed.at[most], sum_send, own_sem, across).wait_send()
        remote(crossed.at[most], crossed.at[most], all_send, own_sem, across).wait_send()
        remote(coef, coef, pair_send, own_sem, across).wait_send()

    with jax.named_scope("back"):
        for g in range(cons):
            for s in range(2):
                both = [
                    rows[pl.ds(s * ring * full + p * cons + g, ring, stride=full), :] for p in range(2)
                ]
                back[2 * g + s] = jnp.concatenate(both, axis=0).astype(BF16)

    for offset in outward:
        exchange(offset, back, out, back_send, back_recv).start()

    kept = pltpu.make_async_copy(back.at[me], out.at[me], own_sem)
    kept.start()

    with jax.named_scope("wait_sends"):
        kept.wait()

    with jax.named_scope("wait_back"):
        exchanged(back, out, back_send, back_recv).wait()


def middle(elevation, legendre, cycle_weight, love_factor, assignment):
    cons = lax.axis_size("cons")
    period = elevation.shape[-1]
    depth = legendre.shape[2]
    ring = 8
    far = ring // 2
    full = 2 * cons
    dma = pltpu.SemaphoreType.DMA
    vmem = pltpu.VMEM
    twiddle, basis = phase_tables(period)
    pieces = (2 * cons, 16, LANES)
    return pl.pallas_call(
        functools.partial(middle_kernel, ring, cons),
        out_shape=jax.ShapeDtypeStruct(pieces, BF16),
        in_specs=[pl.BlockSpec(memory_space=pltpu.HBM)] * 7,
        out_specs=pl.BlockSpec(memory_space=pltpu.HBM),
        scratch_shapes=[
            vmem((1, CYC, period), BF16),
            pltpu.SMEM((CYC,), F32),
            vmem((depth,), F32),
            pltpu.SMEM((cons,), jnp.int32),
            vmem(twiddle.shape, F32),
            vmem(basis.shape, BF16),
            vmem(pieces, BF16),
            vmem((RADIX // TRI * LANES, 2 * LANES), F32),
            vmem((RADIX // TRI * full, LANES), F32),
            vmem((2, CYC, TRI * ring, depth), BF16),
            vmem((depth // LANES, CYC * TRI * ring, LANES), F32),
            vmem((ring, 2 * LANES, depth), BF16),
            vmem(pieces, BF16),
            vmem((2 * cons * 16, LANES), F32),
            vmem((ring, full, 2 * LANES), F32),
            vmem((ring, TRI * full, depth), BF16),
            vmem((2, TRI, cons, depth), BF16),
            vmem((2, far - 1, TRI, 2, cons, depth), BF16),
            vmem((2, far - 1, TRI, 2, cons, depth), BF16),
            vmem((TRI, 2, cons, depth), BF16),
            vmem((TRI, 2, cons, depth), BF16),
            vmem((ring, TRI, cons, depth), BF16),
            vmem((ring, TRI * full, depth), BF16),
            vmem((2 * ring * full, LANES), F32),
            vmem(pieces, BF16),
            dma,
            dma,
            dma,
            dma,
            dma,
            dma,
            dma,
            dma,
            dma((2, far, TRI, 2)),
            dma((2, ring)),
            dma,
            dma,
        ],
        compiler_params=pltpu.CompilerParams(
            collective_id=KERNEL_ID, has_side_effects=True, vmem_limit_bytes=67_000_000
        ),
        name="middle",
    )(
        elevation,
        legendre,
        cycle_weight,
        love_factor,
        assignment,
        jnp.asarray(twiddle),
        jnp.asarray(basis),
    )


def local(elevation, legendre, cycle_weight, love_factor, assignment):
    returned = middle(elevation, legendre, cycle_weight, love_factor, assignment)
    return inverse(returned, elevation.shape[-1])


def solution(mesh):
    placed = (P("cons", "blk", None), P("blk", "cons", None), P("blk"), P(), P())
    return jax.shard_map(
        local, mesh=mesh, in_specs=placed, out_specs=P("cons", "blk", None), check_vma=False
    )
```

```python
import functools
import math
import numpy as np
import jax
import jax.numpy as jnp
from jax import lax
from jax.experimental import pallas as pl
from jax.experimental.pallas import tpu as pltpu
from jax.sharding import PartitionSpec as P

RADIX = 48
LANES = 128
CYC = 40
TRI = 3


def by_phase(value, turn):
    re, im = value
    cos, sin = math.cos(2 * math.pi * turn), math.sin(2 * math.pi * turn)
    cos = 0.0 if abs(cos) < 1e-12 else cos
    sin = 0.0 if abs(sin) < 1e-12 else sin

    def scaled(array, factor):
        if array is None or factor == 0.0:
            return None
        if abs(factor - 1.0) < 1e-12:
            return array
        if abs(factor + 1.0) < 1e-12:
            return -array
        return array * np.float32(factor)

    return (
        added(scaled(re, cos), scaled(im, -sin)),
        added(scaled(re, sin), scaled(im, cos)),
    )


def added(a, b):
    if a is None:
        return b
    return a if b is None else a + b


def plus(a, b):
    return added(a[0], b[0]), added(a[1], b[1])


def conj(a):
    return a[0], None if a[1] is None else -a[1]


def at(half, index, length):
    index %= length
    return half[index] if 2 * index <= length else conj(half[length - index])


def minus(a, b):
    return plus(a, negated(b))


def negated(a):
    return tuple(None if part is None else -part for part in a)


def turned_left(a):
    re, im = a
    return None if im is None else -im, re


def factor_of(length):
    return 4 if length % 4 == 0 else (3 if length % 3 == 0 else 2)


def short_dft(values, sign):
    n = len(values)
    if n != 4:
        out = []
        for k in range(n):
            total = values[0]
            for i in range(1, n):
                total = plus(total, by_phase(values[i], sign * i * k / n))
            out.append(total)
        return out
    even, odd = plus(values[0], values[2]), plus(values[1], values[3])
    even_gap, odd_gap = minus(values[0], values[2]), turned_left(minus(values[1], values[3]))
    ahead, behind = plus(even_gap, odd_gap), minus(even_gap, odd_gap)
    if sign < 0:
        ahead, behind = behind, ahead
    return [plus(even, odd), ahead, minus(even, odd), behind]


def real_fft(values):
    n = len(values)
    if n == 1:
        return [(values[0], None)]
    p = factor_of(n)
    short = n // p
    parts = [real_fft(values[i::p]) for i in range(p)]
    out = [None] * n
    for k in range(short):
        if k > n // 2:
            continue
        spun = [by_phase(at(parts[i], k, short), -i * k / n) for i in range(p)]
        for s, value in enumerate(short_dft(spun, -1)):
            out[k + s * short] = value
    half = out[: n // 2 + 1]
    half[0] = (half[0][0], None)
    if n % 2 == 0:
        half[-1] = (half[-1][0], None)
    return half


def real_inverse(half, n):
    if n == 1:
        return [half[0][0]]
    if n == 3:
        base, (re, im) = half[0][0], half[1]
        middle = base - re
        side = im * np.float32(math.sqrt(3.0))
        return [base + (re + re), middle - side, middle + side]
    p = factor_of(n)
    short = n // p
    folded = [[None] * (short // 2 + 1) for _ in range(p)]
    for r in range(short // 2 + 1):
        mixed = short_dft([at(half, r + s * short, n) for s in range(p)], 1)
        for a in range(p):
            total = by_phase(mixed[a], r * a / n)
            if r == 0 or 2 * r == short:
                total = (total[0], None)
            folded[a][r] = total
    out = [None] * n
    for a in range(p):
        for kk, value in enumerate(real_inverse(folded[a], short)):
            out[p * kk + a] = value
    return out


def phase_tables(period):
    lane = np.arange(LANES)
    turn = np.arange(RADIX)[:, None] * lane[None, :] / period
    twiddle = np.stack([np.cos(2 * np.pi * turn), np.sin(2 * np.pi * turn)], 1)
    q = np.arange(period // RADIX // 8)[:, None] * lane[None, :] / LANES
    cos, sin = np.cos(2 * np.pi * q), np.sin(2 * np.pi * q)
    basis = np.concatenate([np.concatenate([cos, sin], 1), np.concatenate([-sin, cos], 1)], 0)
    return twiddle.reshape(2 * RADIX, LANES).astype(np.float32), basis.astype(jnp.bfloat16)


def transformed(x_ref, weight, twiddle_ref, basis_ref, out_ref, mixed, rows):
    cons = out_ref.shape[0] // 2
    for triple in range(RADIX // TRI):
        mixed[triple * LANES + TRI * CYC : (triple + 1) * LANES, :] = jnp.zeros(
            (LANES - TRI * CYC, 2 * LANES), jnp.float32
        )

    @pl.loop(0, CYC // 8)
    def _(group):
        lines = pl.ds(pl.multiple_of(group * 8, 8), 8)
        half = real_fft(
            [
                x_ref[0, lines, k * LANES : (k + 1) * LANES].astype(jnp.float32)
                for k in range(RADIX)
            ]
        )
        for r in range(RADIX):
            re, im = at(half, r, RADIX)
            cos, sin = twiddle_ref[2 * r : 2 * r + 1, :], twiddle_ref[2 * r + 1 : 2 * r + 2, :]
            if im is None:
                new_re, new_im = re * cos, -re * sin
            else:
                new_re, new_im = re * cos + im * sin, im * cos - re * sin
            start = (r // TRI) * LANES + (r % TRI) * CYC
            place = pl.ds(pl.multiple_of(start + group * 8, 8), 8)
            mixed[place, 0:LANES] = new_re
            mixed[place, LANES:] = new_im

    for triple in range(RADIX // TRI):
        block = mixed[triple * LANES : (triple + 1) * LANES, :].astype(jnp.bfloat16)
        got = lax.dot_general(
            basis_ref[...], block, (((1,), (1,)), ((), ())), preferred_element_type=jnp.float32
        )
        rows[triple * 2 * cons : (triple + 1) * 2 * cons, :] = got * weight
    for c in range(cons):
        for h in range(2):
            both = [
                rows[pl.ds(h * 16 * cons + p * cons + c, 8, stride=2 * cons), :] for p in range(2)
            ]
            out_ref[2 * c + h] = jnp.concatenate(both, axis=0).astype(jnp.bfloat16)


def inverse_kernel(
    z_hbm, twiddle_hbm, basis_hbm, out_hbm, z_ref, twiddle_ref, basis_ref, rows, mixed, done, sems, out_sems
):
    pairs = ((z_hbm, z_ref), (twiddle_hbm, twiddle_ref), (basis_hbm, basis_ref))
    loads = [
        pltpu.make_async_copy(source, target, sems.at[i])
        for i, (source, target) in enumerate(pairs)
    ]
    for load in loads:
        load.start()
    for load in loads:
        load.wait()
    cons = z_ref.shape[0] // 2
    for source in range(2 * cons):
        rows[source * 16 : (source + 1) * 16, :] = z_ref[source].astype(jnp.float32)
    for triple in range(RADIX // TRI):
        h, t = divmod(triple, 8)
        both = [rows[pl.ds(h * 16 + p * 8 + t, cons, stride=32), :] for p in range(2)]
        lines = jnp.concatenate(both, axis=0).T.astype(jnp.bfloat16)
        mixed[triple * LANES : (triple + 1) * LANES, :] = jnp.dot(
            lines, basis_ref[...], preferred_element_type=jnp.float32
        )

    def leave(group):
        lines = pl.ds(pl.multiple_of(group * 8, 8), 8)
        return pltpu.make_async_copy(done.at[group], out_hbm.at[0, lines], out_sems.at[group])

    @pl.loop(0, CYC // 8)
    def _(group):
        turned = []
        for r in range(RADIX):
            start = (r // TRI) * LANES + (r % TRI) * CYC
            place = pl.ds(pl.multiple_of(start + group * 8, 8), 8)
            re, im = mixed[place, 0:LANES], mixed[place, LANES:]
            cos, sin = twiddle_ref[2 * r : 2 * r + 1, :], twiddle_ref[2 * r + 1 : 2 * r + 2, :]
            turned.append((re * cos - im * sin, re * sin + im * cos))
        middle = RADIX // 2
        half = [(turned[0][0] + turned[0][0], None)]
        for r in range(1, middle):
            pair = plus(turned[r], conj(turned[RADIX - r]))
            half.append(pair)
        half.append((turned[middle][0] + turned[middle][0], None))
        for k, value in enumerate(real_inverse(half, RADIX)):
            done[group, :, k * LANES : (k + 1) * LANES] = value
        leave(group).start()

    @pl.loop(0, CYC // 8)
    def _(group):
        leave(group).wait()


def inverse(pieces, period):
    cons = pieces.shape[0] // 2
    twiddle, basis = phase_tables(period)
    twiddle = twiddle * np.float32(0.5)
    return pl.pallas_call(
        inverse_kernel,
        out_shape=jax.ShapeDtypeStruct((1, CYC, period), jnp.float32),
        in_specs=[pl.BlockSpec(memory_space=pltpu.HBM)] * 3,
        out_specs=pl.BlockSpec(memory_space=pltpu.HBM),
        scratch_shapes=[
            pltpu.VMEM(pieces.shape, jnp.bfloat16),
            pltpu.VMEM(twiddle.shape, jnp.float32),
            pltpu.VMEM(basis.shape, jnp.bfloat16),
            pltpu.VMEM((2 * cons * 16, LANES), jnp.float32),
            pltpu.VMEM((RADIX // TRI * LANES, 2 * LANES), jnp.float32),
            pltpu.VMEM((CYC // 8, 8, period), jnp.float32),
            pltpu.SemaphoreType.DMA((3,)),
            pltpu.SemaphoreType.DMA((CYC // 8,)),
        ],
        compiler_params=pltpu.CompilerParams(vmem_limit_bytes=67_000_000),
        name="inverse",
    )(pieces, jnp.asarray(twiddle), jnp.asarray(basis))


MESH = pl.DeviceIdType.MESH
F32 = jnp.float32
BF16 = jnp.bfloat16
KERNEL_ID = 0


def middle_kernel(
    ring, cons, elevation, legendre, cycle_weight, love_factor, assigned, twiddles, bases, out,
    height, weights, love, assignment, twiddle, basis, pieces, spun, spread,
    held, wide, table, got, mixed, lines, part, first, later, staged, sent, other, crossed, coef,
    rows, back,
    own_sem, swap_send, swap_recv, out_send, out_recv, sum_send, pair_send, all_send,
    ring_recv, cross_recv, back_send, back_recv,
):
    c, b = lax.axis_index("cons"), lax.axis_index("blk")
    core = lax.rem(b, 2)
    z = lax.rem(b // 2, ring)
    line = b // (2 * ring)
    chip = b - core
    me = 2 * c + core
    peers = 2 * cons
    far = ring // 2
    depth = legendre.shape[2]
    half_orders = TRI * ring
    full = 2 * cons
    barrier = pltpu.get_barrier_semaphore()

    slots = {offset: lax.rem(z + offset + ring, ring) for offset in range(-far, far + 1)}
    row_start = line * 2 * ring + core
    near = {hops: (c, row_start + 2 * slots[hops]) for hops in (1, -1, 2, -2)}

    def slot(offset):
        return slots[offset]

    def on_ring(offset):
        return near[offset]

    outward = sorted(range(1, peers), key=lambda offset: abs(offset - peers // 2))

    def remote(source, target, send, recv, device):
        return pltpu.make_async_remote_copy(
            src_ref=source,
            dst_ref=target,
            send_sem=send,
            recv_sem=recv,
            device_id=device,
            device_id_type=MESH,
        )

    def peer(offset):
        if offset % 2:
            return lax.rem(c + core + offset // 2, cons), 1 - core
        return lax.rem(c + offset // 2, cons), core

    def exchange(offset, source, landing, send, recv):
        far_c, far_core = peer(offset)
        there = (far_c, chip + far_core)
        return remote(source.at[2 * far_c + far_core], landing.at[me], send, recv, there)

    def exchanged(source, landing, send, recv):
        rest = pl.ds(0, peers - 1)
        return remote(source.at[rest], landing.at[rest], send, recv, (c, chip + 1 - core))

    across = (c, (1 - line) * 2 * ring + z * 2 + core)
    mine_rows = [pl.ds(pl.multiple_of(i * full + line * cons, cons), cons) for i in range(TRI)]
    other_rows = [
        pl.ds(pl.multiple_of(i * full + (1 - line) * cons, cons), cons) for i in range(TRI)
    ]

    def half_of(which):
        return legendre.at[:, pl.ds(pl.multiple_of(which * half_orders, 8), half_orders), :]

    mine = pltpu.make_async_copy(half_of(core), held.at[core], own_sem)
    pairs = (
        (elevation, height),
        (twiddles, twiddle),
        (bases, basis),
        (cycle_weight, weights),
        (assigned, assignment),
        (love_factor, love),
    )
    loads = [
        pltpu.make_async_copy(source, target, cross_recv.at[1, i])
        for i, (source, target) in enumerate(pairs)
    ]
    with jax.named_scope("signals"):
        for load in loads:
            load.start()

        for offset in outward:
            far_c, far_core = peer(offset)
            there = (far_c, chip + far_core)
            pl.semaphore_signal(barrier, inc=1, device_id=there, device_id_type=MESH)

        for target in (on_ring(1), on_ring(-1), on_ring(2), on_ring(-2), across):
            pl.semaphore_signal(barrier, inc=1, device_id=target, device_id_type=MESH)
        mine.start()
    with jax.named_scope("loads"):
        for load in loads:
            load.wait()

    with jax.named_scope("fft"):
        lane_of = lax.broadcasted_iota(jnp.int32, (1, LANES), 1)
        day = lane_of - jnp.where(lane_of < CYC, 0, jnp.where(lane_of < 2 * CYC, CYC, 2 * CYC))
        weight = jnp.zeros((1, LANES), F32)
        for j in range(CYC):
            weight = jnp.where(day == j, weights[j], weight)
        transformed(height, weight, twiddle, basis, pieces, spun, spread)

    with jax.named_scope("barrier"):
        pl.semaphore_wait(barrier, peers + 4)

    swap = remote(half_of(1 - core), held.at[core], swap_send, swap_recv, (c, chip + 1 - core))
    swap.start()

    for offset in outward:
        exchange(offset, pieces, got, out_send, out_recv).start()

    got[me] = pieces[me]

    def turn(which):
        @pl.loop(0, CYC)
        def _(j):
            place = pl.ds(pl.multiple_of(j * half_orders, 8), half_orders)
            for tile in range(depth // LANES):
                wide[tile, place, :] = held[
                    which, j, :, tile * LANES : (tile + 1) * LANES
                ].astype(F32)

        @pl.loop(0, ring)
        def _(t):
            place = pl.ds(pl.multiple_of(which * LANES, LANES), LANES)
            for tile in range(depth // LANES):
                taken = [
                    wide[tile, pl.ds(TRI * t + i, CYC, stride=half_orders), :] for i in range(TRI)
                ]
                taken.append(jnp.zeros((LANES - TRI * CYC, LANES), F32))
                table[t, place, tile * LANES : (tile + 1) * LANES] = jnp.concatenate(
                    taken, axis=0
                ).astype(BF16)

    with jax.named_scope("turn_own"):
        mine.wait()
        turn(core)
    with jax.named_scope("swap_wait"):
        swap.wait()
    with jax.named_scope("turn_other"):
        turn(1 - core)

    with jax.named_scope("wait_out"):
        exchanged(pieces, got, out_send, out_recv).wait()

    with jax.named_scope("lines"):
        for g in range(cons):
            field = assignment[g]
            for s in range(2):
                mixed[(s * cons + g) * 16 : (s * cons + g + 1) * 16, :] = got[2 * field + s].astype(F32)
        for t in range(ring):
            for s in range(2):
                for p in range(2):
                    lines[t, p * cons : (p + 1) * cons, s * LANES : (s + 1) * LANES] = mixed[
                        pl.ds(s * cons * 16 + p * 8 + t, cons, stride=16), :
                    ]

    lane = lax.broadcasted_iota(jnp.int32, (full, 2 * LANES), 1)
    lane = jnp.where(lane >= LANES, lane - LANES, lane)
    which = jnp.where(lane < CYC, 0, jnp.where(lane < 2 * CYC, 1, jnp.where(lane < TRI * CYC, 2, 3)))

    def analysed(t):
        x = lines[t]
        left = [jnp.where(which == i, x, 0.0) for i in range(TRI)]
        part[t] = jnp.dot(
            jnp.concatenate(left, axis=0).astype(BF16), table[t], preferred_element_type=F32
        ).astype(BF16)

    def piece(i, p):
        return pl.ds(pl.multiple_of(i * full + p * cons, cons), cons)

    ways, triples, ends = (1, -1), range(TRI), range(2)
    scale = love[...].reshape(1, depth)

    def synthesised(t):
        got_all = lax.dot_general(
            coef[t], table[t], (((1,), (1,)), ((), ())), preferred_element_type=F32
        )
        chosen = jnp.where(
            which == 0,
            got_all[:full],
            jnp.where(which == 1, got_all[full : 2 * full], got_all[2 * full :]),
        )
        order = which + (TRI * t + core * half_orders + c * 2 * half_orders)
        chosen = chosen * jnp.where(order == 0, 1.0, 2.0).astype(F32)
        for s in range(2):
            place = pl.ds(pl.multiple_of(s * ring * full + t * full, 8), full)
            rows[place, :] = chosen[:, s * LANES : (s + 1) * LANES]

    def sum_sent(source, target, way, step, i, p, hops=1):
        return remote(
            source, target, sum_send, ring_recv.at[way, step, i, p], on_ring(hops * ways[way])
        )

    @pl.when(core == 0)
    def _():
        def sum_step(way, step, i, p):
            if step == 0:
                source = part.at[slot(far), piece(i, p)]
                return sum_sent(source, first.at[way, i], way, step, i, p, 2)
            target = later.at[way, step - 1, i, p]
            if step == 1:
                source = part.at[slot(ways[way] * (far - 1)), piece(i, p)]
            else:
                source = staged.at[way, step - 1, i, p]
            return sum_sent(source, target, way, step, i, p)

        with jax.named_scope("first_part"):
            analysed(slot(far))
            for i in triples:
                for way in ends:
                    sum_step(way, 0, i, way).start()
            for way in ends:
                analysed(slot(ways[way] * (far - 1)))
                for i in triples:
                    for p in (1 - way, way):
                        sum_step(way, 1, i, p).start()
            for step in range(2, far):
                for way in ends:
                    analysed(slot(ways[way] * (far - step)))
            analysed(z)
        for step in range(2, far):
            with jax.named_scope(f"sum#s={step}"):
                for i in triples:
                    for late in ends:
                        for way in ends:
                            p = way if late else 1 - way
                            owner = slot(ways[way] * (far - step))
                            sum_step(way, step - 1, i, p).wait_recv()
                            total = part[owner, piece(i, p), :].astype(F32) + later[
                                way, step - 2, i, p
                            ].astype(F32)
                            if step == 2 and late:
                                sum_step(way, 0, i, p).wait_recv()
                                total = total + first[way, i].astype(F32)
                            staged[way, step - 1, i, p] = total.astype(BF16)
                            sum_step(way, step, i, p).start()

        def pair_step(i, p):
            return remote(
                sent.at[i, p], other.at[i, p], pair_send, cross_recv.at[0, 2 * i + p], across
            )

        with jax.named_scope("last_sum"):
            for i in triples:
                for p in ends:
                    for way in ends:
                        sum_step(way, far - 1, i, p).wait_recv()
                    sent[i, p] = (
                        part[z, piece(i, p), :].astype(F32)
                        + later[0, far - 2, i, p].astype(F32)
                        + later[1, far - 2, i, p].astype(F32)
                    ).astype(BF16)
                    pair_step(i, p).start()

        def all_step(way, step, i, p, late=0):
            hops = 2 if step == far else 1
            distance = far - 2 if step == far else step
            distance = distance + late * hops
            ref = coef.at[slot(-ways[way] * distance), piece(i, p)]
            if step == far:
                recv = cross_recv.at[1, TRI * way + i]
            else:
                recv = ring_recv.at[way, step, i, p]
            return remote(ref, ref, all_send, recv, on_ring(hops * ways[way]))

        with jax.named_scope("pair"):
            for i in triples:
                for p in ends:
                    pair_step(i, p).wait_recv()
                    coef[z, piece(i, p), :] = (
                        (sent[i, p].astype(F32) + other[i, p].astype(F32)) * scale
                    ).astype(BF16)
                    for way in ends:
                        all_step(way, 0, i, p).start()
        for step in range(1, far - 1):
            with jax.named_scope(f"all#s={step}"):
                for i in triples:
                    for p in ends:
                        for way in ends:
                            all_step(way, step - 1, i, p, 1).wait_recv()
                            all_step(way, step, i, p).start()
                            if step == far - 2 and p == way:
                                all_step(way, far, i, p).start()
            with jax.named_scope(f"synth#s={step}"):
                for owner in (0,) if step == 1 else (step - 1, 1 - step):
                    synthesised(slot(owner))
        with jax.named_scope("synth_last"):
            for owner in (far - 2, 2 - far):
                synthesised(slot(owner))
        with jax.named_scope("all_last"):
            for i in triples:
                for p in ends:
                    for way in ends:
                        all_step(way, far - 2, i, p, 1).wait_recv()
            for owner in (far - 1, 1 - far):
                synthesised(slot(owner))
            for i in triples:
                for way in ends:
                    all_step(way, far, i, way, 1).wait_recv()
        with jax.named_scope("synth_far"):
            synthesised(slot(far))
        most = pl.ds(0, ring - 1)
        remote(part.at[most], part.at[most], sum_send, own_sem, across).wait_send()
        remote(coef.at[most], coef.at[most], all_send, own_sem, across).wait_send()
        remote(sent, other, pair_send, own_sem, across).wait_send()

    @pl.when(core == 1)
    def _():
        owners = [far]
        for distance in range(far - 1, 0, -1):
            owners += [distance, -distance]
        owners.append(0)

        def mixed_sum(owner, i):
            k = owners.index(owner)
            return part[slot(owner), mine_rows[i], :].astype(F32) + crossed[k, i].astype(F32)

        def taken(owner, turn):
            k = owners.index(owner)
            remote(
                crossed.at[k], crossed.at[k], pair_send, cross_recv.at[turn, k], across
            ).wait_recv()

        def sum_step(way, step, i):
            if step == 0:
                return sum_sent(sent.at[i, 0], first.at[way, i], way, 0, i, 0)
            source, target = staged.at[way, step - 1, i, 0], later.at[way, step - 1, i, 0]
            return sum_sent(source, target, way, step, i, 0)

        with jax.named_scope("first_part"):
            for k, owner in enumerate(owners):
                analysed(slot(owner))
                for i in triples:
                    remote(
                        part.at[slot(owner), other_rows[i]],
                        crossed.at[k, i],
                        pair_send,
                        cross_recv.at[0, k],
                        across,
                    ).start()
        with jax.named_scope("sum#s=0"):
            taken(far, 0)
            for i in triples:
                sent[i, 0] = mixed_sum(far, i).astype(BF16)
                sum_step(i % 2, 0, i).start()
        for step in range(1, far):
            with jax.named_scope(f"sum#s={step}"):
                for way in ends:
                    taken(ways[way] * (far - step), 0)
                for late in ends:
                    for i in triples:
                        for way in ends:
                            if late != (way == i % 2):
                                continue
                            total = mixed_sum(ways[way] * (far - step), i)
                            if step > 1 or late:
                                sum_step(way, step - 1, i).wait_recv()
                                come = first[way, i] if step == 1 else later[way, step - 2, i, 0]
                                total = total + come.astype(F32)
                            staged[way, step - 1, i, 0] = total.astype(BF16)
                            sum_step(way, step, i).start()

        def all_step(way, step, i, late=0):
            ref = coef.at[slot(-ways[way] * (step + late)), mine_rows[i]]
            return remote(
                ref, ref, all_send, ring_recv.at[way, step, i, 0], on_ring(ways[way])
            )

        def shared(owner, i):
            ref = coef.at[slot(owner), mine_rows[i]]
            k = owners.index(owner)
            return remote(ref, ref, pair_send, cross_recv.at[1, k], across)

        with jax.named_scope("last_sum"):
            taken(0, 0)
            for i in triples:
                for way in ends:
                    sum_step(way, far - 1, i).wait_recv()
                coef[z, mine_rows[i], :] = (
                    (
                        mixed_sum(0, i)
                        + later[0, far - 2, i, 0].astype(F32)
                        + later[1, far - 2, i, 0].astype(F32)
                    )
                    * scale
                ).astype(BF16)
                for way in ends:
                    all_step(way, 0, i).start()
                shared(0, i).start()

        def ended(owner):
            taken(owner, 1)
            synthesised(slot(owner))

        for step in range(1, far):
            with jax.named_scope(f"all#s={step}"):
                for i in triples:
                    for way in ends:
                        all_step(way, step - 1, i, 1).wait_recv()
                        if step < far - 1 or way == i % 2:
                            all_step(way, step, i).start()
                        shared(-ways[way] * step, i).start()
            with jax.named_scope(f"synth#s={step}"):
                if step == 2:
                    ended(0)
                elif step == 3:
                    for way in ways:
                        ended(way)
        with jax.named_scope("all_last"):
            for i in triples:
                all_step(i % 2, far - 1, i, 1).wait_recv()
                shared(far, i).start()
        with jax.named_scope("synth_last"):
            for distance in range(2, far):
                for way in ways:
                    ended(way * distance)
            ended(far)
        most = pl.ds(0, ring - 1)
        remote(crossed.at[most], crossed.at[most], sum_send, own_sem, across).wait_send()
        remote(crossed.at[most], crossed.at[most], all_send, own_sem, across).wait_send()
        remote(coef, coef, pair_send, own_sem, across).wait_send()

    with jax.named_scope("back"):
        for g in range(cons):
            for s in range(2):
                both = [
                    rows[pl.ds(s * ring * full + p * cons + g, ring, stride=full), :] for p in range(2)
                ]
                back[2 * g + s] = jnp.concatenate(both, axis=0).astype(BF16)

    for offset in outward:
        exchange(offset, back, out, back_send, back_recv).start()

    kept = pltpu.make_async_copy(back.at[me], out.at[me], own_sem)
    kept.start()

    with jax.named_scope("wait_sends"):
        kept.wait()

    with jax.named_scope("wait_back"):
        exchanged(back, out, back_send, back_recv).wait()


def middle(elevation, legendre, cycle_weight, love_factor, assignment):
    cons = lax.axis_size("cons")
    period = elevation.shape[-1]
    depth = legendre.shape[2]
    ring = 8
    far = ring // 2
    full = 2 * cons
    dma = pltpu.SemaphoreType.DMA
    vmem = pltpu.VMEM
    twiddle, basis = phase_tables(period)
    pieces = (2 * cons, 16, LANES)
    return pl.pallas_call(
        functools.partial(middle_kernel, ring, cons),
        out_shape=jax.ShapeDtypeStruct(pieces, BF16),
        in_specs=[pl.BlockSpec(memory_space=pltpu.HBM)] * 7,
        out_specs=pl.BlockSpec(memory_space=pltpu.HBM),
        scratch_shapes=[
            vmem((1, CYC, period), BF16),
            pltpu.SMEM((CYC,), F32),
            vmem((depth,), F32),
            pltpu.SMEM((cons,), jnp.int32),
            vmem(twiddle.shape, F32),
            vmem(basis.shape, BF16),
            vmem(pieces, BF16),
            vmem((RADIX // TRI * LANES, 2 * LANES), F32),
            vmem((RADIX // TRI * full, LANES), F32),
            vmem((2, CYC, TRI * ring, depth), BF16),
            vmem((depth // LANES, CYC * TRI * ring, LANES), F32),
            vmem((ring, 2 * LANES, depth), BF16),
            vmem(pieces, BF16),
            vmem((2 * cons * 16, LANES), F32),
            vmem((ring, full, 2 * LANES), F32),
            vmem((ring, TRI * full, depth), BF16),
            vmem((2, TRI, cons, depth), BF16),
            vmem((2, far - 1, TRI, 2, cons, depth), BF16),
            vmem((2, far - 1, TRI, 2, cons, depth), BF16),
            vmem((TRI, 2, cons, depth), BF16),
            vmem((TRI, 2, cons, depth), BF16),
            vmem((ring, TRI, cons, depth), BF16),
            vmem((ring, TRI * full, depth), BF16),
            vmem((2 * ring * full, LANES), F32),
            vmem(pieces, BF16),
            dma,
            dma,
            dma,
            dma,
            dma,
            dma,
            dma,
            dma,
            dma((2, far, TRI, 2)),
            dma((2, ring)),
            dma,
            dma,
        ],
        compiler_params=pltpu.CompilerParams(
            collective_id=KERNEL_ID, has_side_effects=True, vmem_limit_bytes=67_000_000
        ),
        name="middle",
    )(
        elevation,
        legendre,
        cycle_weight,
        love_factor,
        assignment,
        jnp.asarray(twiddle),
        jnp.asarray(basis),
    )


def local(elevation, legendre, cycle_weight, love_factor, assignment):
    returned = middle(elevation, legendre, cycle_weight, love_factor, assignment)
    return inverse(returned, elevation.shape[-1])


def solution(mesh):
    placed = (P("cons", "blk", None), P("blk", "cons", None), P("blk"), P(), P())
    return jax.shard_map(
        local, mesh=mesh, in_specs=placed, out_specs=P("cons", "blk", None), check_vma=False
    )
```

```python
import functools
import math
import numpy as np
import jax
import jax.numpy as jnp
from jax import lax
from jax.experimental import pallas as pl
from jax.experimental.pallas import tpu as pltpu
from jax.sharding import PartitionSpec as P

RADIX = 48
LANES = 128
CYC = 40
TRI = 3


def by_phase(value, turn):
    re, im = value
    cos, sin = math.cos(2 * math.pi * turn), math.sin(2 * math.pi * turn)
    cos = 0.0 if abs(cos) < 1e-12 else cos
    sin = 0.0 if abs(sin) < 1e-12 else sin

    def scaled(array, factor):
        if array is None or factor == 0.0:
            return None
        if abs(factor - 1.0) < 1e-12:
            return array
        if abs(factor + 1.0) < 1e-12:
            return -array
        return array * np.float32(factor)

    return (
        added(scaled(re, cos), scaled(im, -sin)),
        added(scaled(re, sin), scaled(im, cos)),
    )


def added(a, b):
    if a is None:
        return b
    return a if b is None else a + b


def plus(a, b):
    return added(a[0], b[0]), added(a[1], b[1])


def conj(a):
    return a[0], None if a[1] is None else -a[1]


def at(half, index, length):
    index %= length
    return half[index] if 2 * index <= length else conj(half[length - index])


def minus(a, b):
    return plus(a, negated(b))


def negated(a):
    return tuple(None if part is None else -part for part in a)


def turned_left(a):
    re, im = a
    return None if im is None else -im, re


def factor_of(length):
    return 4 if length % 4 == 0 else (3 if length % 3 == 0 else 2)


def short_dft(values, sign):
    n = len(values)
    if n != 4:
        out = []
        for k in range(n):
            total = values[0]
            for i in range(1, n):
                total = plus(total, by_phase(values[i], sign * i * k / n))
            out.append(total)
        return out
    even, odd = plus(values[0], values[2]), plus(values[1], values[3])
    even_gap, odd_gap = minus(values[0], values[2]), turned_left(minus(values[1], values[3]))
    ahead, behind = plus(even_gap, odd_gap), minus(even_gap, odd_gap)
    if sign < 0:
        ahead, behind = behind, ahead
    return [plus(even, odd), ahead, minus(even, odd), behind]


def real_fft(values):
    n = len(values)
    if n == 1:
        return [(values[0], None)]
    p = factor_of(n)
    short = n // p
    parts = [real_fft(values[i::p]) for i in range(p)]
    out = [None] * n
    for k in range(short):
        if k > n // 2:
            continue
        spun = [by_phase(at(parts[i], k, short), -i * k / n) for i in range(p)]
        for s, value in enumerate(short_dft(spun, -1)):
            out[k + s * short] = value
    half = out[: n // 2 + 1]
    half[0] = (half[0][0], None)
    if n % 2 == 0:
        half[-1] = (half[-1][0], None)
    return half


def real_inverse(half, n):
    if n == 1:
        return [half[0][0]]
    if n == 3:
        base, (re, im) = half[0][0], half[1]
        middle = base - re
        side = im * np.float32(math.sqrt(3.0))
        return [base + (re + re), middle - side, middle + side]
    p = factor_of(n)
    short = n // p
    folded = [[None] * (short // 2 + 1) for _ in range(p)]
    for r in range(short // 2 + 1):
        mixed = short_dft([at(half, r + s * short, n) for s in range(p)], 1)
        for a in range(p):
            total = by_phase(mixed[a], r * a / n)
            if r == 0 or 2 * r == short:
                total = (total[0], None)
            folded[a][r] = total
    out = [None] * n
    for a in range(p):
        for kk, value in enumerate(real_inverse(folded[a], short)):
            out[p * kk + a] = value
    return out


def phase_tables(period):
    lane = np.arange(LANES)
    turn = np.arange(RADIX)[:, None] * lane[None, :] / period
    twiddle = np.stack([np.cos(2 * np.pi * turn), np.sin(2 * np.pi * turn)], 1)
    q = np.arange(period // RADIX // 8)[:, None] * lane[None, :] / LANES
    cos, sin = np.cos(2 * np.pi * q), np.sin(2 * np.pi * q)
    basis = np.concatenate([np.concatenate([cos, sin], 1), np.concatenate([-sin, cos], 1)], 0)
    return twiddle.reshape(2 * RADIX, LANES).astype(np.float32), basis.astype(jnp.bfloat16)


def transformed(x_ref, weight, twiddle_ref, basis_ref, out_ref, mixed, rows):
    cons = out_ref.shape[0] // 2
    for triple in range(RADIX // TRI):
        mixed[triple * LANES + TRI * CYC : (triple + 1) * LANES, :] = jnp.zeros(
            (LANES - TRI * CYC, 2 * LANES), jnp.float32
        )

    @pl.loop(0, CYC // 8)
    def _(group):
        lines = pl.ds(pl.multiple_of(group * 8, 8), 8)
        half = real_fft(
            [
                x_ref[0, lines, k * LANES : (k + 1) * LANES].astype(jnp.float32)
                for k in range(RADIX)
            ]
        )
        for r in range(RADIX):
            re, im = at(half, r, RADIX)
            cos, sin = twiddle_ref[2 * r : 2 * r + 1, :], twiddle_ref[2 * r + 1 : 2 * r + 2, :]
            if im is None:
                new_re, new_im = re * cos, -re * sin
            else:
                new_re, new_im = re * cos + im * sin, im * cos - re * sin
            start = (r // TRI) * LANES + (r % TRI) * CYC
            place = pl.ds(pl.multiple_of(start + group * 8, 8), 8)
            mixed[place, 0:LANES] = new_re
            mixed[place, LANES:] = new_im

    for triple in range(RADIX // TRI):
        block = mixed[triple * LANES : (triple + 1) * LANES, :].astype(jnp.bfloat16)
        got = lax.dot_general(
            basis_ref[...], block, (((1,), (1,)), ((), ())), preferred_element_type=jnp.float32
        )
        rows[triple * 2 * cons : (triple + 1) * 2 * cons, :] = got * weight
    for c in range(cons):
        for h in range(2):
            both = [
                rows[pl.ds(h * 16 * cons + p * cons + c, 8, stride=2 * cons), :] for p in range(2)
            ]
            out_ref[2 * c + h] = jnp.concatenate(both, axis=0).astype(jnp.bfloat16)


def inverse_kernel(
    z_hbm, twiddle_hbm, basis_hbm, out_hbm, z_ref, twiddle_ref, basis_ref, rows, mixed, done, sems, out_sems
):
    pairs = ((z_hbm, z_ref), (twiddle_hbm, twiddle_ref), (basis_hbm, basis_ref))
    loads = [
        pltpu.make_async_copy(source, target, sems.at[i])
        for i, (source, target) in enumerate(pairs)
    ]
    for load in loads:
        load.start()
    for load in loads:
        load.wait()
    cons = z_ref.shape[0] // 2
    for source in range(2 * cons):
        rows[source * 16 : (source + 1) * 16, :] = z_ref[source].astype(jnp.float32)
    for triple in range(RADIX // TRI):
        h, t = divmod(triple, 8)
        both = [rows[pl.ds(h * 16 + p * 8 + t, cons, stride=32), :] for p in range(2)]
        lines = jnp.concatenate(both, axis=0).T.astype(jnp.bfloat16)
        mixed[triple * LANES : (triple + 1) * LANES, :] = jnp.dot(
            lines, basis_ref[...], preferred_element_type=jnp.float32
        )

    def leave(group):
        lines = pl.ds(pl.multiple_of(group * 8, 8), 8)
        return pltpu.make_async_copy(done.at[group], out_hbm.at[0, lines], out_sems.at[group])

    @pl.loop(0, CYC // 8)
    def _(group):
        turned = []
        for r in range(RADIX):
            start = (r // TRI) * LANES + (r % TRI) * CYC
            place = pl.ds(pl.multiple_of(start + group * 8, 8), 8)
            re, im = mixed[place, 0:LANES], mixed[place, LANES:]
            cos, sin = twiddle_ref[2 * r : 2 * r + 1, :], twiddle_ref[2 * r + 1 : 2 * r + 2, :]
            turned.append((re * cos - im * sin, re * sin + im * cos))
        middle = RADIX // 2
        half = [(turned[0][0] + turned[0][0], None)]
        for r in range(1, middle):
            pair = plus(turned[r], conj(turned[RADIX - r]))
            half.append(pair)
        half.append((turned[middle][0] + turned[middle][0], None))
        for k, value in enumerate(real_inverse(half, RADIX)):
            done[group, :, k * LANES : (k + 1) * LANES] = value
        leave(group).start()

    @pl.loop(0, CYC // 8)
    def _(group):
        leave(group).wait()


def inverse(pieces, period):
    cons = pieces.shape[0] // 2
    twiddle, basis = phase_tables(period)
    twiddle = twiddle * np.float32(0.5)
    return pl.pallas_call(
        inverse_kernel,
        out_shape=jax.ShapeDtypeStruct((1, CYC, period), jnp.float32),
        in_specs=[pl.BlockSpec(memory_space=pltpu.HBM)] * 3,
        out_specs=pl.BlockSpec(memory_space=pltpu.HBM),
        scratch_shapes=[
            pltpu.VMEM(pieces.shape, jnp.bfloat16),
            pltpu.VMEM(twiddle.shape, jnp.float32),
            pltpu.VMEM(basis.shape, jnp.bfloat16),
            pltpu.VMEM((2 * cons * 16, LANES), jnp.float32),
            pltpu.VMEM((RADIX // TRI * LANES, 2 * LANES), jnp.float32),
            pltpu.VMEM((CYC // 8, 8, period), jnp.float32),
            pltpu.SemaphoreType.DMA((3,)),
            pltpu.SemaphoreType.DMA((CYC // 8,)),
        ],
        compiler_params=pltpu.CompilerParams(vmem_limit_bytes=67_000_000),
        name="inverse",
    )(pieces, jnp.asarray(twiddle), jnp.asarray(basis))


MESH = pl.DeviceIdType.MESH
F32 = jnp.float32
BF16 = jnp.bfloat16
KERNEL_ID = 0


def middle_kernel(
    ring, cons, elevation, legendre, cycle_weight, love_factor, assigned, twiddles, bases, out,
    height, weights, love, assignment, twiddle, basis, pieces, spun, spread,
    held, wide, table, got, mixed, lines, part, first, later, staged, sent, other, crossed, coef,
    rows, back,
    own_sem, swap_send, swap_recv, out_send, out_recv, sum_send, pair_send, all_send,
    ring_recv, cross_recv, back_send, back_recv,
):
    c, b = lax.axis_index("cons"), lax.axis_index("blk")
    core = lax.rem(b, 2)
    z = lax.rem(b // 2, ring)
    line = b // (2 * ring)
    chip = b - core
    me = 2 * c + core
    peers = 2 * cons
    far = ring // 2
    depth = legendre.shape[2]
    half_orders = TRI * ring
    full = 2 * cons
    barrier = pltpu.get_barrier_semaphore()

    slots = {offset: lax.rem(z + offset + ring, ring) for offset in range(-far, far + 1)}
    row_start = line * 2 * ring + core
    near = {hops: (c, row_start + 2 * slots[hops]) for hops in (1, -1, 2, -2)}

    def slot(offset):
        return slots[offset]

    def on_ring(offset):
        return near[offset]

    outward = sorted(range(1, peers), key=lambda offset: abs(offset - peers // 2))

    def remote(source, target, send, recv, device):
        return pltpu.make_async_remote_copy(
            src_ref=source,
            dst_ref=target,
            send_sem=send,
            recv_sem=recv,
            device_id=device,
            device_id_type=MESH,
        )

    def peer(offset):
        if offset % 2:
            return lax.rem(c + core + offset // 2, cons), 1 - core
        return lax.rem(c + offset // 2, cons), core

    def exchange(offset, source, landing, send, recv):
        far_c, far_core = peer(offset)
        there = (far_c, chip + far_core)
        return remote(source.at[2 * far_c + far_core], landing.at[me], send, recv, there)

    def exchanged(source, landing, send, recv):
        rest = pl.ds(0, peers - 1)
        return remote(source.at[rest], landing.at[rest], send, recv, (c, chip + 1 - core))

    across = (c, (1 - line) * 2 * ring + z * 2 + core)
    mine_rows = [pl.ds(pl.multiple_of(i * full + line * cons, cons), cons) for i in range(TRI)]
    other_rows = [
        pl.ds(pl.multiple_of(i * full + (1 - line) * cons, cons), cons) for i in range(TRI)
    ]

    def half_of(which):
        return legendre.at[:, pl.ds(pl.multiple_of(which * half_orders, 8), half_orders), :]

    mine = pltpu.make_async_copy(half_of(core), held.at[core], own_sem)
    pairs = (
        (elevation, height),
        (twiddles, twiddle),
        (bases, basis),
        (cycle_weight, weights),
        (assigned, assignment),
        (love_factor, love),
    )
    loads = [
        pltpu.make_async_copy(source, target, cross_recv.at[1, i])
        for i, (source, target) in enumerate(pairs)
    ]
    with jax.named_scope("signals"):
        for load in loads:
            load.start()

        for offset in outward:
            far_c, far_core = peer(offset)
            there = (far_c, chip + far_core)
            pl.semaphore_signal(barrier, inc=1, device_id=there, device_id_type=MESH)

        for target in (on_ring(1), on_ring(-1), on_ring(2), on_ring(-2), across):
            pl.semaphore_signal(barrier, inc=1, device_id=target, device_id_type=MESH)
        mine.start()
    with jax.named_scope("loads"):
        for load in loads:
            load.wait()

    with jax.named_scope("fft"):
        lane_of = lax.broadcasted_iota(jnp.int32, (1, LANES), 1)
        day = lane_of - jnp.where(lane_of < CYC, 0, jnp.where(lane_of < 2 * CYC, CYC, 2 * CYC))
        weight = jnp.zeros((1, LANES), F32)
        for j in range(CYC):
            weight = jnp.where(day == j, weights[j], weight)
        transformed(height, weight, twiddle, basis, pieces, spun, spread)

    with jax.named_scope("barrier"):
        pl.semaphore_wait(barrier, peers + 4)

    swap = remote(half_of(1 - core), held.at[core], swap_send, swap_recv, (c, chip + 1 - core))
    swap.start()

    for offset in outward:
        exchange(offset, pieces, got, out_send, out_recv).start()

    got[me] = pieces[me]

    def turn(which):
        @pl.loop(0, CYC)
        def _(j):
            place = pl.ds(pl.multiple_of(j * half_orders, 8), half_orders)
            for tile in range(depth // LANES):
                wide[tile, place, :] = held[
                    which, j, :, tile * LANES : (tile + 1) * LANES
                ].astype(F32)

        @pl.loop(0, ring)
        def _(t):
            place = pl.ds(pl.multiple_of(which * LANES, LANES), LANES)
            for tile in range(depth // LANES):
                taken = [
                    wide[tile, pl.ds(TRI * t + i, CYC, stride=half_orders), :] for i in range(TRI)
                ]
                taken.append(jnp.zeros((LANES - TRI * CYC, LANES), F32))
                table[t, place, tile * LANES : (tile + 1) * LANES] = jnp.concatenate(
                    taken, axis=0
                ).astype(BF16)

    with jax.named_scope("turn_own"):
        mine.wait()
        turn(core)
    with jax.named_scope("swap_wait"):
        swap.wait()
    with jax.named_scope("turn_other"):
        turn(1 - core)

    with jax.named_scope("wait_out"):
        exchanged(pieces, got, out_send, out_recv).wait()

    with jax.named_scope("lines"):
        for g in range(cons):
            field = assignment[g]
            for s in range(2):
                mixed[(s * cons + g) * 16 : (s * cons + g + 1) * 16, :] = got[2 * field + s].astype(F32)
        for t in range(ring):
            for s in range(2):
                for p in range(2):
                    lines[t, p * cons : (p + 1) * cons, s * LANES : (s + 1) * LANES] = mixed[
                        pl.ds(s * cons * 16 + p * 8 + t, cons, stride=16), :
                    ]

    lane = lax.broadcasted_iota(jnp.int32, (full, 2 * LANES), 1)
    lane = jnp.where(lane >= LANES, lane - LANES, lane)
    which = jnp.where(lane < CYC, 0, jnp.where(lane < 2 * CYC, 1, jnp.where(lane < TRI * CYC, 2, 3)))

    def analysed(t):
        x = lines[t]
        left = [jnp.where(which == i, x, 0.0) for i in range(TRI)]
        part[t] = jnp.dot(
            jnp.concatenate(left, axis=0).astype(BF16), table[t], preferred_element_type=F32
        ).astype(BF16)

    def piece(i, p):
        return pl.ds(pl.multiple_of(i * full + p * cons, cons), cons)

    ways, triples, ends = (1, -1), range(TRI), range(2)
    scale = love[...].reshape(1, depth)

    def synthesised(t):
        got_all = lax.dot_general(
            coef[t], table[t], (((1,), (1,)), ((), ())), preferred_element_type=F32
        )
        chosen = jnp.where(
            which == 0,
            got_all[:full],
            jnp.where(which == 1, got_all[full : 2 * full], got_all[2 * full :]),
        )
        order = which + (TRI * t + core * half_orders + c * 2 * half_orders)
        chosen = chosen * jnp.where(order == 0, 1.0, 2.0).astype(F32)
        for s in range(2):
            place = pl.ds(pl.multiple_of(s * ring * full + t * full, 8), full)
            rows[place, :] = chosen[:, s * LANES : (s + 1) * LANES]

    def sum_sent(source, target, way, step, i, p, hops=1):
        return remote(
            source, target, sum_send, ring_recv.at[way, step, i, p], on_ring(hops * ways[way])
        )

    @pl.when(core == 0)
    def _():
        def sum_step(way, step, i, p):
            if step == 0:
                source = part.at[slot(far), piece(i, p)]
                return sum_sent(source, first.at[way, i], way, step, i, p, 2)
            target = later.at[way, step - 1, i, p]
            if step == 1:
                source = part.at[slot(ways[way] * (far - 1)), piece(i, p)]
            else:
                source = staged.at[way, step - 1, i, p]
            return sum_sent(source, target, way, step, i, p)

        with jax.named_scope("first_part"):
            analysed(slot(far))
            for way in ends:
                sum_step(way, 0, 0, way).start()
            for way in ends:
                analysed(slot(ways[way] * (far - 1)))
                for i in triples:
                    if i:
                        sum_step(way, 0, i, way).start()
                    for p in (1 - way, way):
                        sum_step(way, 1, i, p).start()
            for step in range(2, far):
                for way in ends:
                    analysed(slot(ways[way] * (far - step)))
            analysed(z)
        for step in range(2, far):
            with jax.named_scope(f"sum#s={step}"):
                for i in triples:
                    for late in ends:
                        for way in ends:
                            p = way if late else 1 - way
                            owner = slot(ways[way] * (far - step))
                            sum_step(way, step - 1, i, p).wait_recv()
                            total = part[owner, piece(i, p), :].astype(F32) + later[
                                way, step - 2, i, p
                            ].astype(F32)
                            if step == 2 and late:
                                sum_step(way, 0, i, p).wait_recv()
                                total = total + first[way, i].astype(F32)
                            staged[way, step - 1, i, p] = total.astype(BF16)
                            sum_step(way, step, i, p).start()

        def pair_step(i, p):
            return remote(
                sent.at[i, p], other.at[i, p], pair_send, cross_recv.at[0, 2 * i + p], across
            )

        with jax.named_scope("last_sum"):
            for i in triples:
                for p in ends:
                    for way in ends:
                        sum_step(way, far - 1, i, p).wait_recv()
                    sent[i, p] = (
                        part[z, piece(i, p), :].astype(F32)
                        + later[0, far - 2, i, p].astype(F32)
                        + later[1, far - 2, i, p].astype(F32)
                    ).astype(BF16)
                    pair_step(i, p).start()

        def all_step(way, step, i, p, late=0):
            hops = 2 if step == far else 1
            distance = far - 2 if step == far else step
            distance = distance + late * hops
            ref = coef.at[slot(-ways[way] * distance), piece(i, p)]
            if step == far:
                recv = cross_recv.at[1, TRI * way + i]
            else:
                recv = ring_recv.at[way, step, i, p]
            return remote(ref, ref, all_send, recv, on_ring(hops * ways[way]))

        with jax.named_scope("pair"):
            for i in triples:
                for p in ends:
                    pair_step(i, p).wait_recv()
                    coef[z, piece(i, p), :] = (
                        (sent[i, p].astype(F32) + other[i, p].astype(F32)) * scale
                    ).astype(BF16)
                    for way in ends:
                        all_step(way, 0, i, p).start()
        for step in range(1, far - 1):
            with jax.named_scope(f"all#s={step}"):
                for i in triples:
                    for p in ends:
                        for way in ends:
                            all_step(way, step - 1, i, p, 1).wait_recv()
                            if step == far - 2 and p == way:
                                all_step(way, far, i, p).start()
                            all_step(way, step, i, p).start()
            with jax.named_scope(f"synth#s={step}"):
                for owner in (0,) if step == 1 else (step - 1, 1 - step):
                    synthesised(slot(owner))
        with jax.named_scope("synth_last"):
            for owner in (far - 2, 2 - far):
                synthesised(slot(owner))
        with jax.named_scope("all_last"):
            for i in triples:
                for p in ends:
                    for way in ends:
                        all_step(way, far - 2, i, p, 1).wait_recv()
            for owner in (far - 1, 1 - far):
                synthesised(slot(owner))
            for i in triples:
                for way in ends:
                    all_step(way, far, i, way, 1).wait_recv()
        with jax.named_scope("synth_far"):
            synthesised(slot(far))
        most = pl.ds(0, ring - 1)
        remote(part.at[most], part.at[most], sum_send, own_sem, across).wait_send()
        remote(coef.at[most], coef.at[most], all_send, own_sem, across).wait_send()
        remote(sent, other, pair_send, own_sem, across).wait_send()

    @pl.when(core == 1)
    def _():
        owners = [far]
        for distance in range(far - 1, 0, -1):
            owners += [distance, -distance]
        owners.append(0)

        def mixed_sum(owner, i):
            k = owners.index(owner)
            return part[slot(owner), mine_rows[i], :].astype(F32) + crossed[k, i].astype(F32)

        def taken(owner, turn):
            k = owners.index(owner)
            remote(
                crossed.at[k], crossed.at[k], pair_send, cross_recv.at[turn, k], across
            ).wait_recv()

        def sum_step(way, step, i):
            if step == 0:
                return sum_sent(sent.at[i, 0], first.at[way, i], way, 0, i, 0)
            source, target = staged.at[way, step - 1, i, 0], later.at[way, step - 1, i, 0]
            return sum_sent(source, target, way, step, i, 0)

        with jax.named_scope("first_part"):
            for k, owner in enumerate(owners):
                analysed(slot(owner))
                for i in triples:
                    remote(
                        part.at[slot(owner), other_rows[i]],
                        crossed.at[k, i],
                        pair_send,
                        cross_recv.at[0, k],
                        across,
                    ).start()
        with jax.named_scope("sum#s=0"):
            taken(far, 0)
            for i in triples:
                sent[i, 0] = mixed_sum(far, i).astype(BF16)
                sum_step(i % 2, 0, i).start()
        for step in range(1, far):
            with jax.named_scope(f"sum#s={step}"):
                for way in ends:
                    taken(ways[way] * (far - step), 0)
                for late in ends:
                    for i in triples:
                        for way in ends:
                            if late != (way == i % 2):
                                continue
                            total = mixed_sum(ways[way] * (far - step), i)
                            if step > 1 or late:
                                sum_step(way, step - 1, i).wait_recv()
                                come = first[way, i] if step == 1 else later[way, step - 2, i, 0]
                                total = total + come.astype(F32)
                            staged[way, step - 1, i, 0] = total.astype(BF16)
                            sum_step(way, step, i).start()

        def all_step(way, step, i, late=0):
            direct = int(step == far - 1)
            distance = step - direct + late * (1 + direct)
            ref = coef.at[slot(-ways[way] * distance), mine_rows[i]]
            recv = ring_recv.at[way, step, i, direct]
            return remote(ref, ref, all_send, recv, on_ring((1 + direct) * ways[way]))

        def shared(owner, i):
            ref = coef.at[slot(owner), mine_rows[i]]
            k = owners.index(owner)
            return remote(ref, ref, pair_send, cross_recv.at[1, k], across)

        with jax.named_scope("last_sum"):
            taken(0, 0)
            for i in triples:
                for way in ends:
                    sum_step(way, far - 1, i).wait_recv()
                coef[z, mine_rows[i], :] = (
                    (
                        mixed_sum(0, i)
                        + later[0, far - 2, i, 0].astype(F32)
                        + later[1, far - 2, i, 0].astype(F32)
                    )
                    * scale
                ).astype(BF16)
                for way in ends:
                    all_step(way, 0, i).start()
                shared(0, i).start()

        def ended(owner):
            taken(owner, 1)
            synthesised(slot(owner))

        for step in range(1, far):
            with jax.named_scope(f"all#s={step}"):
                for i in triples:
                    for way in ends:
                        all_step(way, step - 1, i, 1).wait_recv()
                        if step == far - 2 and way == i % 2:
                            all_step(way, far - 1, i).start()
                        if step < far - 1:
                            all_step(way, step, i).start()
                        shared(-ways[way] * step, i).start()
            with jax.named_scope(f"synth#s={step}"):
                if step == 2:
                    ended(0)
                elif step == 3:
                    for way in ways:
                        ended(way)
        with jax.named_scope("all_last"):
            for i in triples:
                all_step(i % 2, far - 1, i, 1).wait_recv()
                shared(far, i).start()
        with jax.named_scope("synth_last"):
            for distance in range(2, far):
                for way in ways:
                    ended(way * distance)
            ended(far)
        most = pl.ds(0, ring - 1)
        remote(crossed.at[most], crossed.at[most], sum_send, own_sem, across).wait_send()
        remote(crossed.at[most], crossed.at[most], all_send, own_sem, across).wait_send()
        remote(coef, coef, pair_send, own_sem, across).wait_send()

    with jax.named_scope("back"):
        for g in range(cons):
            for s in range(2):
                both = [
                    rows[pl.ds(s * ring * full + p * cons + g, ring, stride=full), :] for p in range(2)
                ]
                back[2 * g + s] = jnp.concatenate(both, axis=0).astype(BF16)

    for offset in outward:
        exchange(offset, back, out, back_send, back_recv).start()

    kept = pltpu.make_async_copy(back.at[me], out.at[me], own_sem)
    kept.start()

    with jax.named_scope("wait_sends"):
        kept.wait()

    with jax.named_scope("wait_back"):
        exchanged(back, out, back_send, back_recv).wait()


def middle(elevation, legendre, cycle_weight, love_factor, assignment):
    cons = lax.axis_size("cons")
    period = elevation.shape[-1]
    depth = legendre.shape[2]
    ring = 8
    far = ring // 2
    full = 2 * cons
    dma = pltpu.SemaphoreType.DMA
    vmem = pltpu.VMEM
    twiddle, basis = phase_tables(period)
    pieces = (2 * cons, 16, LANES)
    return pl.pallas_call(
        functools.partial(middle_kernel, ring, cons),
        out_shape=jax.ShapeDtypeStruct(pieces, BF16),
        in_specs=[pl.BlockSpec(memory_space=pltpu.HBM)] * 7,
        out_specs=pl.BlockSpec(memory_space=pltpu.HBM),
        scratch_shapes=[
            vmem((1, CYC, period), BF16),
            pltpu.SMEM((CYC,), F32),
            vmem((depth,), F32),
            pltpu.SMEM((cons,), jnp.int32),
            vmem(twiddle.shape, F32),
            vmem(basis.shape, BF16),
            vmem(pieces, BF16),
            vmem((RADIX // TRI * LANES, 2 * LANES), F32),
            vmem((RADIX // TRI * full, LANES), F32),
            vmem((2, CYC, TRI * ring, depth), BF16),
            vmem((depth // LANES, CYC * TRI * ring, LANES), F32),
            vmem((ring, 2 * LANES, depth), BF16),
            vmem(pieces, BF16),
            vmem((2 * cons * 16, LANES), F32),
            vmem((ring, full, 2 * LANES), F32),
            vmem((ring, TRI * full, depth), BF16),
            vmem((2, TRI, cons, depth), BF16),
            vmem((2, far - 1, TRI, 2, cons, depth), BF16),
            vmem((2, far - 1, TRI, 2, cons, depth), BF16),
            vmem((TRI, 2, cons, depth), BF16),
            vmem((TRI, 2, cons, depth), BF16),
            vmem((ring, TRI, cons, depth), BF16),
            vmem((ring, TRI * full, depth), BF16),
            vmem((2 * ring * full, LANES), F32),
            vmem(pieces, BF16),
            dma,
            dma,
            dma,
            dma,
            dma,
            dma,
            dma,
            dma,
            dma((2, far, TRI, 2)),
            dma((2, ring)),
            dma,
            dma,
        ],
        compiler_params=pltpu.CompilerParams(
            collective_id=KERNEL_ID, has_side_effects=True, vmem_limit_bytes=67_000_000
        ),
        name="middle",
    )(
        elevation,
        legendre,
        cycle_weight,
        love_factor,
        assignment,
        jnp.asarray(twiddle),
        jnp.asarray(basis),
    )


def local(elevation, legendre, cycle_weight, love_factor, assignment):
    returned = middle(elevation, legendre, cycle_weight, love_factor, assignment)
    return inverse(returned, elevation.shape[-1])


def solution(mesh):
    placed = (P("cons", "blk", None), P("blk", "cons", None), P("blk"), P(), P())
    return jax.shard_map(
        local, mesh=mesh, in_specs=placed, out_specs=P("cons", "blk", None), check_vma=False
    )
```

```python
import functools
import math
import numpy as np
import jax
import jax.numpy as jnp
from jax import lax
from jax.experimental import pallas as pl
from jax.experimental.pallas import tpu as pltpu
from jax.sharding import PartitionSpec as P

RADIX = 48
LANES = 128
CYC = 40
TRI = 3


def by_phase(value, turn):
    re, im = value
    cos, sin = math.cos(2 * math.pi * turn), math.sin(2 * math.pi * turn)
    cos = 0.0 if abs(cos) < 1e-12 else cos
    sin = 0.0 if abs(sin) < 1e-12 else sin

    def scaled(array, factor):
        if array is None or factor == 0.0:
            return None
        if abs(factor - 1.0) < 1e-12:
            return array
        if abs(factor + 1.0) < 1e-12:
            return -array
        return array * np.float32(factor)

    return (
        added(scaled(re, cos), scaled(im, -sin)),
        added(scaled(re, sin), scaled(im, cos)),
    )


def added(a, b):
    if a is None:
        return b
    return a if b is None else a + b


def plus(a, b):
    return added(a[0], b[0]), added(a[1], b[1])


def conj(a):
    return a[0], None if a[1] is None else -a[1]


def at(half, index, length):
    index %= length
    return half[index] if 2 * index <= length else conj(half[length - index])


def minus(a, b):
    return plus(a, negated(b))


def negated(a):
    return tuple(None if part is None else -part for part in a)


def turned_left(a):
    re, im = a
    return None if im is None else -im, re


def factor_of(length):
    return 4 if length % 4 == 0 else (3 if length % 3 == 0 else 2)


def short_dft(values, sign):
    n = len(values)
    if n != 4:
        out = []
        for k in range(n):
            total = values[0]
            for i in range(1, n):
                total = plus(total, by_phase(values[i], sign * i * k / n))
            out.append(total)
        return out
    even, odd = plus(values[0], values[2]), plus(values[1], values[3])
    even_gap, odd_gap = minus(values[0], values[2]), turned_left(minus(values[1], values[3]))
    ahead, behind = plus(even_gap, odd_gap), minus(even_gap, odd_gap)
    if sign < 0:
        ahead, behind = behind, ahead
    return [plus(even, odd), ahead, minus(even, odd), behind]


def real_fft(values):
    n = len(values)
    if n == 1:
        return [(values[0], None)]
    p = factor_of(n)
    short = n // p
    parts = [real_fft(values[i::p]) for i in range(p)]
    out = [None] * n
    for k in range(short):
        if k > n // 2:
            continue
        spun = [by_phase(at(parts[i], k, short), -i * k / n) for i in range(p)]
        for s, value in enumerate(short_dft(spun, -1)):
            out[k + s * short] = value
    half = out[: n // 2 + 1]
    half[0] = (half[0][0], None)
    if n % 2 == 0:
        half[-1] = (half[-1][0], None)
    return half


def real_inverse(half, n):
    if n == 1:
        return [half[0][0]]
    if n == 3:
        base, (re, im) = half[0][0], half[1]
        middle = base - re
        side = im * np.float32(math.sqrt(3.0))
        return [base + (re + re), middle - side, middle + side]
    p = factor_of(n)
    short = n // p
    folded = [[None] * (short // 2 + 1) for _ in range(p)]
    for r in range(short // 2 + 1):
        mixed = short_dft([at(half, r + s * short, n) for s in range(p)], 1)
        for a in range(p):
            total = by_phase(mixed[a], r * a / n)
            if r == 0 or 2 * r == short:
                total = (total[0], None)
            folded[a][r] = total
    out = [None] * n
    for a in range(p):
        for kk, value in enumerate(real_inverse(folded[a], short)):
            out[p * kk + a] = value
    return out


def phase_tables(period):
    lane = np.arange(LANES)
    turn = np.arange(RADIX)[:, None] * lane[None, :] / period
    twiddle = np.stack([np.cos(2 * np.pi * turn), np.sin(2 * np.pi * turn)], 1)
    q = np.arange(period // RADIX // 8)[:, None] * lane[None, :] / LANES
    cos, sin = np.cos(2 * np.pi * q), np.sin(2 * np.pi * q)
    basis = np.concatenate([np.concatenate([cos, sin], 1), np.concatenate([-sin, cos], 1)], 0)
    return twiddle.reshape(2 * RADIX, LANES).astype(np.float32), basis.astype(jnp.bfloat16)


def transformed(x_ref, weight, twiddle_ref, basis_ref, out_ref, mixed, rows):
    cons = out_ref.shape[0] // 2
    for triple in range(RADIX // TRI):
        mixed[triple * LANES + TRI * CYC : (triple + 1) * LANES, :] = jnp.zeros(
            (LANES - TRI * CYC, 2 * LANES), jnp.float32
        )

    @pl.loop(0, CYC // 8)
    def _(group):
        lines = pl.ds(pl.multiple_of(group * 8, 8), 8)
        half = real_fft(
            [
                x_ref[0, lines, k * LANES : (k + 1) * LANES].astype(jnp.float32)
                for k in range(RADIX)
            ]
        )
        for r in range(RADIX):
            re, im = at(half, r, RADIX)
            cos, sin = twiddle_ref[2 * r : 2 * r + 1, :], twiddle_ref[2 * r + 1 : 2 * r + 2, :]
            if im is None:
                new_re, new_im = re * cos, -re * sin
            else:
                new_re, new_im = re * cos + im * sin, im * cos - re * sin
            start = (r // TRI) * LANES + (r % TRI) * CYC
            place = pl.ds(pl.multiple_of(start + group * 8, 8), 8)
            mixed[place, 0:LANES] = new_re
            mixed[place, LANES:] = new_im

    for triple in range(RADIX // TRI):
        block = mixed[triple * LANES : (triple + 1) * LANES, :].astype(jnp.bfloat16)
        got = lax.dot_general(
            basis_ref[...], block, (((1,), (1,)), ((), ())), preferred_element_type=jnp.float32
        )
        rows[triple * 2 * cons : (triple + 1) * 2 * cons, :] = got * weight
    for c in range(cons):
        for h in range(2):
            both = [
                rows[pl.ds(h * 16 * cons + p * cons + c, 8, stride=2 * cons), :] for p in range(2)
            ]
            out_ref[2 * c + h] = jnp.concatenate(both, axis=0).astype(jnp.bfloat16)


def inverse_kernel(
    z_hbm, twiddle_hbm, basis_hbm, out_hbm, z_ref, twiddle_ref, basis_ref, rows, mixed, done, sems, out_sems
):
    pairs = ((z_hbm, z_ref), (twiddle_hbm, twiddle_ref), (basis_hbm, basis_ref))
    loads = [
        pltpu.make_async_copy(source, target, sems.at[i])
        for i, (source, target) in enumerate(pairs)
    ]
    for load in loads:
        load.start()
    for load in loads:
        load.wait()
    cons = z_ref.shape[0] // 2
    for source in range(2 * cons):
        rows[source * 16 : (source + 1) * 16, :] = z_ref[source].astype(jnp.float32)
    for triple in range(RADIX // TRI):
        h, t = divmod(triple, 8)
        both = [rows[pl.ds(h * 16 + p * 8 + t, cons, stride=32), :] for p in range(2)]
        lines = jnp.concatenate(both, axis=0).T.astype(jnp.bfloat16)
        mixed[triple * LANES : (triple + 1) * LANES, :] = jnp.dot(
            lines, basis_ref[...], preferred_element_type=jnp.float32
        )

    def leave(group):
        lines = pl.ds(pl.multiple_of(group * 8, 8), 8)
        return pltpu.make_async_copy(done.at[group], out_hbm.at[0, lines], out_sems.at[group])

    @pl.loop(0, CYC // 8)
    def _(group):
        turned = []
        for r in range(RADIX):
            start = (r // TRI) * LANES + (r % TRI) * CYC
            place = pl.ds(pl.multiple_of(start + group * 8, 8), 8)
            re, im = mixed[place, 0:LANES], mixed[place, LANES:]
            cos, sin = twiddle_ref[2 * r : 2 * r + 1, :], twiddle_ref[2 * r + 1 : 2 * r + 2, :]
            turned.append((re * cos - im * sin, re * sin + im * cos))
        middle = RADIX // 2
        half = [(turned[0][0] + turned[0][0], None)]
        for r in range(1, middle):
            pair = plus(turned[r], conj(turned[RADIX - r]))
            half.append(pair)
        half.append((turned[middle][0] + turned[middle][0], None))
        for k, value in enumerate(real_inverse(half, RADIX)):
            done[group, :, k * LANES : (k + 1) * LANES] = value
        leave(group).start()

    @pl.loop(0, CYC // 8)
    def _(group):
        leave(group).wait()


def inverse(pieces, period):
    cons = pieces.shape[0] // 2
    twiddle, basis = phase_tables(period)
    twiddle = twiddle * np.float32(0.5)
    return pl.pallas_call(
        inverse_kernel,
        out_shape=jax.ShapeDtypeStruct((1, CYC, period), jnp.float32),
        in_specs=[pl.BlockSpec(memory_space=pltpu.HBM)] * 3,
        out_specs=pl.BlockSpec(memory_space=pltpu.HBM),
        scratch_shapes=[
            pltpu.VMEM(pieces.shape, jnp.bfloat16),
            pltpu.VMEM(twiddle.shape, jnp.float32),
            pltpu.VMEM(basis.shape, jnp.bfloat16),
            pltpu.VMEM((2 * cons * 16, LANES), jnp.float32),
            pltpu.VMEM((RADIX // TRI * LANES, 2 * LANES), jnp.float32),
            pltpu.VMEM((CYC // 8, 8, period), jnp.float32),
            pltpu.SemaphoreType.DMA((3,)),
            pltpu.SemaphoreType.DMA((CYC // 8,)),
        ],
        compiler_params=pltpu.CompilerParams(vmem_limit_bytes=67_000_000),
        name="inverse",
    )(pieces, jnp.asarray(twiddle), jnp.asarray(basis))


MESH = pl.DeviceIdType.MESH
F32 = jnp.float32
BF16 = jnp.bfloat16
KERNEL_ID = 0


def middle_kernel(
    ring, cons, elevation, legendre, cycle_weight, love_factor, assigned, twiddles, bases, out,
    height, weights, love, assignment, twiddle, basis, pieces, spun, spread,
    held, wide, table, got, mixed, lines, part, first, later, staged, sent, other, crossed, coef,
    rows, back,
    own_sem, swap_send, swap_recv, out_send, out_recv, sum_send, pair_send, all_send,
    ring_recv, cross_recv, back_send, back_recv,
):
    c, b = lax.axis_index("cons"), lax.axis_index("blk")
    core = lax.rem(b, 2)
    z = lax.rem(b // 2, ring)
    line = b // (2 * ring)
    chip = b - core
    me = 2 * c + core
    peers = 2 * cons
    far = ring // 2
    depth = legendre.shape[2]
    half_orders = TRI * ring
    full = 2 * cons
    barrier = pltpu.get_barrier_semaphore()

    slots = {offset: lax.rem(z + offset + ring, ring) for offset in range(-far, far + 1)}
    row_start = line * 2 * ring + core
    near = {hops: (c, row_start + 2 * slots[hops]) for hops in (1, -1, 2, -2)}

    def slot(offset):
        return slots[offset]

    def on_ring(offset):
        return near[offset]

    outward = sorted(range(1, peers), key=lambda offset: abs(offset - peers // 2))

    def remote(source, target, send, recv, device):
        return pltpu.make_async_remote_copy(
            src_ref=source,
            dst_ref=target,
            send_sem=send,
            recv_sem=recv,
            device_id=device,
            device_id_type=MESH,
        )

    def peer(offset):
        if offset % 2:
            return lax.rem(c + core + offset // 2, cons), 1 - core
        return lax.rem(c + offset // 2, cons), core

    def exchange(offset, source, landing, send, recv):
        far_c, far_core = peer(offset)
        there = (far_c, chip + far_core)
        return remote(source.at[2 * far_c + far_core], landing.at[me], send, recv, there)

    def exchanged(source, landing, send, recv):
        rest = pl.ds(0, peers - 1)
        return remote(source.at[rest], landing.at[rest], send, recv, (c, chip + 1 - core))

    across = (c, (1 - line) * 2 * ring + z * 2 + core)
    mine_rows = [pl.ds(pl.multiple_of(i * full + line * cons, cons), cons) for i in range(TRI)]

    def half_of(which):
        return legendre.at[:, pl.ds(pl.multiple_of(which * half_orders, 8), half_orders), :]

    mine = pltpu.make_async_copy(half_of(core), held.at[core], own_sem)
    pairs = (
        (elevation, height),
        (twiddles, twiddle),
        (bases, basis),
        (cycle_weight, weights),
        (assigned, assignment),
        (love_factor, love),
    )
    loads = [
        pltpu.make_async_copy(source, target, cross_recv.at[1, i])
        for i, (source, target) in enumerate(pairs)
    ]
    with jax.named_scope("signals"):
        for load in loads:
            load.start()

        for offset in outward:
            far_c, far_core = peer(offset)
            there = (far_c, chip + far_core)
            pl.semaphore_signal(barrier, inc=1, device_id=there, device_id_type=MESH)

        for target in (on_ring(1), on_ring(-1), on_ring(2), on_ring(-2), across):
            pl.semaphore_signal(barrier, inc=1, device_id=target, device_id_type=MESH)
        mine.start()
    with jax.named_scope("loads"):
        for load in loads:
            load.wait()

    with jax.named_scope("fft"):
        lane_of = lax.broadcasted_iota(jnp.int32, (1, LANES), 1)
        day = lane_of - jnp.where(lane_of < CYC, 0, jnp.where(lane_of < 2 * CYC, CYC, 2 * CYC))
        weight = jnp.zeros((1, LANES), F32)
        for j in range(CYC):
            weight = jnp.where(day == j, weights[j], weight)
        transformed(height, weight, twiddle, basis, pieces, spun, spread)

    with jax.named_scope("barrier"):
        pl.semaphore_wait(barrier, peers + 4)

    swap = remote(half_of(1 - core), held.at[core], swap_send, swap_recv, (c, chip + 1 - core))
    swap.start()

    for offset in outward:
        exchange(offset, pieces, got, out_send, out_recv).start()

    got[me] = pieces[me]

    def turn(which):
        @pl.loop(0, CYC)
        def _(j):
            place = pl.ds(pl.multiple_of(j * half_orders, 8), half_orders)
            for tile in range(depth // LANES):
                wide[tile, place, :] = held[
                    which, j, :, tile * LANES : (tile + 1) * LANES
                ].astype(F32)

        @pl.loop(0, ring)
        def _(t):
            place = pl.ds(pl.multiple_of(which * LANES, LANES), LANES)
            for tile in range(depth // LANES):
                taken = [
                    wide[tile, pl.ds(TRI * t + i, CYC, stride=half_orders), :] for i in range(TRI)
                ]
                taken.append(jnp.zeros((LANES - TRI * CYC, LANES), F32))
                table[t, place, tile * LANES : (tile + 1) * LANES] = jnp.concatenate(
                    taken, axis=0
                ).astype(BF16)

    with jax.named_scope("turn_own"):
        mine.wait()
        turn(core)
    with jax.named_scope("swap_wait"):
        swap.wait()
    with jax.named_scope("turn_other"):
        turn(1 - core)

    with jax.named_scope("wait_out"):
        exchanged(pieces, got, out_send, out_recv).wait()

    with jax.named_scope("lines"):
        for g in range(cons):
            field = assignment[g]
            for s in range(2):
                mixed[(s * cons + g) * 16 : (s * cons + g + 1) * 16, :] = got[2 * field + s].astype(F32)
        for t in range(ring):
            for s in range(2):
                for p in range(2):
                    lines[t, p * cons : (p + 1) * cons, s * LANES : (s + 1) * LANES] = mixed[
                        pl.ds(s * cons * 16 + p * 8 + t, cons, stride=16), :
                    ]

    lane = lax.broadcasted_iota(jnp.int32, (full, 2 * LANES), 1)
    lane = jnp.where(lane >= LANES, lane - LANES, lane)
    which = jnp.where(lane < CYC, 0, jnp.where(lane < 2 * CYC, 1, jnp.where(lane < TRI * CYC, 2, 3)))

    def analysed(t):
        x = lines[t]
        left = [jnp.where(which == i, x, 0.0) for i in range(TRI)]
        made = jnp.dot(
            jnp.concatenate(left, axis=0).astype(BF16), table[t], preferred_element_type=F32
        )
        part[t] = made.astype(BF16).reshape(TRI, 2, cons, depth)

    def piece(i, p):
        return pl.ds(pl.multiple_of(i * full + p * cons, cons), cons)

    ways, triples, ends = (1, -1), range(TRI), range(2)
    scale = love[...].reshape(1, depth)

    def synthesised(t):
        got_all = lax.dot_general(
            coef[t], table[t], (((1,), (1,)), ((), ())), preferred_element_type=F32
        )
        chosen = jnp.where(
            which == 0,
            got_all[:full],
            jnp.where(which == 1, got_all[full : 2 * full], got_all[2 * full :]),
        )
        order = which + (TRI * t + core * half_orders + c * 2 * half_orders)
        chosen = chosen * jnp.where(order == 0, 1.0, 2.0).astype(F32)
        for s in range(2):
            place = pl.ds(pl.multiple_of(s * ring * full + t * full, 8), full)
            rows[place, :] = chosen[:, s * LANES : (s + 1) * LANES]

    def sum_sent(source, target, way, step, i, p, hops=1):
        return remote(
            source, target, sum_send, ring_recv.at[way, step, i, p], on_ring(hops * ways[way])
        )

    @pl.when(core == 0)
    def _():
        def sum_step(way, step, i, p):
            if step == 0:
                source = part.at[slot(far), i, p]
                return sum_sent(source, first.at[way, i], way, step, i, p, 2)
            target = later.at[way, step - 1, i, p]
            if step == 1:
                source = part.at[slot(ways[way] * (far - 1)), i, p]
            else:
                source = staged.at[way, step - 1, i, p]
            return sum_sent(source, target, way, step, i, p)

        with jax.named_scope("first_part"):
            analysed(slot(far))
            for way in ends:
                sum_step(way, 0, 0, way).start()
            for way in ends:
                analysed(slot(ways[way] * (far - 1)))
                for i in triples:
                    if i:
                        sum_step(way, 0, i, way).start()
                    for p in (1 - way, way):
                        sum_step(way, 1, i, p).start()
            for step in range(2, far):
                for way in ends:
                    analysed(slot(ways[way] * (far - step)))
            analysed(z)
        for step in range(2, far):
            with jax.named_scope(f"sum#s={step}"):
                for i in triples:
                    for late in ends:
                        for way in ends:
                            p = way if late else 1 - way
                            owner = slot(ways[way] * (far - step))
                            sum_step(way, step - 1, i, p).wait_recv()
                            total = part[owner, i, p].astype(F32) + later[
                                way, step - 2, i, p
                            ].astype(F32)
                            if step == 2 and late:
                                sum_step(way, 0, i, p).wait_recv()
                                total = total + first[way, i].astype(F32)
                            staged[way, step - 1, i, p] = total.astype(BF16)
                            sum_step(way, step, i, p).start()

        def pair_step(i, p):
            return remote(
                sent.at[i, p], other.at[i, p], pair_send, cross_recv.at[0, 2 * i + p], across
            )

        with jax.named_scope("last_sum"):
            for i in triples:
                for p in ends:
                    for way in ends:
                        sum_step(way, far - 1, i, p).wait_recv()
                    sent[i, p] = (
                        part[z, i, p].astype(F32)
                        + later[0, far - 2, i, p].astype(F32)
                        + later[1, far - 2, i, p].astype(F32)
                    ).astype(BF16)
                    pair_step(i, p).start()

        def all_step(way, step, i, p, late=0):
            hops = 2 if step == far else 1
            distance = far - 2 if step == far else step
            distance = distance + late * hops
            ref = coef.at[slot(-ways[way] * distance), piece(i, p)]
            if step == far:
                recv = cross_recv.at[1, TRI * way + i]
            else:
                recv = ring_recv.at[way, step, i, p]
            return remote(ref, ref, all_send, recv, on_ring(hops * ways[way]))

        with jax.named_scope("pair"):
            for i in triples:
                for p in ends:
                    pair_step(i, p).wait_recv()
                    coef[z, piece(i, p), :] = (
                        (sent[i, p].astype(F32) + other[i, p].astype(F32)) * scale
                    ).astype(BF16)
                    for way in ends:
                        all_step(way, 0, i, p).start()
        for step in range(1, far - 1):
            with jax.named_scope(f"all#s={step}"):
                for i in triples:
                    for p in ends:
                        for way in ends:
                            all_step(way, step - 1, i, p, 1).wait_recv()
                            if step == far - 2 and p == way:
                                all_step(way, far, i, p).start()
                            all_step(way, step, i, p).start()
            with jax.named_scope(f"synth#s={step}"):
                for owner in (0,) if step == 1 else (step - 1, 1 - step):
                    synthesised(slot(owner))
        with jax.named_scope("synth_last"):
            for owner in (far - 2, 2 - far):
                synthesised(slot(owner))
        with jax.named_scope("all_last"):
            for i in triples:
                for p in ends:
                    for way in ends:
                        all_step(way, far - 2, i, p, 1).wait_recv()
            for owner in (far - 1, 1 - far):
                synthesised(slot(owner))
            for i in triples:
                for way in ends:
                    all_step(way, far, i, way, 1).wait_recv()
        with jax.named_scope("synth_far"):
            synthesised(slot(far))
        most = pl.ds(0, ring - 1)
        remote(part.at[most], part.at[most], sum_send, own_sem, across).wait_send()
        remote(coef.at[most], coef.at[most], all_send, own_sem, across).wait_send()
        remote(sent, other, pair_send, own_sem, across).wait_send()

    @pl.when(core == 1)
    def _():
        owners = [far]
        for distance in range(far - 1, 0, -1):
            owners += [distance, -distance]
        owners.append(0)

        def mixed_sum(owner, i):
            k = owners.index(owner)
            return part[slot(owner), i, line].astype(F32) + crossed[k, i].astype(F32)

        def taken(owner, turn):
            k = owners.index(owner)
            remote(
                crossed.at[k], crossed.at[k], pair_send, cross_recv.at[turn, k], across
            ).wait_recv()

        def sum_step(way, step, i):
            if step == 0:
                return sum_sent(sent.at[i, 0], first.at[way, i], way, 0, i, 0)
            source, target = staged.at[way, step - 1, i, 0], later.at[way, step - 1, i, 0]
            return sum_sent(source, target, way, step, i, 0)

        with jax.named_scope("first_part"):
            for k, owner in enumerate(owners):
                analysed(slot(owner))
                remote(
                    part.at[slot(owner), :, 1 - line],
                    crossed.at[k],
                    pair_send,
                    cross_recv.at[0, k],
                    across,
                ).start()
        with jax.named_scope("sum#s=0"):
            taken(far, 0)
            for i in triples:
                sent[i, 0] = mixed_sum(far, i).astype(BF16)
                sum_step(i % 2, 0, i).start()
        for step in range(1, far):
            with jax.named_scope(f"sum#s={step}"):
                for way in ends:
                    taken(ways[way] * (far - step), 0)
                for late in ends:
                    for i in triples:
                        for way in ends:
                            if late != (way == i % 2):
                                continue
                            total = mixed_sum(ways[way] * (far - step), i)
                            if step > 1 or late:
                                sum_step(way, step - 1, i).wait_recv()
                                come = first[way, i] if step == 1 else later[way, step - 2, i, 0]
                                total = total + come.astype(F32)
                            staged[way, step - 1, i, 0] = total.astype(BF16)
                            sum_step(way, step, i).start()

        def all_step(way, step, i, late=0):
            direct = int(step == far - 1)
            distance = step - direct + late * (1 + direct)
            ref = coef.at[slot(-ways[way] * distance), mine_rows[i]]
            recv = ring_recv.at[way, step, i, direct]
            return remote(ref, ref, all_send, recv, on_ring((1 + direct) * ways[way]))

        def shared(owner, i):
            ref = coef.at[slot(owner), mine_rows[i]]
            k = owners.index(owner)
            return remote(ref, ref, pair_send, cross_recv.at[1, k], across)

        with jax.named_scope("last_sum"):
            taken(0, 0)
            for i in triples:
                for way in ends:
                    sum_step(way, far - 1, i).wait_recv()
                coef[z, mine_rows[i], :] = (
                    (
                        mixed_sum(0, i)
                        + later[0, far - 2, i, 0].astype(F32)
                        + later[1, far - 2, i, 0].astype(F32)
                    )
                    * scale
                ).astype(BF16)
                for way in ends:
                    all_step(way, 0, i).start()
                shared(0, i).start()

        def ended(owner):
            taken(owner, 1)
            synthesised(slot(owner))

        for step in range(1, far):
            with jax.named_scope(f"all#s={step}"):
                for i in triples:
                    for way in ends:
                        all_step(way, step - 1, i, 1).wait_recv()
                        if step == far - 2 and way == i % 2:
                            all_step(way, far - 1, i).start()
                        if step < far - 1:
                            all_step(way, step, i).start()
                        shared(-ways[way] * step, i).start()
            with jax.named_scope(f"synth#s={step}"):
                if step == 2:
                    ended(0)
                elif step == 3:
                    for way in ways:
                        ended(way)
        with jax.named_scope("all_last"):
            for i in triples:
                all_step(i % 2, far - 1, i, 1).wait_recv()
                shared(far, i).start()
        with jax.named_scope("synth_last"):
            for distance in range(2, far):
                for way in ways:
                    ended(way * distance)
            ended(far)
        most = pl.ds(0, ring - 1)
        remote(crossed.at[most], crossed.at[most], sum_send, own_sem, across).wait_send()
        remote(crossed.at[most], crossed.at[most], all_send, own_sem, across).wait_send()
        remote(coef, coef, pair_send, own_sem, across).wait_send()

    with jax.named_scope("back"):
        for g in range(cons):
            for s in range(2):
                both = [
                    rows[pl.ds(s * ring * full + p * cons + g, ring, stride=full), :] for p in range(2)
                ]
                back[2 * g + s] = jnp.concatenate(both, axis=0).astype(BF16)

    for offset in outward:
        exchange(offset, back, out, back_send, back_recv).start()

    kept = pltpu.make_async_copy(back.at[me], out.at[me], own_sem)
    kept.start()

    with jax.named_scope("wait_sends"):
        kept.wait()

    with jax.named_scope("wait_back"):
        exchanged(back, out, back_send, back_recv).wait()


def middle(elevation, legendre, cycle_weight, love_factor, assignment):
    cons = lax.axis_size("cons")
    period = elevation.shape[-1]
    depth = legendre.shape[2]
    ring = 8
    far = ring // 2
    full = 2 * cons
    dma = pltpu.SemaphoreType.DMA
    vmem = pltpu.VMEM
    twiddle, basis = phase_tables(period)
    pieces = (2 * cons, 16, LANES)
    return pl.pallas_call(
        functools.partial(middle_kernel, ring, cons),
        out_shape=jax.ShapeDtypeStruct(pieces, BF16),
        in_specs=[pl.BlockSpec(memory_space=pltpu.HBM)] * 7,
        out_specs=pl.BlockSpec(memory_space=pltpu.HBM),
        scratch_shapes=[
            vmem((1, CYC, period), BF16),
            pltpu.SMEM((CYC,), F32),
            vmem((depth,), F32),
            pltpu.SMEM((cons,), jnp.int32),
            vmem(twiddle.shape, F32),
            vmem(basis.shape, BF16),
            vmem(pieces, BF16),
            vmem((RADIX // TRI * LANES, 2 * LANES), F32),
            vmem((RADIX // TRI * full, LANES), F32),
            vmem((2, CYC, TRI * ring, depth), BF16),
            vmem((depth // LANES, CYC * TRI * ring, LANES), F32),
            vmem((ring, 2 * LANES, depth), BF16),
            vmem(pieces, BF16),
            vmem((2 * cons * 16, LANES), F32),
            vmem((ring, full, 2 * LANES), F32),
            vmem((ring, TRI, 2, cons, depth), BF16),
            vmem((2, TRI, cons, depth), BF16),
            vmem((2, far - 1, TRI, 2, cons, depth), BF16),
            vmem((2, far - 1, TRI, 2, cons, depth), BF16),
            vmem((TRI, 2, cons, depth), BF16),
            vmem((TRI, 2, cons, depth), BF16),
            vmem((ring, TRI, cons, depth), BF16),
            vmem((ring, TRI * full, depth), BF16),
            vmem((2 * ring * full, LANES), F32),
            vmem(pieces, BF16),
            dma,
            dma,
            dma,
            dma,
            dma,
            dma,
            dma,
            dma,
            dma((2, far, TRI, 2)),
            dma((2, ring)),
            dma,
            dma,
        ],
        compiler_params=pltpu.CompilerParams(
            collective_id=KERNEL_ID, has_side_effects=True, vmem_limit_bytes=67_000_000
        ),
        name="middle",
    )(
        elevation,
        legendre,
        cycle_weight,
        love_factor,
        assignment,
        jnp.asarray(twiddle),
        jnp.asarray(basis),
    )


def local(elevation, legendre, cycle_weight, love_factor, assignment):
    returned = middle(elevation, legendre, cycle_weight, love_factor, assignment)
    return inverse(returned, elevation.shape[-1])


def solution(mesh):
    placed = (P("cons", "blk", None), P("blk", "cons", None), P("blk"), P(), P())
    return jax.shard_map(
        local, mesh=mesh, in_specs=placed, out_specs=P("cons", "blk", None), check_vma=False
    )
```
